16 devices in a mesh: rep: 1, dp: 16 (over x, y, z, core).
Axes of the slice: x: 2, y: 2, z: 2, core: 2. Of those that a mesh axis runs over, the one named last changes fastest.
Arguments:
- x: bfloat16 [16, 2048, 1024], P(('rep', 'dp'))
- dy: bfloat16 [16, 2048, 1024], P(('rep', 'dp'))
- wq: bfloat16 [2, 1024, 1024], P(None, 'dp')
- wk: bfloat16 [2, 1024, 256], P(None, 'dp')
- wv: bfloat16 [2, 1024, 256], P(None, 'dp')
- wo: bfloat16 [2, 1024, 1024], P(None, 'dp')
- w_gate: bfloat16 [2, 1024, 3200], P(None, 'dp')
- w_up: bfloat16 [2, 1024, 3200], P(None, 'dp')
- w_down: bfloat16 [2, 3200, 1024], P(None, 'dp')
Outputs:
- output 1: bfloat16 [16, 2048, 1024], P(('rep', 'dp'))
- output 2: bfloat16 [2, 1024, 1024], P('rep', 'dp')
- output 3: bfloat16 [2, 1024, 256], P('rep', 'dp')
- output 4: bfloat16 [2, 1024, 256], P('rep', 'dp')
- output 5: bfloat16 [2, 1024, 1024], P('rep', 'dp')
- output 6: bfloat16 [2, 1024, 3200], P('rep', 'dp')
- output 7: bfloat16 [2, 1024, 3200], P('rep', 'dp')
- output 8: bfloat16 [2, 3200, 1024], P('rep', 'dp')
All inputs are finite; a program needn't handle non-finite values.
Results may differ from the reference program's by a relative error of at most 0.0241.
Values are sent between devices in bfloat16 or wider.
A program may use at most 2 GiB of HBM per device.

```python
import jax
import jax.numpy as jnp
from jax import lax

SEQUENCES = 16
TOKENS = 2048
D = 1024
HEADS = 8
KV_HEADS = 2
HEAD = 128
FF = 3200
LAYERS = 2
THETA = 10000
NAMES = ("wq", "wk", "wv", "wo", "w_gate", "w_up", "w_down")
SHAPES = {
    "wq": (LAYERS, D, HEADS * HEAD),
    "wk": (LAYERS, D, KV_HEADS * HEAD),
    "wv": (LAYERS, D, KV_HEADS * HEAD),
    "wo": (LAYERS, HEADS * HEAD, D),
    "w_gate": (LAYERS, D, FF),
    "w_up": (LAYERS, D, FF),
    "w_down": (LAYERS, FF, D),
}


def bump(key, n, height):
    away = (jnp.arange(n, dtype=jnp.int32) - jax.random.randint(key, (), 0, n, jnp.int32)) % n
    return jnp.where(away < n // 8, height, 1.0)


def together(key, own, strength):
    shared = jax.random.normal(key, own.shape[1:], jnp.float32)
    return (own + strength * shared) * lax.rsqrt(1 + strength * strength)


def setup_inputs(seed: int = 0, part: int = 0) -> dict:
    kx, kdy, ka, kb, kz, kf, kh, kl, *keys = jax.random.split(jax.random.key(seed), 8 + 3 * len(NAMES))
    kx, kdy, ka, kb = (jax.random.fold_in(k, part) for k in (kx, kdy, ka, kb))
    kw, km, kv = (keys[i::3] for i in range(3))
    shape = (SEQUENCES, TOKENS, D)
    much_x, much_dy = jax.random.uniform(kz, (2,), jnp.float32, 0.0, 1.0)
    loud = 2.0 ** jax.random.uniform(jax.random.fold_in(kz, 1), (), jnp.float32, -1.0, 2.0)
    layers = 2.0 ** jax.random.uniform(kl, (LAYERS, 1, 1), jnp.float32, -1.0, 1.0)
    times = {"wq": 1.0, "wk": 1.0, "wv": 2.0, "wo": layers, "w_gate": 1.0, "w_up": bump(kh, FF, 4.0), "w_down": layers}
    x = together(ka, jax.random.normal(kx, shape, jnp.float32), much_x) * bump(kf, D, 4.0)
    dy = together(kb, jax.random.normal(kdy, shape, jnp.float32), much_dy)
    drawn = {"x": x.astype(jnp.bfloat16), "dy": (loud * dy * (SEQUENCES * TOKENS) ** -0.5).astype(jnp.bfloat16)}
    for key, name in zip(kw, NAMES, strict=True):
        drawn[name] = (jax.random.normal(key, SHAPES[name], jnp.float32) * SHAPES[name][1] ** -0.5 * times[name]).astype(jnp.bfloat16)
    return drawn


def matmul(a, w):
    return jnp.dot(a, w, preferred_element_type=jnp.float32).astype(jnp.bfloat16)


def normed(h):
    wide = h.astype(jnp.float32)
    scale = lax.rsqrt(jnp.mean(wide**2, -1, keepdims=True) + 1e-6)
    return (wide * scale).astype(jnp.bfloat16)


def turned(t, theta):
    half = t.shape[-1] // 2
    angle = jnp.arange(t.shape[0], dtype=jnp.float32)[:, None] * theta ** (-jnp.arange(half, dtype=jnp.float32) / half)
    cos, sin = jnp.cos(angle)[:, None], jnp.sin(angle)[:, None]
    a, b = t[..., :half].astype(jnp.float32), t[..., half:].astype(jnp.float32)
    return jnp.concatenate([a * cos - b * sin, b * cos + a * sin], -1).astype(jnp.bfloat16)


def seen_by(q, k, v):
    tokens, kv = q.shape[0], k.shape[1]
    q = q.reshape(tokens, kv, -1, q.shape[-1])
    scores = jnp.einsum("tgsd,ugd->gstu", q.astype(jnp.float32), k.astype(jnp.float32)) * q.shape[-1] ** -0.5
    place = jnp.arange(tokens)
    weights = jax.nn.softmax(jnp.where(place[:, None] >= place, scores, -jnp.inf), -1).astype(jnp.bfloat16)
    return jnp.einsum("gstu,ugd->tgsd", weights.astype(jnp.float32), v.astype(jnp.float32)).astype(jnp.bfloat16).reshape(tokens, -1)


def layer(h, w):
    a = normed(h)
    q, k = (turned(matmul(a, w[name]).reshape(h.shape[0], -1, HEAD), THETA) for name in ("wq", "wk"))
    h = h + matmul(seen_by(q, k, matmul(a, w["wv"]).reshape(h.shape[0], -1, HEAD)), w["wo"])
    b = normed(h)
    gate = jnp.dot(b, w["w_gate"], preferred_element_type=jnp.float32)
    up = jnp.dot(b, w["w_up"], preferred_element_type=jnp.float32)
    return h + matmul((jax.nn.silu(gate) * up).astype(jnp.bfloat16), w["w_down"])


def stack(weights, h):
    return lax.scan(lambda h, w: (layer(h, w), None), h, weights)[0]


def reference(x, dy, wq, wk, wv, wo, w_gate, w_up, w_down):
    weights = dict(zip(NAMES, (wq, wk, wv, wo, w_gate, w_up, w_down), strict=True))

    def take(so_far, sequence):
        h, by_y = sequence
        _, back = jax.vjp(stack, weights, h)
        by_weights, by_h = back(by_y)
        return jax.tree.map(lambda total, term: total + term.astype(jnp.float32), so_far, by_weights), by_h

    none_yet = {name: jnp.zeros(w.shape, jnp.float32) for name, w in weights.items()}
    by_weights, by_x = lax.scan(take, none_yet, (x, dy))
    return (by_x, *(by_weights[name].astype(jnp.bfloat16) for name in NAMES))
```

```python
import functools

import jax
import jax.numpy as jnp
import numpy as np
from jax import lax
from jax.experimental import pallas as pl
from jax.experimental.pallas import tpu as pltpu
from jax.sharding import PartitionSpec as P

T, D, HEADS, KV, HEAD, FF, THETA = 2048, 1024, 8, 2, 128, 3200, 10000
G = HEADS // KV
QKV = D + 2 * KV * HEAD
THIRD = QKV // 3
BF, F32 = jnp.bfloat16, jnp.float32
LOG2E = 1.4426950408889634
SCALE = HEAD**-0.5
NEG, HIDDEN = -1e30, -2e30
ANY = pl.BlockSpec(memory_space=pl.ANY)


def params(**kw):
    return pltpu.CompilerParams(vmem_limit_bytes=62 * 2**20, **kw)


def sds(shape, dtype=BF):
    return jax.ShapeDtypeStruct(shape, dtype)


def rows(bm, n):
    return pl.BlockSpec((bm, n), lambda i: (i, 0))


def held(shape):
    return pl.BlockSpec(shape, lambda i: (0,) * len(shape), pipeline_mode=pl.Buffered(1))


def dot(a, b, ca=1, cb=0):
    return lax.dot_general(a, b, (((ca,), (cb,)), ((), ())), preferred_element_type=F32)


def low(x):
    return x.astype(BF)


def wide(x):
    return x.astype(F32)


def norm_scale(w):
    return lax.rsqrt(jnp.mean(w * w, -1, keepdims=True) + 1e-6)


def normed(h):
    w = wide(h)
    return low(w * norm_scale(w))


def norm_back(h, c):
    w = wide(h)
    s = norm_scale(w)
    return s * (c - w * (s * s) * jnp.mean(c * w, -1, keepdims=True))


def tables():
    half = HEAD // 2
    angle = np.arange(T, dtype=np.float32)[:, None] * (np.float32(THETA) ** (-np.arange(half, dtype=np.float32) / np.float32(half)))
    cos, sin = np.cos(angle).astype(np.float32), np.sin(angle).astype(np.float32)
    return np.concatenate([cos, cos], 1), np.concatenate([-sin, sin], 1)


def heads_of(x):
    return [x[:, HEAD * n : HEAD * (n + 1)] for n in range(x.shape[1] // HEAD)]


def turned(x, c, s):
    return [low(t * c + pltpu.roll(t, HEAD // 2, 1) * s) for t in heads_of(x)]


def flipped(number, bits):
    for bit in (1, 2, 4, 8):
        if bits & bit:
            number = number + bit - 2 * bit * (lax.div(number, bit) % 2)
    return number


AXES = ((4, 2, 1), (2, 1, 4), (1, 4, 2))


def thirds(n):
    units = n // 128
    sizes = [128 * (units // 3 + (r < units % 3)) for r in range(3)]
    return [(sum(sizes[:r]), sizes[r], axes) for r, axes in enumerate(AXES)]


class Gather:
    copies = 48
    partners = {1, 2, 4, 8}

    def __init__(self, src, layer, part=None):
        self.src, self.layer, self.part = src, layer, part
        rows, n = src.shape[1:]
        self.shapes = [(8, 2, rows, n if part is None else part[1])]

    def bind(self, src, dst, send, recv):
        me = lax.axis_index("dp")
        chip, core = lax.div(me, 2), me % 2
        self.stages = [[], [], [], []]
        at = 0 if self.part is None else self.part[0]
        for r, (first, n, (a, b, c)) in enumerate(thirds(dst.shape[3])):
            own = src.at[self.layer, :, pl.ds(at + first, n)]
            block = lambda bits: dst.at[flipped(chip, bits), core, :, pl.ds(first, n)]

            def to(k, what, bits, where):
                k += 16 * r
                return pltpu.make_async_remote_copy(what, block(where), send.at[k], recv.at[k], device_id={"dp": flipped(me, bits)})

            here = lambda m: block(m) if m else own
            self.stages[0].append(([to(0, own, 2 * a, 0)], [to(1, own, 1, 0)]))
            self.stages[1].append(([to(2 + k, here(m), 2 * b, m) for k, m in enumerate((0, a))], [to(4, block(a), 1, a)]))
            self.stages[2].append(([to(5 + k, here(m), 2 * c, m) for k, m in enumerate((0, a, b, a | b))],
                                   [to(9 + k, block(m), 1, m) for k, m in enumerate((b, a | b))]))
            self.stages[3].append(([], [to(11 + k, block(c | m), 1, c | m) for k, m in enumerate((0, a, b, a | b))]))
        self.local = pltpu.make_async_copy(src.at[self.layer, :, pl.ds(at, dst.shape[3])], dst.at[chip, core], send.at[15])

    def stage(self, n):
        if n == 0:
            self.local.start()
        else:
            for first, _ in self.stages[n - 1]:
                for c in first:
                    c.wait_recv()
        for first, rest in self.stages[n]:
            for c in first + rest:
                c.start()

    def end(self):
        for s in self.stages:
            for first, rest in s:
                for c in rest:
                    c.wait_recv()
                for c in first + rest:
                    c.wait_send()
        self.local.wait()


class Once:
    def stage(self, n):
        if n == 0:
            for c in self.all:
                c.start()

    def end(self):
        for c in self.all:
            c.wait()


class Swap(Once):
    copies = 1
    partners = {1}

    def __init__(self, src):
        self.src = src
        self.shapes = [(src.shape[0], *src.shape[2:])]

    def bind(self, src, dst, send, recv):
        me = lax.axis_index("dp")
        self.all = [pltpu.make_async_remote_copy(src.at[:, 1 - me % 2], dst, send.at[0], recv.at[0], device_id={"dp": flipped(me, 1)})]


class Scatter(Once):
    copies = 7
    partners = {2, 4, 6, 8, 10, 12, 14}

    def __init__(self, src):
        self.src = src
        self.shapes = [(7, *src.shape[1:])]

    def bind(self, src, dst, send, recv):
        me = lax.axis_index("dp")
        chip = lax.div(me, 2)
        self.all = [
            pltpu.make_async_remote_copy(src.at[flipped(chip, m)], dst.at[m - 1], send.at[m - 1], recv.at[m - 1], device_id={"dp": flipped(me, 2 * m)})
            for m in (7, 3, 5, 6, 1, 2, 4)
        ]


def across(ref, axis, index):
    return ref.at[{4: (index,), 2: (slice(None), index), 1: (slice(None), slice(None), index)}[axis]]


def bit(chip, axis):
    return lax.div(chip, axis) % 2


class Halve(Once):
    copies = 3
    partners = {2, 4, 8}

    def __init__(self, src):
        self.src = src
        self.shapes = [(2, 2, src.shape[3], n) for _, n, _ in thirds(src.shape[4])]

    def bind(self, src, dst, send, recv):
        me = lax.axis_index("dp")
        chip = lax.div(me, 2)
        self.all = []
        for r, (first, n, (a, _, _)) in enumerate(thirds(src.shape[4])):
            what = across(src.at[:, :, :, :, pl.ds(first, n)], a, 1 - bit(chip, a))
            self.all.append(pltpu.make_async_remote_copy(what, dst[r], send.at[r], recv.at[r], device_id={"dp": flipped(me, 2 * a)}))


class Spread(Once):
    copies = 3

    def __init__(self, src, axis):
        self.src, self.axis = src, axis
        self.planes = tuple(b for b in (4, 2, 1) if b != axis)
        p, q = self.planes
        self.partners = {2 * p, 2 * q, 2 * (p + q)}
        self.shapes = [(3, *src.shape[2:])]

    def bind(self, src, dst, send, recv):
        me = lax.axis_index("dp")
        chip = lax.div(me, 2)
        p, q = self.planes
        self.all = []
        for k, (fp, fq) in enumerate(((1, 1), (1, 0), (0, 1))):
            i, j = ((1 - bit(chip, a)) if f else bit(chip, a) for a, f in ((p, fp), (q, fq)))
            self.all.append(pltpu.make_async_remote_copy(src.at[i, j], dst.at[k], send.at[k], recv.at[k],
                                                         device_id={"dp": flipped(me, 2 * (p * fp + q * fq))}))


def meet(partners):
    me = lax.axis_index("dp")
    barrier = pltpu.get_barrier_semaphore()
    for bits in sorted(partners):
        pl.semaphore_signal(barrier, inc=1, device_id={"dp": flipped(me, bits)})
    pl.semaphore_wait(barrier, len(partners))


def run(body, name, steps, ins, in_specs, outs, out_specs, scratch=(), flops=0, moved=0, exps=0, send=(), ident=None, marks=None, partners=()):
    n_in, n_out, n_send, n_scratch = len(ins), len(outs), len(send), len(scratch)
    counts = [len(t.shapes) for t in send]
    marks = (0, *(marks or (1, 2, 3)))
    partners = set(partners).union(*(t.partners for t in send))

    def kernel(*refs):
        def take(n):
            nonlocal refs
            got, refs = refs[:n], refs[n:]
            return got

        a, c_src, o = take(n_in), take(n_send), take(n_out)
        c_dst = [take(n) for n in counts]
        s, sems = take(n_scratch), refs
        i = pl.program_id(0)
        for n, t in enumerate(send):
            t.bind(c_src[n], c_dst[n] if counts[n] > 1 else c_dst[n][0], sems[2 * n], sems[2 * n + 1])
        staged = any(isinstance(t, Gather) for t in send)
        if partners:
            for n, mark in enumerate(marks if staged else marks[:1]):
                if mark < steps:
                    @pl.when(i == mark)
                    def _():
                        if n == 0:
                            meet(partners)
                        for t in send:
                            t.stage(n)

        body(*a, *o, *s)
        if send:
            @pl.when(i == steps - 1)
            def _():
                for n, mark in enumerate(marks if staged else ()):
                    if mark >= steps:
                        for t in send:
                            t.stage(n)
                for t in send:
                    t.end()

    got = list(pl.pallas_call(
        kernel, grid=(steps,), in_specs=[*in_specs, *[ANY] * n_send], out_specs=[*out_specs, *[ANY] * sum(counts)],
        out_shape=[*outs, *(sds(shape) for t in send for shape in t.shapes)],
        scratch_shapes=[*scratch, *(pltpu.SemaphoreType.DMA((t.copies,)) for t in send for _ in range(2))],
        compiler_params=params(**(dict(collective_id=ident, has_side_effects=True) if partners else {})), name=name,
        cost_estimate=pl.CostEstimate(flops=flops, bytes_accessed=moved, transcendentals=exps),
    )(*ins, *(t.src for t in send)))
    results, got = got[:n_out], got[n_out:]
    sent = []
    for n in counts:
        sent.append(got[:n] if n > 1 else got[0])
        got = got[n:]
    return results, sent


def _qkv(h, c, s, w0, w1, w2, q, k, v, a_out):
    a = normed(h[...])
    a_out[...] = a
    cc, ss = c[...], s[...]
    for part, w in enumerate((w0, w1)):
        for n, t in enumerate(turned(wide(low(dot(a, w[...]))), cc, ss)):
            at = HEAD * (n + part * G)
            q[:, at : at + HEAD] = t
    kv = low(dot(a, w2[...]))
    for n, t in enumerate(turned(wide(kv[:, : KV * HEAD]), cc, ss)):
        k[:, HEAD * n : HEAD * (n + 1)] = t
    v[...] = kv[:, KV * HEAD :]


def qkv(h, w, cs, bm=512, **kw):
    kv = KV * HEAD
    return run(_qkv, "qkv", T // bm, [h, *cs, *w], [rows(bm, D), rows(bm, HEAD), rows(bm, HEAD)] + [held((D, THIRD))] * 3,
               [sds((T, D)), sds((T, kv)), sds((T, kv)), sds((T, D))], [rows(bm, D), rows(bm, kv), rows(bm, kv), rows(bm, D)],
               flops=2 * T * D * QKV, moved=12 * 2**20, **kw)


def _attend(q, k, v, o, lse, top_s, mix_s, *, bq, bk):
    iq = pl.program_id(0)
    e = SCALE * LOG2E
    top_s[...] = jnp.full(top_s.shape, NEG, F32)
    mix_s[...] = jnp.zeros(mix_s.shape, F32)
    ones = jnp.ones((8, bk), BF)
    per = bq // bk

    def block(j, ok):
        here = pl.ds(pl.multiple_of(j * bk, bk), bk)
        scores = [dot(k[here, HEAD * (n // G) : HEAD * (n // G + 1)], q[:, HEAD * n : HEAD * (n + 1)], 1, 1) for n in range(HEADS)]
        weights, keeps = [], []
        for n, s in enumerate(scores):
            if ok is not None:
                s = jnp.where(ok, s, HIDDEN)
            old = top_s[n : n + 1, :]
            top = jnp.maximum(old, s.max(axis=0, keepdims=True))
            top_s[n : n + 1, :] = top
            weights.append(low(jnp.exp2((s - top) * e)))
            keeps.append(jnp.exp2((old - top) * e))
        for n in range(HEADS):
            i = n // G
            values = jnp.concatenate([v[here, HEAD * i : HEAD * (i + 1)].T, ones], axis=0)
            mix_s[n] = mix_s[n] * keeps[n] + dot(values, weights[n], 1, 0)

    lax.fori_loop(0, iq * per, lambda j, _: block(j, None), None)
    gap = lax.broadcasted_iota(jnp.int32, (bk, bq), 1) - lax.broadcasted_iota(jnp.int32, (bk, bq), 0)
    for r in range(per):
        block(iq * per + r, gap >= r * bk)
    for n in range(HEADS):
        total = mix_s[n, HEAD : HEAD + 1, :]
        o[:, HEAD * n : HEAD * (n + 1)] = low((mix_s[n, :HEAD, :] * (1 / total)).T)
        lse[n : n + 1, :] = top_s[n : n + 1, :] * SCALE + jnp.log(total)


def attend(q, k, v, bq=512, bk=512, **kw):
    return run(functools.partial(_attend, bq=bq, bk=bk), "attend", T // bq, [q, k, v],
               [rows(bq, D), held((T, KV * HEAD)), held((T, KV * HEAD))],
               [sds((T, D)), sds((HEADS, T), F32)], [rows(bq, D), pl.BlockSpec((HEADS, bq), lambda i: (0, i))],
               [pltpu.VMEM((HEADS, bq), F32), pltpu.VMEM((HEADS, HEAD + 8, bq), F32)],
               flops=4 * T * T * D, moved=12 * 2**20, exps=HEADS * T * T, **kw)


CHUNKS = ((0, 768), (768, 768), (1536, 768), (2304, 896))


def fetched(pairs, sem):
    return [pltpu.make_async_copy(a, b, sem.at[n]) for n, (a, b) in enumerate(pairs)]


def into(w, pieces):
    at, out = 0, []
    for p in pieces:
        out.append((p, w.at[:, pl.ds(at, p.shape[1])]))
        at += p.shape[1]
    return out


def _mlp_up(h, at, wo_h, *rest, n_gate, n_up):
    wg_h, wu_h, (hm, gate, up, act, wo, wg, wu, sem) = rest[:n_gate], rest[n_gate : n_gate + n_up], rest[n_gate + n_up :]
    first = pl.program_id(0) == 0
    cp = fetched([(wo_h, wo), *into(wg, wg_h), *into(wu, wu_h)], sem)

    @pl.when(first)
    def _():
        for c in cp:
            c.start()
        cp[0].wait()

    m = low(wide(h[...]) + wide(low(dot(at[...], wo[...]))))
    hm[...] = m
    b = normed(m)

    @pl.when(first)
    def _():
        for c in cp[1:]:
            c.wait()

    for a, n in CHUNKS:
        g, u = dot(b, wg[:, a : a + n]), dot(b, wu[:, a : a + n])
        gate[:, a : a + n] = g
        up[:, a : a + n] = u
        act[:, a : a + n] = low(jax.nn.silu(g) * u)


def mlp_up(h, at, wo, wg, wu, bm=256, **kw):
    return run(functools.partial(_mlp_up, n_gate=len(wg), n_up=len(wu)), "mlp_up", T // bm, [h, at, wo, *wg, *wu],
               [rows(bm, D), rows(bm, D)] + [ANY] * (1 + len(wg) + len(wu)),
               [sds((T, D)), sds((T, FF), F32), sds((T, FF), F32), sds((T, FF))], [rows(bm, D), rows(bm, FF), rows(bm, FF), rows(bm, FF)],
               [pltpu.VMEM((D, D), BF), pltpu.VMEM((D, FF), BF), pltpu.VMEM((D, FF), BF), pltpu.SemaphoreType.DMA((1 + len(wg) + len(wu),))],
               flops=2 * T * D * (D + 2 * FF), moved=90 * 2**20, exps=T * FF, **kw)


def _mlp_down(m, act, wd, y):
    y[...] = low(wide(m[...]) + wide(low(dot(act[...], wd[...]))))


def mlp_down(m, act, wd, bm=512, **kw):
    return run(_mlp_down, "mlp_down", T // bm, [m, act, wd], [rows(bm, D), rows(bm, FF), held((FF, D))], [sds((T, D))], [rows(bm, D)],
               flops=2 * T * D * FF, moved=28 * 2**20, **kw)


def _mlp_back(dy, hm, at, gate, up, wo_h, wd_h, *rest, n_gate, n_up):
    wg_h, wu_h, rest = rest[:n_gate], rest[n_gate : n_gate + n_up], rest[n_gate + n_up :]
    dgu, b_out, dhm, dat, delta, wo, wg, wu, wd, sem = rest
    first = pl.program_id(0) == 0
    cp = fetched([(wd_h, wd), *into(wg, wg_h), *into(wu, wu_h), (wo_h, wo)], sem)

    @pl.when(first)
    def _():
        for c in cp:
            c.start()
        cp[0].wait()

    d = dy[...]
    for a, n in CHUNKS:
        da = wide(low(dot(d, wd[a : a + n, :], 1, 1)))
        g, u = gate[:, a : a + n], up[:, a : a + n]
        s = jax.nn.sigmoid(g)
        gs = g * s
        dgu[:, a : a + n] = low(da * u * (s + gs * (1 - s)))
        dgu[:, FF + a : FF + a + n] = low(da * gs)

    @pl.when(first)
    def _():
        for c in cp[1:-1]:
            c.wait()

    db = wide(low(dot(dgu[:, :FF], wg[...], 1, 1))) + wide(low(dot(dgu[:, FF:], wu[...], 1, 1)))
    db = wide(low(db))
    w = wide(hm[...])
    s = norm_scale(w)
    b_out[...] = low(w * s)
    m = low(wide(d) + wide(low(s * (db - w * (s * s) * jnp.mean(db * w, -1, keepdims=True)))))
    dhm[...] = m

    @pl.when(first)
    def _():
        cp[-1].wait()

    x = low(dot(m, wo[...], 1, 1))
    dat[...] = x
    lane = lax.broadcasted_iota(jnp.int32, (d.shape[0], HEAD), 1)
    sums = jnp.zeros((d.shape[0], HEAD), F32)
    for n, t in enumerate(heads_of(wide(x) * wide(at[...]))):
        sums = jnp.where(lane == n, t.sum(-1, keepdims=True), sums)
    delta[...] = sums.T[:HEADS, :]


def mlp_back(dy, hm, at, gate, up, wo, wg, wu, wd, bm=256, **kw):
    n = len(wg) + len(wu)
    return run(functools.partial(_mlp_back, n_gate=len(wg), n_up=len(wu)), "mlp_back", T // bm, [dy, hm, at, gate, up, wo, wd, *wg, *wu],
               [rows(bm, D)] * 3 + [rows(bm, FF)] * 2 + [ANY] * (2 + n),
               [sds((T, 2 * FF)), sds((T, D)), sds((T, D)), sds((T, D)), sds((HEADS, T), F32)],
               [rows(bm, 2 * FF), rows(bm, D), rows(bm, D), rows(bm, D), pl.BlockSpec((HEADS, bm), lambda i: (0, i))],
               [pltpu.VMEM((D, D), BF), pltpu.VMEM((D, FF), BF), pltpu.VMEM((D, FF), BF), pltpu.VMEM((FF, D), BF), pltpu.SemaphoreType.DMA((2 + n,))],
               flops=2 * T * D * (D + 3 * FF), moved=120 * 2**20, exps=T * FF, **kw)


def _down_grad(act, dy, out):
    out[...] = low(dot(act[...], dy[...], 0, 0))


def down_grad(act, dy, steps=5, **kw):
    n = FF // steps
    return run(_down_grad, "down_grad", steps, [act, dy], [pl.BlockSpec((T, n), lambda i: (0, i)), held((T, D))],
               [sds((FF, D))], [pl.BlockSpec((n, D), lambda i: (i, 0))], flops=2 * T * D * FF, moved=24 * 2**20, **kw)


ROWS, N_GU = D // 16, 5
GU = 2 * FF // N_GU


def _pair(t, tiles, sums, owns, tile, out, back, send, recv):
    me = lax.axis_index("dp")
    chip, core = lax.div(me, 2), me % 2
    now, last = lax.rem(t, 2), lax.rem(t + 1, 2)

    def passed():
        return pltpu.make_async_remote_copy(out.at[last], back.at[last], send.at[last], recv.at[last], device_id={"dp": flipped(me, 1)})

    @pl.when(t > 0)
    def _():
        passed().start()

    def keep(make):
        x = make()
        w = x.shape[1]
        tile[now, :, :, :, :w] = x.reshape(8, 2, ROWS, w)
        out[now, :, :, :w] = low(tile[now, :, 1 - core, :, :w])

    def finish(sums, own):
        passed().wait()
        w = own.shape[1]
        sums[...] = low(tile[last, :, core, :, :w] + wide(back[last, :, :, :w]))
        own[...] = tile[last, chip, core, :, :w] + wide(back[last, chip, :, :w])

    for first, after, make in tiles:
        @pl.when((t >= first) & (t < after))
        def _():
            keep(make)

    for (first, after, _), s, own in zip(tiles, sums, owns, strict=True):
        @pl.when((t > first) & (t <= after))
        def _():
            finish(s, own)


def pair_scratch(w):
    return [pltpu.VMEM((2, 8, 2, ROWS, w), F32), pltpu.VMEM((2, 8, ROWS, w), BF), pltpu.VMEM((2, 8, ROWS, w), BF),
            pltpu.SemaphoreType.DMA((2,)), pltpu.SemaphoreType.DMA((2,))]


def _pair_grads(b, dgu, at, dhm, gu, gu_own, o, o_own, *scratch):
    _pair(pl.program_id(0), [(0, N_GU, lambda: dot(b[...], dgu[...], 0, 0)), (N_GU, N_GU + 1, lambda: dot(at[...], dhm[...], 0, 0))],
          (gu, o), (gu_own, o_own), *scratch)


def pair_grads(b, dgu, at, dhm, **kw):
    step = lambda i: jnp.minimum(i, N_GU - 1)
    done = lambda i: jnp.clip(i - 1, 0, N_GU - 1)
    return run(_pair_grads, "pair_grads", N_GU + 2, [b, dgu, at, dhm],
               [held((T, D)), pl.BlockSpec((T, GU), lambda i: (0, step(i))), held((T, D)), held((T, D))],
               [sds((8, ROWS, 2 * FF)), sds((ROWS, 2 * FF), F32), sds((8, ROWS, D)), sds((ROWS, D), F32)],
               [pl.BlockSpec((8, ROWS, GU), lambda i: (0, 0, done(i))), pl.BlockSpec((ROWS, GU), lambda i: (0, done(i))),
                held((8, ROWS, D)), held((ROWS, D))],
               pair_scratch(GU), flops=2 * T * D * (D + 2 * FF), moved=60 * 2**20, partners={1}, **kw)


def _qkv_grads(a, g0, g1, kv0, kv1, dw, own, *scratch):
    t = pl.program_id(0)

    def tile(n):
        if n < 2:
            return lambda: dot(a[...], (g0, g1)[n][...], 0, 0)
        return lambda: dot(a[...], jnp.concatenate([kv0[:, :HEAD], kv1[:, :HEAD], kv0[:, HEAD:], kv1[:, HEAD:]], axis=1), 0, 0)

    _pair(t, [(n, n + 1, tile(n)) for n in range(3)], [dw] * 3, [own] * 3, *scratch)


def qkv_grads(a, g0, g1, kv0, kv1, **kw):
    done = lambda i: jnp.clip(i - 1, 0, 2)
    return run(_qkv_grads, "qkv_grads", 4, [a, g0, g1, kv0, kv1],
               [held((T, D)), held((T, THIRD)), held((T, THIRD)), held((T, KV * HEAD)), held((T, KV * HEAD))],
               [sds((8, ROWS, QKV)), sds((ROWS, QKV), F32)],
               [pl.BlockSpec((8, ROWS, THIRD), lambda i: (0, 0, done(i))), pl.BlockSpec((ROWS, THIRD), lambda i: (0, done(i)))],
               pair_scratch(THIRD), flops=2 * T * D * QKV, moved=14 * 2**20, partners={1}, **kw)


def _attend_back(q, k, v, do, lse, delta, c, s, c_all, s_all, dq, dkv, dq_s, dk_s, dv_s, *, bq, bk, head):
    iq = pl.program_id(0)
    e = SCALE * LOG2E

    @pl.when(iq == 0)
    def _():
        dk_s[...] = jnp.zeros_like(dk_s)
        dv_s[...] = jnp.zeros_like(dv_s)

    dq_s[...] = jnp.zeros_like(dq_s)
    lses = [lse[head * G + n : head * G + n + 1, :] * LOG2E for n in range(G)]
    deltas = [delta[head * G + n : head * G + n + 1, :] for n in range(G)]

    def block(j, ok):
        here = pl.ds(pl.multiple_of(j * bk, bk), bk)
        qs, dos = heads_of(q), heads_of(do)
        kk, vv = k[here, :], v[here, :]
        scores = [dot(kk, qs[n], 1, 1) for n in range(G)]
        dps = [dot(vv, dos[n], 1, 1) for n in range(G)]
        for n in range(G):
            p = jnp.exp2(scores[n] * e - lses[n])
            if ok is not None:
                p = jnp.where(ok, p, 0.0)
            ds = low(p * (dps[n] - deltas[n]))
            dv_s[here, :] += dot(low(p), dos[n], 1, 0)
            dk_s[here, :] += dot(ds, qs[n], 1, 0)
            dq_s[n] += dot(kk.T, ds, 1, 0)

    lax.fori_loop(0, iq, lambda j, _: block(j, None), None)
    gap = lax.broadcasted_iota(jnp.int32, (bk, bq), 1) - lax.broadcasted_iota(jnp.int32, (bk, bq), 0)
    block(iq, gap >= 0)
    for n in range(G):
        dq[:, HEAD * n : HEAD * (n + 1)] = turned(wide(low((dq_s[n] * SCALE).T)), c[...], -s[...])[0]

    @pl.when(iq == pl.num_programs(0) - 1)
    def _():
        dkv[:, :HEAD] = turned(wide(low(dk_s[...] * SCALE)), c_all[...], -s_all[...])[0]
        dkv[:, HEAD:] = low(dv_s[...])


def attend_back(q, k, v, do, lse, delta, cs, head, bq=512, **kw):
    stats = pl.BlockSpec((HEADS, bq), lambda i: (0, i))
    queries = pl.BlockSpec((bq, G * HEAD), lambda i: (i, head))
    keys = pl.BlockSpec((T, HEAD), lambda i: (0, head), pipeline_mode=pl.Buffered(1))
    return run(functools.partial(_attend_back, bq=bq, bk=bq, head=head), f"attend_back{head}", T // bq, [q, k, v, do, lse, delta, *cs, *cs],
               [queries, keys, keys, queries, stats, stats, rows(bq, HEAD), rows(bq, HEAD), held((T, HEAD)), held((T, HEAD))],
               [sds((T, G * HEAD)), sds((T, 2 * HEAD))], [rows(bq, G * HEAD), held((T, 2 * HEAD))],
               [pltpu.VMEM((G, HEAD, bq), F32), pltpu.VMEM((T, HEAD), F32), pltpu.VMEM((T, HEAD), F32)],
               flops=10 * T * T * D // KV, moved=12 * 2**20, exps=G * T * T, **kw)


def _qkv_back(h, g0, g1, kv0, kv1, dhm, w0, w1, w2, dh):
    kv = KV * HEAD
    da = wide(low(dot(g0[...], w0[...], 1, 1) + dot(g1[...], w1[...], 1, 1)))
    dk = jnp.concatenate([kv0[:, :HEAD], kv1[:, :HEAD]], axis=1)
    dv = jnp.concatenate([kv0[:, HEAD:], kv1[:, HEAD:]], axis=1)
    da = wide(low(da + wide(low(dot(dk, w2[:, :kv], 1, 1)))))
    da = wide(low(da + wide(low(dot(dv, w2[:, kv:], 1, 1)))))
    dh[...] = low(wide(dhm[...]) + wide(low(norm_back(h[...], da))))


def qkv_back(h, g0, g1, kv0, kv1, dhm, w, bm=512, **kw):
    kv = KV * HEAD
    (dh,), sent = run(_qkv_back, "qkv_back", T // bm, [h, g0, g1, kv0, kv1, dhm, *w],
                      [rows(bm, D), rows(bm, THIRD), rows(bm, THIRD), rows(bm, kv), rows(bm, kv), rows(bm, D)] + [held((D, THIRD))] * 3,
                      [sds((T, D))], [rows(bm, D)], flops=2 * T * D * QKV, moved=22 * 2**20, **kw)
    return dh, sent


def bare(name, send, ident):
    return run(lambda: None, name, 1, [], [], [], [], send=send, ident=ident)[1]


def solution(mesh):
    def step(x, dy, wq, wk, wv, wo, wg, wu, wd):
        cs = tuple(jnp.asarray(t) for t in tables())
        wkv = jnp.concatenate([wk, wv], axis=2)
        core = lax.axis_index("dp") % 2
        chip = lax.div(lax.axis_index("dp"), 2)
        flat = lambda w: w.reshape(-1, w.shape[3])

        def projections(n):
            return [Gather(wq, n, (0, THIRD)), Gather(wq, n, (THIRD, THIRD)), Gather(wkv, n)]

        w_qkv0 = [flat(w) for w in bare("fetch", projections(0), 0)]
        h0 = x[0]
        (q0, k0, v0, a0), (wo0,) = qkv(h0, w_qkv0, cs, send=[Gather(wo, 0)], ident=1)
        (at0, lse0), (wg0, wu0) = attend(q0, k0, v0, send=[Gather(wg, 0), Gather(wu, 0)], ident=2, marks=(2, 3, 9))
        wo0, wg0, wu0 = flat(wo0), [flat(wg0)], [flat(wu0)]
        (hm0, gate0, up0, act0), (wd0, *w_qkv1, wo1) = mlp_up(h0, at0, wo0, wg0, wu0, send=[Gather(wd, 0), *projections(1), Gather(wo, 1)],
                                                              ident=3, marks=(1, 3, 7))
        wd0, w_qkv1, wo1 = flat(wd0), [flat(w) for w in w_qkv1], flat(wo1)
        cut = 1280
        (h1,), (wg1a,) = mlp_down(hm0, act0, wd0, send=[Gather(wg, 1, (0, cut))], ident=4)
        (q1, k1, v1, a1), _ = qkv(h1, w_qkv1, cs)
        (at1, lse1), (wg1b, wu1) = attend(q1, k1, v1, send=[Gather(wg, 1, (cut, FF - cut)), Gather(wu, 1)], ident=6, marks=(2, 3, 9))
        wg1, wu1 = [flat(wg1a), flat(wg1b)], [flat(wu1)]
        (hm1, gate1, up1, act1), (wd1,) = mlp_up(h1, at1, wo1, wg1, wu1, send=[Gather(wd, 1)], ident=7, marks=(1, 3, 6))
        wd1 = flat(wd1)

        halves = lambda g: g.reshape(8, 2, -1, g.shape[1])
        cube = lambda g: g.reshape(2, 2, 2, *g.shape[1:])
        mine = lambda g: lax.dynamic_index_in_dim(halves(g), core, 1, keepdims=False)
        at_chip = lambda a: lax.dynamic_index_in_dim(a, chip, 0, keepdims=False)

        def halved(sums, got):
            out = []
            for (first, n, (a, _, _)), g in zip(thirds(sums.shape[2]), got, strict=True):
                at = {4: 0, 2: 1, 1: 2}[a]
                side = lax.dynamic_index_in_dim(cube(sums)[..., first : first + n], bit(chip, a), at, keepdims=False)
                out.append(low(wide(side) + wide(g)))
            return out

        def spread(parts):
            return [Spread(p, a) for p, (a, _, _) in zip(parts, AXES, strict=True)]

        def total(own, got, parts):
            out = []
            for (first, n, (a, _, _)), g, p in zip(thirds(own.shape[1]), got, parts, strict=True):
                i, j = (bit(chip, b) for b in (4, 2, 1) if b != a)
                mine = lax.dynamic_slice(g, (i, j, 0, 0), (1, 1, *g.shape[2:]))[0, 0]
                out.append(low(own[:, first : first + n] + wide(mine) + wide(p).sum(0)))
            return jnp.concatenate(out, axis=1)

        def backward(d, ident, last, h, a, q, k, v, at, lse, hm, gate, up, act, w_qkv, wo, wg, wu, wd, before=()):
            (down,), _ = down_grad(act, d)
            (dgu, b, dhm, dat, delta), (got, *got_before) = mlp_back(d, hm, at, gate, up, wo, wg, wu, wd, send=[Swap(halves(down)), *before], ident=ident)
            down_own = wide(at_chip(mine(down))) + wide(at_chip(got))
            (gu, gu_own, o, o_own), (down_in,) = pair_grads(b, dgu, at, dhm, send=[Scatter(low(wide(mine(down)) + wide(got)))], ident=ident + 1)
            (g0, kv0), (gu_half, o_half) = attend_back(q, k, v, dat, lse, delta, cs, 0, send=[Halve(cube(gu)), Halve(cube(o))], ident=ident + 2)
            (g1, kv1), sent = attend_back(q, k, v, dat, lse, delta, cs, 1, send=spread(halved(gu, gu_half)) + spread(halved(o, o_half)), ident=ident + 3)
            (dw, dw_own), _ = qkv_grads(a, g0, g1, kv0, kv1, ident=ident + 4)
            dh, dw_in = qkv_back(h, g0, g1, kv0, kv1, dhm, w_qkv, **(dict(send=[Scatter(dw)], ident=ident + 5) if last else {}))
            done = total(o_own, o_half, sent[3:]), total(gu_own, gu_half, sent[:3]), low(down_own + wide(down_in).sum(0))
            return dh, (dw, dw_own, dw_in), done, got_before

        d0, (dw1, dw1_own, _), done1, _ = backward(dy[0], 8, False, h1, a1, q1, k1, v1, at1, lse1, hm1, gate1, up1, act1, w_qkv1, wo1, wg1, wu1, wd1)
        dx, (_, dw0_own, dw0_in), done0, dw1_in = backward(d0, 14, True, h0, a0, q0, k0, v0, at0, lse0, hm0, gate0, up0, act0, w_qkv0, wo0, wg0, wu0,
                                                           wd0, [Scatter(dw1)])

        def weights(dw_own, dw_in, done):
            dw = low(dw_own + wide(dw_in).sum(0))
            o, gu, down = done
            kv = KV * HEAD
            return dw[:, :D], dw[:, D : D + kv], dw[:, D + kv :], o, gu[:, :FF], gu[:, FF:], down

        first, second = weights(dw0_own, dw0_in[0], done0), weights(dw1_own, dw1_in[0], done1)
        return (dx[None], *(jnp.stack(g) for g in zip(first, second, strict=True)))

    states, cut = P(("rep", "dp"), None, None), P(None, "dp", None)
    return jax.shard_map(
        step,
        mesh=mesh,
        in_specs=(states, states) + (cut,) * 7,
        out_specs=(states,) + (P("rep", "dp", None),) * 7,
        check_vma=False,
    )
```

```python
import functools

import jax
import jax.numpy as jnp
import numpy as np
from jax import lax
from jax.experimental import pallas as pl
from jax.experimental.pallas import tpu as pltpu
from jax.sharding import PartitionSpec as P

T, D, HEADS, KV, HEAD, FF, THETA = 2048, 1024, 8, 2, 128, 3200, 10000
G = HEADS // KV
QKV = D + 2 * KV * HEAD
THIRD = QKV // 3
BF, F32 = jnp.bfloat16, jnp.float32
LOG2E = 1.4426950408889634
SCALE = HEAD**-0.5
NEG, HIDDEN = -1e30, -2e30
ANY = pl.BlockSpec(memory_space=pl.ANY)


def step():
    return pl.program_id(0)


def steps():
    return pl.num_programs(0)


def params(**kw):
    return pltpu.CompilerParams(vmem_limit_bytes=62 * 2**20, **kw)


def sds(shape, dtype=BF):
    return jax.ShapeDtypeStruct(shape, dtype)


def rows(bm, n):
    return pl.BlockSpec((bm, n), lambda i: (i, 0))


def held(shape):
    return pl.BlockSpec(shape, lambda i: (0,) * len(shape), pipeline_mode=pl.Buffered(1))


def dot(a, b, ca=1, cb=0):
    return lax.dot_general(a, b, (((ca,), (cb,)), ((), ())), preferred_element_type=F32)


def dot_nt(a, b):
    return dot(a, b, 1, 1)


def dot_tn(a, b):
    return dot(a, b, 0, 0)


def low(x):
    return x.astype(BF)


def wide(x):
    return x.astype(F32)


def norm_scale(w):
    return lax.rsqrt(jnp.mean(w * w, -1, keepdims=True) + 1e-6)


def normed(h):
    w = wide(h)
    return low(w * norm_scale(w))


def norm_back(h, c):
    w = wide(h)
    s = norm_scale(w)
    return s * (c - w * (s * s) * jnp.mean(c * w, -1, keepdims=True))


def tables():
    half = HEAD // 2
    angle = np.arange(T, dtype=np.float32)[:, None] * (np.float32(THETA) ** (-np.arange(half, dtype=np.float32) / np.float32(half)))
    cos, sin = np.cos(angle).astype(np.float32), np.sin(angle).astype(np.float32)
    return np.concatenate([cos, cos], 1), np.concatenate([-sin, sin], 1)


def flat(w):
    return w.reshape(-1, w.shape[-1])


def heads_of(x):
    return [x[:, HEAD * n : HEAD * (n + 1)] for n in range(x.shape[1] // HEAD)]


def turned(x, c, s):
    return [low(t * c + pltpu.roll(t, HEAD // 2, 1) * s) for t in heads_of(x)]


X, Y, Z = 4, 2, 1
NEAR = {1, 2 * X, 2 * Y, 2 * Z}
FAR = {2 * n for n in range(1, 8)}


def place():
    me = lax.axis_index("dp")
    return me, lax.div(me, 2), me % 2


def flipped(number, bits):
    for bit in sorted(NEAR):
        if bits & bit:
            number = number + bit - 2 * bit * (lax.div(number, bit) % 2)
    return number


AXES = ((X, Y, Z), (Y, Z, X), (Z, X, Y))
OTHERS = ((0, 1), (1, 1), (1, 0))


def thirds(n):
    units = n // 128
    sizes = [128 * (units // 3 + (r < units % 3)) for r in range(3)]
    return [(sum(sizes[:r]), sizes[r], axes) for r, axes in enumerate(AXES)]


class Gather:
    copies = 48
    partners = NEAR

    def __init__(self, src, layer, part=None):
        self.src, self.layer, self.part = src, layer, part
        rows, n = src.shape[1:]
        self.shape = (8, 2, rows, n if part is None else part[1])

    def bind(self, src, dst, send, recv):
        me, chip, core = place()
        at = 0 if self.part is None else self.part[0]
        self.ended = False
        self.links, self.pairs = [], []
        for r, (first, n, (a, b, c)) in enumerate(thirds(dst.shape[3])):
            block = lambda bits: dst.at[flipped(chip, bits), core, :, pl.ds(first, n)]
            count = [16 * r - 1]

            def to(bits, where):
                count[0] += 1
                k = count[0]
                what = block(where) if where else src.at[self.layer, :, pl.ds(at + first, n)]
                return pltpu.make_async_remote_copy(what, block(where), send.at[k], recv.at[k], device_id={"dp": flipped(me, bits)})

            ab, abc = a | b, a | b | c
            self.links.append([[to(2 * m, 0) for m in (a, b, c)], [to(2 * b, a), to(2 * c, a), to(2 * c, b)], [to(2 * c, ab)]])
            self.pairs.append([[to(1, 0)], [to(1, m) for m in (a, b, c)], [to(1, m) for m in (ab, a | c, b | c)], [to(1, abc)]])
        self.local = pltpu.make_async_copy(src.at[self.layer, :, pl.ds(at, dst.shape[3])], dst.at[chip, core], send.at[15])

    def stage(self, n):
        if n == 0:
            self.local.start()
        if n < 3:
            for k in range(len(self.links[0][n])):
                for links, pairs in zip(self.links, self.pairs):
                    if n:
                        self.arrived(links, pairs, n, k)
                    links[n][k].start()
                    if n == 0 and k == 0:
                        pairs[0][0].start()
            if n == 2:
                for k in (1, 2):
                    for links, pairs in zip(self.links, self.pairs):
                        self.arrived(links, pairs, n, k)
        else:
            for links, pairs in zip(self.links, self.pairs):
                self.arrived(links, pairs, n, 0)

    def arrived(self, links, pairs, n, k):
        links[n - 1][k].wait_recv()
        pairs[n][k].start()

    def end(self):
        if self.ended:
            return
        self.ended = True
        for links, pairs in zip(self.links, self.pairs):
            for c in sum(pairs, []):
                c.wait_recv()
            for c in sum(links + pairs, []):
                c.wait_send()
        self.local.wait()


class Once:
    def stage(self, n):
        if n == 0:
            for c in self.all:
                c.start()

    def end(self):
        for c in self.all:
            c.wait()


class Scatter(Once):
    copies = 7
    partners = FAR

    def __init__(self, src):
        self.src = src
        self.shape = (7, *src.shape[1:])

    def bind(self, src, dst, send, recv):
        me, chip, _ = place()
        self.all = [
            pltpu.make_async_remote_copy(src.at[flipped(chip, m)], dst.at[m - 1], send.at[m - 1], recv.at[m - 1], device_id={"dp": flipped(me, 2 * m)})
            for m in (Z, Y | Z, Y, X | Y, X, X | Z, X | Y | Z)
        ]


def side(axis, index):
    return {X: (index,), Y: (slice(None), index), Z: (slice(None), slice(None), index)}[axis]


CUBE = (2, 2, 2)


def bit(chip, axis):
    return lax.div(chip, axis) % 2


def spreads(src, dst, axis, send, recv):
    me, chip, _ = place()
    out = []
    for k, far in enumerate(OTHERS):
        bits = [b for b in AXES[0] if b != axis]
        i, j = (1 - bit(chip, b) if f else bit(chip, b) for b, f in zip(bits, far))
        where = 2 * sum(b * f for b, f in zip(bits, far))
        out.append(pltpu.make_async_remote_copy(src.at[i, j], dst.at[k], send.at[k], recv.at[k], device_id={"dp": flipped(me, where)}))
    return out


class Spread(Once):
    copies = 3

    def __init__(self, src, axis):
        self.src, self.axis = src, axis
        self.planes = tuple(b for b in AXES[0] if b != axis)
        p, q = self.planes
        self.partners = {2 * p, 2 * q, 2 * (p + q)}
        self.shape = (3, *src.shape[2:])

    def bind(self, src, dst, send, recv):
        self.all = spreads(src, dst, self.axis, send, recv)


def meet(partners):
    me = lax.axis_index("dp")
    barrier = pltpu.get_barrier_semaphore()
    for bits in sorted(partners):
        pl.semaphore_signal(barrier, inc=1, device_id={"dp": flipped(me, bits)})
    pl.semaphore_wait(barrier, len(partners))


def staged(send, marks, count):
    marks = (0, *marks) if any(isinstance(t, Gather) for t in send) else (0,)

    def stage(n):
        for t in send:
            t.stage(n)

    def end():
        for n, mark in enumerate(marks):
            if mark == count:
                stage(n)
        for t in send:
            t.end()

    return {mark: functools.partial(stage, n) for n, mark in enumerate(marks) if mark != count}, end


def run(body, name, count, ins, in_specs, outs, out_specs, scratch=(), send=(), ident=None, marks=(1, 2, 3), partners=(), plan=staged, shown=0):
    n_in, n_out, n_send, n_scratch = len(ins), len(outs), len(send), len(scratch)
    partners = set(partners).union(*(t.partners for t in send))

    def kernel(*refs):
        def take(n):
            nonlocal refs
            got, refs = refs[:n], refs[n:]
            return got

        a, c_src, o, c_dst = take(n_in), take(n_send), take(n_out), take(n_send)
        s, sems = take(n_scratch), refs
        i = step()
        for n, t in enumerate(send):
            t.bind(c_src[n], c_dst[n], sems[2 * n], sems[2 * n + 1])
        starts, end = plan(send, marks, count)
        inner = {mark: act for mark, act in starts.items() if isinstance(mark, tuple)}
        if partners:
            for mark, act in starts.items():
                if mark not in inner:
                    @pl.when(i == mark)
                    def _():
                        if mark == 0:
                            meet(partners)
                        act()

        def tick(j):
            for (first, then), act in inner.items():
                pl.when((i == first) & (j == then))(act)

        body(*a, *c_dst[:shown], *o, *s, **({"tick": tick} if inner else {}))
        if send:
            pl.when(i == count - 1)(end)

    got = list(pl.pallas_call(
        kernel, grid=(count,), in_specs=[*in_specs, *[ANY] * n_send], out_specs=[*out_specs, *[ANY] * n_send],
        out_shape=[*outs, *(sds(t.shape) for t in send)],
        scratch_shapes=[*scratch, *(pltpu.SemaphoreType.DMA((t.copies,)) for t in send for _ in range(2))],
        compiler_params=params(**(dict(collective_id=ident, has_side_effects=True) if partners else {})), name=name,
    )(*ins, *(t.src for t in send)))
    return got[:n_out], got[n_out:]


def steps_of(t, first, after):
    return pl.when((t >= first) & (t < after))


def fetched(pairs, sem):
    return [pltpu.make_async_copy(a, b, sem.at[n]) for n, (a, b) in enumerate(pairs)]


def _qkv(h, c, s, w0, w1, w2, q, k, v, a_out):
    a = normed(h[:])
    a_out[:] = a
    cc, ss = c[:], s[:]
    for part, w in enumerate((w0, w1)):
        for n, t in enumerate(turned(wide(low(dot(a, flat(w[:])))), cc, ss)):
            at = HEAD * (n + part * G)
            q[:, at : at + HEAD] = t
    kv = low(dot(a, flat(w2[:])))
    for n, t in enumerate(turned(wide(kv[:, : KV * HEAD]), cc, ss)):
        k[:, HEAD * n : HEAD * (n + 1)] = t
    v[:] = kv[:, KV * HEAD :]


def later(bk, bq):
    return lax.broadcasted_iota(jnp.int32, (bk, bq), 1) - lax.broadcasted_iota(jnp.int32, (bk, bq), 0)


def _attend(q, k, v, o, lse, top_s, mix_s, *, bq, bk, iq=None, tick=lambda j: None):
    iq = step() if iq is None else iq
    e = SCALE * LOG2E
    top_s[:] = jnp.full(top_s.shape, NEG, F32)
    mix_s[:] = jnp.zeros(mix_s.shape, F32)
    ones = jnp.ones((8, bk), BF)
    per = bq // bk

    def block(j, ok):
        tick(j)
        here = pl.ds(pl.multiple_of(j * bk, bk), bk)
        scores = [dot_nt(k[here, HEAD * (n // G) : HEAD * (n // G + 1)], q[:, HEAD * n : HEAD * (n + 1)]) for n in range(HEADS)]
        weights, keeps = [], []
        for n, s in enumerate(scores):
            if ok is not None:
                s = jnp.where(ok, s, HIDDEN)
            old = top_s[n : n + 1, :]
            top = jnp.maximum(old, s.max(axis=0, keepdims=True))
            top_s[n : n + 1, :] = top
            weights.append(low(jnp.exp2((s - top) * e)))
            keeps.append(jnp.exp2((old - top) * e))
        for n in range(HEADS):
            i = n // G
            values = jnp.concatenate([v[here, HEAD * i : HEAD * (i + 1)].T, ones], axis=0)
            mix_s[n] = mix_s[n] * keeps[n] + dot(values, weights[n])

    lax.fori_loop(0, iq * per, lambda j, _: block(j, None), None)
    gap = later(bk, bq)
    for r in range(per):
        block(iq * per + r, gap >= r * bk)
    for n in range(HEADS):
        total = mix_s[n, HEAD : HEAD + 1, :]
        o[:, HEAD * n : HEAD * (n + 1)] = low((mix_s[n, :HEAD, :] * (1 / total)).T)
        lse[n : n + 1, :] = top_s[n : n + 1, :] * SCALE + jnp.log(total)


def attend(q, k, v, bq=512, bk=512, **kw):
    return run(functools.partial(_attend, bq=bq, bk=bk), "attend", T // bq, [q, k, v],
               [rows(bq, D), held((T, KV * HEAD)), held((T, KV * HEAD))],
               [sds((T, D)), sds((HEADS, T), F32)], [rows(bq, D), pl.BlockSpec((HEADS, bq), lambda i: (0, i))],
               [pltpu.VMEM((HEADS, bq), F32), pltpu.VMEM((HEADS, HEAD + 8, bq), F32)], **kw)


TILES = 4


def _first(x, c, s, h0, h1, h2, q_out, k_out, v_out, a_out, o, lse, q, k, v, w0, w1, w2, sem, top_s, mix_s, *, bm, tick):
    i = step()

    @pl.when(i == 0)
    def _():
        cp = fetched(list(zip((h0, h1, h2), (w0, w1, w2))), sem)
        for d in cp:
            d.start()
        for d in cp:
            d.wait()

    @steps_of(i, 1, TILES + 1)
    def _():
        _qkv(x, c, s, w0, w1, w2, q_out, k_out, v_out, a_out)
        here = pl.ds(pl.multiple_of((i - 1) * bm, bm), bm)
        q[here, :] = q_out[:]
        k[here, :] = k_out[:]
        v[here, :] = v_out[:]

    @pl.when(i > TILES)
    def _():
        iq = i - TILES - 1
        _attend(q.at[pl.ds(pl.multiple_of(iq * bm, bm), bm)], k, v, o, lse, top_s, mix_s, bq=bm, bk=bm, iq=iq, tick=tick)


def first(x, cs, own, rest):
    bm, kv = T // TILES, KV * HEAD
    early = lambda i: (jnp.clip(i - 1, 0, TILES - 1), 0)
    late = lambda i: jnp.maximum(i - TILES - 1, 0)

    def plan(send, marks, count):
        def start():
            for stage in range(4):
                for t in own:
                    t.stage(stage)
                for t in {1: rest[:1], 2: rest[1:]}.get(stage, ()):
                    t.stage(0)
            for t in own:
                t.end()

        starts, end = staged(rest, marks, count)
        return {**starts, 0: start}, end

    return run(functools.partial(_first, bm=bm), "first", 2 * TILES + 1, [x, *cs], [pl.BlockSpec((bm, D), early)] + [pl.BlockSpec((bm, HEAD), early)] * 2,
               [sds((T, D)), sds((T, kv)), sds((T, kv)), sds((T, D)), sds((T, D)), sds((HEADS, T), F32)],
               [pl.BlockSpec((bm, w), early) for w in (D, kv, kv, D)] + [pl.BlockSpec((bm, D), lambda i: (late(i), 0)), pl.BlockSpec((HEADS, bm), lambda i: (0, late(i)))],
               [pltpu.VMEM((T, D), BF), pltpu.VMEM((T, kv), BF), pltpu.VMEM((T, kv), BF)] + [pltpu.VMEM((8, 2, D // 16, THIRD), BF)] * 3
               + [pltpu.SemaphoreType.DMA((3,)), pltpu.VMEM((HEADS, bm), F32), pltpu.VMEM((HEADS, HEAD + 8, bm), F32)],
               send=[*own, *rest], ident=0, marks=(TILES + 2, (2 * TILES, 2), 2 * TILES + 1), plan=plan, shown=len(own))


CHUNK = 768
CHUNKS = [(a, CHUNK if a + 2 * CHUNK <= FF else FF - a) for a in range(0, FF - CHUNK, CHUNK)]


def into(w, pieces):
    at, out = 0, []
    for p in pieces:
        out.append((p, w.at[:, pl.ds(at, p.shape[1])]))
        at += p.shape[1]
    return out


def lagged(bm, n):
    return pl.BlockSpec((bm, n), lambda i: (jnp.maximum(i - 1, 0), 0))


def ahead(bm, n):
    return pl.BlockSpec((bm, n), lambda i: (jnp.minimum(i, T // bm - 1), 0))


def _mlp_up(h, at, wo_h, *rest, n_gate, n_up):
    wg_h, wu_h, (hm, gate, up, act, wo, wg, wu, sem) = rest[:n_gate], rest[n_gate : n_gate + n_up], rest[n_gate + n_up :]
    first = step() == 0
    cp = fetched([(wo_h, wo), *into(wg, wg_h), *into(wu, wu_h)], sem)

    @pl.when(first)
    def _():
        for c in cp:
            c.start()
        cp[0].wait()

    m = low(wide(h[:]) + wide(low(dot(at[:], wo[:]))))
    hm[:] = m
    b = normed(m)

    @pl.when(first)
    def _():
        for c in cp[1:]:
            c.wait()

    for a, n in CHUNKS:
        g, u = dot(b, wg[:, a : a + n]), dot(b, wu[:, a : a + n])
        gate[:, a : a + n] = g
        up[:, a : a + n] = u
        act[:, a : a + n] = low(jax.nn.silu(g) * u)


def mlp_up(h, at, wo, wg, wu, bm=256, **kw):
    return run(functools.partial(_mlp_up, n_gate=len(wg), n_up=len(wu)), "mlp_up", T // bm, [h, at, wo, *wg, *wu],
               [rows(bm, D), rows(bm, D)] + [ANY] * (1 + len(wg) + len(wu)),
               [sds((T, D)), sds((T, FF), F32), sds((T, FF), F32), sds((T, FF))], [rows(bm, D), rows(bm, FF), rows(bm, FF), rows(bm, FF)],
               [pltpu.VMEM((D, D), BF), pltpu.VMEM((D, FF), BF), pltpu.VMEM((D, FF), BF), pltpu.SemaphoreType.DMA((1 + len(wg) + len(wu),))], **kw)


def _down_qkv(m, act, wd, c, s, w0, w1, w2, y, q, k, v, a):
    y[:] = low(wide(m[:]) + wide(low(dot(act[:], wd[:]))))
    _qkv(y, c, s, w0, w1, w2, q, k, v, a)


def down_qkv(m, act, wd, cs, w, bm=256, **kw):
    kv = KV * HEAD
    return run(_down_qkv, "down_qkv", T // bm, [m, act, wd, *cs, *w],
               [rows(bm, D), rows(bm, FF), held((FF, D)), rows(bm, HEAD), rows(bm, HEAD)] + [held((D, THIRD))] * 3,
               [sds((T, D)), sds((T, D)), sds((T, kv)), sds((T, kv)), sds((T, D))], [rows(bm, w) for w in (D, D, kv, kv, D)], **kw)


def _mlp_back(dy, hm, at, gate, up, wo_h, wd_h, *rest, n_gate, n_up):
    wg_h, wu_h, rest = rest[:n_gate], rest[n_gate : n_gate + n_up], rest[n_gate + n_up :]
    dgu, b_out, dhm, dat, delta, wo, wg, wu, wd, sem, d_s, db_s = rest
    t, count = step(), steps() - 1
    now, last = t % 2, (t + 1) % 2
    cp = fetched([(wd_h, wd), *into(wg, wg_h), *into(wu, wu_h), (wo_h, wo)], sem)

    def grads(before=lambda: None):
        d = dy[:]
        d_s[now] = d
        for a, n in CHUNKS:
            da = wide(low(dot_nt(d, wd[a : a + n, :])))
            g, u = gate[:, a : a + n], up[:, a : a + n]
            s = jax.nn.sigmoid(g)
            gs = g * s
            dgu[:, a : a + n] = low(da * u * (s + gs * (1 - s)))
            dgu[:, FF + a : FF + a + n] = low(da * gs)
        before()
        db_s[now] = low(wide(low(dot_nt(dgu[:, :FF], wg[:]))) + wide(low(dot_nt(dgu[:, FF:], wu[:]))))

    def leave():
        db, w = wide(db_s[last]), wide(hm[:])
        s = norm_scale(w)
        b_out[:] = low(w * s)
        m = low(wide(d_s[last]) + wide(low(s * (db - w * (s * s) * jnp.mean(db * w, -1, keepdims=True)))))
        dhm[:] = m
        x = low(dot_nt(m, wo[:]))
        dat[:] = x
        lane = lax.broadcasted_iota(jnp.int32, (m.shape[0], HEAD), 1)
        sums = jnp.zeros((m.shape[0], HEAD), F32)
        for n, r in enumerate(heads_of(wide(x) * wide(at[:]))):
            sums = jnp.where(lane == n, r.sum(-1, keepdims=True), sums)
        delta[:] = sums.T[:HEADS, :]

    @pl.when(t == 0)
    def _():
        for c in cp:
            c.start()
        cp[0].wait()
        grads(lambda: [c.wait() for c in cp[1:]])

    @steps_of(t, 1, count)
    def _():
        leave()
        grads()

    pl.when(t == count)(leave)


def mlp_back(dy, hm, at, gate, up, wo, wg, wu, wd, bm=256, **kw):
    n = len(wg) + len(wu)
    return run(functools.partial(_mlp_back, n_gate=len(wg), n_up=len(wu)), "mlp_back", T // bm + 1, [dy, hm, at, gate, up, wo, wd, *wg, *wu],
               [ahead(bm, D), lagged(bm, D), lagged(bm, D), ahead(bm, FF), ahead(bm, FF)] + [ANY] * (2 + n),
               [sds((T, 2 * FF)), sds((T, D)), sds((T, D)), sds((T, D)), sds((HEADS, T), F32)],
               [ahead(bm, 2 * FF), lagged(bm, D), lagged(bm, D), lagged(bm, D), pl.BlockSpec((HEADS, bm), lambda i: (0, jnp.maximum(i - 1, 0)))],
               [pltpu.VMEM((D, D), BF), pltpu.VMEM((D, FF), BF), pltpu.VMEM((D, FF), BF), pltpu.VMEM((FF, D), BF), pltpu.SemaphoreType.DMA((2 + n,)),
                pltpu.VMEM((2, bm, D), BF), pltpu.VMEM((2, bm, D), BF)], **kw)


def passed(out, back, send, recv, slot, bits):
    return pltpu.make_async_remote_copy(out.at[slot], back.at[slot], send.at[slot], recv.at[slot], device_id={"dp": flipped(lax.axis_index("dp"), bits)})


def keep(x, tile, out, slot, core):
    w = x.shape[1]
    tile[slot, :, :, :, :, :, :w] = x.reshape(*tile.shape[1:6], w)
    out[slot, :, :, :, :, :w] = low(tile[slot, :, :, :, 1 - core, :, :w])


def _pair(act, dy, sums, own, tile, out, back, send, recv):
    t = step()
    me, chip, core = place()
    now, last = t % 2, (t + 1) % 2
    count = steps() - 1

    @pl.when(t > 0)
    def _():
        passed(out, back, send, recv, last, 1).start()

    @pl.when(t < count)
    def _():
        keep(dot_tn(act[:], dy[:]), tile, out, now, core)

    @pl.when(t > 0)
    def _():
        passed(out, back, send, recv, last, 1).wait()
        sums[:] = low(tile[last, :, :, :, core] + wide(back[last])).reshape(sums.shape)
        here = (last, *(bit(chip, b) for b in AXES[0]))
        own[:] = tile[(*here, core)] + wide(back[here])


def pair_scratch(r, w):
    return [pltpu.VMEM((2, *CUBE, 2, r, w), F32), pltpu.VMEM((2, *CUBE, r, w), BF), pltpu.VMEM((2, *CUBE, r, w), BF),
            pltpu.SemaphoreType.DMA((2,)), pltpu.SemaphoreType.DMA((2,))]


def down_grad(act, dy, w=256, **kw):
    r, n = FF // 16, D // w
    done = lambda i: jnp.maximum(i - 1, 0)
    return run(_pair, "down_grad", n + 1, [act, dy], [held((T, FF)), pl.BlockSpec((T, w), lambda i: (0, jnp.minimum(i, n - 1)))],
               [sds((8, r, D)), sds((r, D), F32)], [pl.BlockSpec((8, r, w), lambda i: (0, 0, done(i))), pl.BlockSpec((r, w), lambda i: (0, done(i)))],
               pair_scratch(r, w), partners={1}, **kw)


ROWS = D // 16


def _quad(tiles, outs, tile, out, back, send, recv, half, *rest):
    half_out, half_back, half_send, half_recv = rest[:3], rest[3:6], rest[6:9], rest[9:12]
    t = step()
    me, chip, core = place()
    now, last = t % 2, (t + 1) % 2
    count = tiles[-1][1]

    def turn(r, n):
        return pltpu.make_async_remote_copy(half_out[r].at[n % 2], half_back[r].at[n % 4], half_send[r].at[n % 2], half_recv[r].at[n % 4],
                                            device_id={"dp": flipped(me, 2 * AXES[r][0])})

    @pl.when((t > 0) & (t <= count))
    def _():
        passed(out, back, send, recv, last, 1).start()

    @pl.when((t > 1) & (t <= count + 1))
    def _():
        for r in range(3):
            turn(r, t - 2).start()

    for first, after, make in tiles:
        @steps_of(t, first, after)
        def _():
            keep(make(), tile, out, now, core)

    for (first, after, _), thirds_out in zip(tiles, outs):
        w = sum(o.shape[1] for _, o in thirds_out)

        @steps_of(t, first + 3, after + 3)
        def _():
            for r, ((at, n, (a, _, _)), (sums, own)) in enumerate(zip(thirds(w), thirds_out)):
                turn(r, t - 3).wait()
                here = pl.ds(at, n)
                came = half_back[r].at[(t - 3) % 4]
                sums[:] = low(half[last, :, :, :, here] + wide(came[:, :, :, :n]))
                i, j = (bit(chip, x) for x in AXES[0] if x != a)
                own[:] = half[last, i, j, :, here] + wide(came[i, j, :, :n])

        @steps_of(t, first + 1, after + 1)
        def _():
            passed(out, back, send, recv, last, 1).wait()
            for r, (at, n, (a, _, _)) in enumerate(thirds(w)):
                here = pl.ds(at, n)

                def pair(index):
                    index = side(a, index)
                    index = (last, *index, *[slice(None)] * (3 - len(index)))
                    return tile[(*index, core, slice(None), here)] + wide(back[(*index, slice(None), here)])

                half[last, :, :, :, here] = pair(bit(chip, a))
                half_out[r][last, :, :, :, :n] = low(pair(1 - bit(chip, a)))


def quad_scratch(widths):
    parts = [max(thirds(w)[r][1] for w in widths) for r in range(3)]
    sems = lambda n: [pltpu.SemaphoreType.DMA((n,))] * 3
    return [*pair_scratch(ROWS, max(widths)), pltpu.VMEM((*CUBE, ROWS, max(widths)), F32), *(pltpu.VMEM((*CUBE, ROWS, n), BF) for n in parts),
            *(pltpu.VMEM((4, 2, 2, ROWS, n), BF) for n in parts), *sems(2), *sems(4)]


def quad_outs(sizes):
    outs, specs = [], []
    for count, w, first in sizes:
        at = lambda i, first=first, count=count: jnp.clip(i - first - 3, 0, count - 1)
        for _, n, _ in thirds(w):
            outs += [sds((2, 2, ROWS, count * n)), sds((ROWS, count * n), F32)]
            specs += [pl.BlockSpec((2, 2, ROWS, n), lambda i, at=at: (0, 0, 0, at(i))), pl.BlockSpec((ROWS, n), lambda i, at=at: (0, at(i)))]
    return outs, specs


def grouped(refs):
    pairs = list(zip(refs[::2], refs[1::2]))
    return [pairs[n : n + 3] for n in range(0, len(pairs), 3)]


N_GU = 5
GU = 2 * FF // N_GU


def _mlp_grads(b, dgu, at_h, dhm_h, *rest):
    rest, (at, dhm, sem) = rest[:-3], rest[-3:]
    t = step()
    cp = fetched([(at_h, at), (dhm_h, dhm)], sem)

    @pl.when(t == 1)
    def _():
        for c in cp:
            c.start()

    @pl.when(t == N_GU)
    def _():
        for c in cp:
            c.wait()

    _quad([(0, N_GU, lambda: dot_tn(b[:], dgu[:])), (N_GU, N_GU + 1, lambda: dot_tn(at[:], dhm[:]))], grouped(rest[:12]), *rest[12:])


def mlp_grads(b, dgu, at, dhm, **kw):
    tile = lambda i: jnp.minimum(i, N_GU - 1)
    outs, specs = quad_outs([(N_GU, GU, 0), (1, D, N_GU)])
    got, _ = run(_mlp_grads, "mlp_grads", N_GU + 4, [b, dgu, at, dhm], [held((T, D)), pl.BlockSpec((T, GU), lambda i: (0, tile(i))), ANY, ANY],
                 outs, specs, [*quad_scratch((GU, D)), pltpu.VMEM((T, D), BF), pltpu.VMEM((T, D), BF), pltpu.SemaphoreType.DMA((2,))],
                 partners=NEAR, **kw)
    return grouped(got)


def _attend_back(q, k, v, do, lse, delta, c, s, c_all, s_all, dq, dkv, dq_s, dk_s, dv_s, *, bq, bk):
    iq = step()
    e = SCALE * LOG2E

    @pl.when(iq == 0)
    def _():
        dk_s[:] = jnp.zeros_like(dk_s)
        dv_s[:] = jnp.zeros_like(dv_s)

    dq_s[:] = jnp.zeros_like(dq_s)
    lses = [lse[n : n + 1, :] * LOG2E for n in range(HEADS)]
    deltas = [delta[n : n + 1, :] for n in range(HEADS)]

    def block(j, ok):
        here = pl.ds(pl.multiple_of(j * bk, bk), bk)
        qs, dos = heads_of(q), heads_of(do)
        ks, vs = ([x[here, HEAD * i : HEAD * (i + 1)] for i in range(KV)] for x in (k, v))
        scores = [dot_nt(ks[n // G], qs[n]) for n in range(HEADS)]
        dps = [dot_nt(vs[n // G], dos[n]) for n in range(HEADS)]
        for n in range(HEADS):
            i = n // G
            p = jnp.exp2(scores[n] * e - lses[n])
            if ok is not None:
                p = jnp.where(ok, p, 0.0)
            ds = low(p * (dps[n] - deltas[n]))
            dv_s[i, here, :] += dot(low(p), dos[n])
            dk_s[i, here, :] += dot(ds, qs[n])
            dq_s[n] += dot(ks[i].T, ds)

    lax.fori_loop(0, iq, lambda j, _: block(j, None), None)
    gap = later(bk, bq)
    block(iq, gap >= 0)
    for n in range(HEADS):
        dq[:, HEAD * n : HEAD * (n + 1)] = turned(wide(low((dq_s[n] * SCALE).T)), c[:], -s[:])[0]

    @pl.when(iq == steps() - 1)
    def _():
        for i in range(KV):
            dkv[:, HEAD * i : HEAD * (i + 1)] = turned(wide(low(dk_s[i] * SCALE)), c_all[:], -s_all[:])[0]
            dkv[:, HEAD * (KV + i) : HEAD * (KV + i + 1)] = low(dv_s[i])


def attend_back(q, k, v, do, lse, delta, cs, bq=512, **kw):
    stats = pl.BlockSpec((HEADS, bq), lambda i: (0, i))
    keys = held((T, KV * HEAD))
    return run(functools.partial(_attend_back, bq=bq, bk=bq), "attend_back", T // bq, [q, k, v, do, lse, delta, *cs, *cs],
               [rows(bq, D), keys, keys, rows(bq, D), stats, stats, rows(bq, HEAD), rows(bq, HEAD), held((T, HEAD)), held((T, HEAD))],
               [sds((T, D)), sds((T, THIRD))], [rows(bq, D), held((T, THIRD))],
               [pltpu.VMEM((HEADS, HEAD, bq), F32), pltpu.VMEM((KV, T, HEAD), F32), pltpu.VMEM((KV, T, HEAD), F32)], **kw)


N_QKV = 3


def _qkv_back(h, a, dq, dkv, dhm, w0, w1, w2, dh, *rest, bm, final):
    t = step()
    moves = []
    if final:
        owns, came, rest, (*sums, send, recv) = rest[:6], rest[6:12], rest[12:-5], rest[-5:]
        outs = [[(sums[r].at[t - 3], owns[g + r]) for r in range(3)] for g in (0, 3)]
        for n in range(N_QKV):
            g, at = (0, n) if n < 2 else (3, 0)
            moves.append([c for r, (_, w, axes) in enumerate(thirds(THIRD))
                          for c in spreads(sums[r].at[n], came[g + r].at[:, :, pl.ds(at * w, w)], axes[0], send.at[n, r], recv.at[n, r])])
    else:
        outs, rest = grouped(rest[:12]), rest[12:]
    _quad([(0, 2, lambda: dot_tn(a[:], dq[:, pl.ds(pl.multiple_of(t * THIRD, THIRD), THIRD)])), (2, N_QKV, lambda: dot_tn(a[:], dkv[:]))], outs, *rest)
    for n, copies in enumerate(moves):
        @pl.when(t == n + 4)
        def _():
            for c in copies:
                c.start()

    @pl.when(t >= N_QKV)
    def _():
        kv = KV * HEAD
        here = pl.ds(pl.multiple_of((t - N_QKV) * bm, bm), bm)
        da = wide(low(dot_nt(dq[here, :THIRD], w0[:]) + dot_nt(dq[here, THIRD:], w1[:])))
        da = wide(low(da + wide(low(dot_nt(dkv[here, :kv], w2[:, :kv])))))
        da = wide(low(da + wide(low(dot_nt(dkv[here, kv:], w2[:, kv:])))))
        dh[:] = low(wide(dhm[:]) + wide(low(norm_back(h[:], da))))

    if final:
        @pl.when(t == steps() - 1)
        def _():
            for c in sum(moves, []):
                c.wait()


def qkv_back(h, a, dq, dkv, dhm, w, bm=512, final=False, **kw):
    at = lambda i: (jnp.maximum(i - N_QKV, 0), 0)
    outs, specs = quad_outs([(2, THIRD, 0), (1, THIRD, 2)])
    scratch, partners = quad_scratch((THIRD,)), NEAR
    if final:
        partners = NEAR | FAR
        scratch += [pltpu.VMEM((N_QKV, *CUBE[1:], ROWS, n), BF) for _, n, _ in thirds(THIRD)] + [pltpu.SemaphoreType.DMA((N_QKV, 3, 3))] * 2
        outs, specs = outs[1::2] + [sds((3, *o.shape[2:])) for o in outs[::2]], specs[1::2] + [ANY] * 6
    (dh, *got), _ = run(functools.partial(_qkv_back, bm=bm, final=final), "qkv_back", N_QKV + T // bm, [h, a, dq, dkv, dhm, *w],
                        [pl.BlockSpec((bm, D), at), held((T, D)), held((T, D)), held((T, THIRD)), pl.BlockSpec((bm, D), at)] + [held((D, THIRD))] * 3,
                        [sds((T, D)), *outs], [pl.BlockSpec((bm, D), at), *specs], scratch, partners=partners, **kw)
    return dh, ([x for pair in zip(got[:6], got[6:]) for x in pair] if final else grouped(got))


def _finish(*refs, layers):
    outs = refs[len(refs) - 7 :]
    refs = list(refs[: len(refs) - 7])
    take = lambda: low(refs.pop(0)[:] + wide(refs.pop(0)[:]).sum(0))
    q, k, v, o, gate, up, down = outs
    for layer in range(layers):
        for parts, count, w in (((q,), 2, THIRD), ((k, v), 1, THIRD), ((gate, up), N_GU, GU), ((o,), 1, D)):
            ends = [sum(p.shape[2] for p in parts[:n]) for n in range(len(parts) + 1)]
            for first, n, _ in thirds(w):
                got = take()
                for t in range(count):
                    at = t * w + first
                    for p, begin, end in zip(parts, ends, ends[1:]):
                        a, b = max(at, begin), min(at + n, end)
                        if a < b:
                            p[layer, :, a - begin : b - begin] = got[:, t * n + a - at : t * n + b - at]
        down[layer] = take()


def finish(per_layer):
    ins = [a for arrays in per_layer for a in arrays]
    kv, layers = KV * HEAD, len(per_layer)
    shapes = [(layers, ROWS, n) for n in (D, kv, kv, D, FF, FF)] + [(layers, FF // 16, D)]
    whole = [pl.BlockSpec(memory_space=pltpu.VMEM)] * len(ins)
    return pl.pallas_call(functools.partial(_finish, layers=layers), in_specs=whole, out_specs=[pl.BlockSpec(memory_space=pltpu.VMEM)] * 7,
                          out_shape=[sds(s) for s in shapes], compiler_params=params(), name="finish")(*ins)


def solution(mesh):
    def both(x, dy, wq, wk, wv, wo, wg, wu, wd):
        cs = tuple(jnp.asarray(t) for t in tables())
        wkv = jnp.concatenate([wk, wv], axis=2)

        def projections(n):
            return [Gather(wq, n, (0, THIRD)), Gather(wq, n, (THIRD, THIRD)), Gather(wkv, n)]

        h0 = x[0]
        (q0, k0, v0, a0, at0, lse0), (*w_qkv0, wo0, wg0, wu0) = first(h0, cs, projections(0), [Gather(wo, 0), Gather(wg, 0), Gather(wu, 0)])
        w_qkv0, wo0, wg0, wu0 = [flat(w) for w in w_qkv0], flat(wo0), [flat(wg0)], [flat(wu0)]
        (hm0, gate0, up0, act0), (wd0, *w_qkv1) = mlp_up(h0, at0, wo0, wg0, wu0, send=[Gather(wd, 0), *projections(1)], ident=1, marks=(2, 5, 7))
        wd0, w_qkv1 = flat(wd0), [flat(w) for w in w_qkv1]
        (h1, q1, k1, v1, a1), (wg1,) = down_qkv(hm0, act0, wd0, cs, w_qkv1, send=[Gather(wg, 1)], ident=2, marks=(4, 7, 8))
        (at1, lse1), (wo1, wu1) = attend(q1, k1, v1, send=[Gather(wo, 1), Gather(wu, 1)], ident=3, marks=((2, 2), (3, 3), 4))
        wo1, wg1, wu1 = flat(wo1), [flat(wg1)], [flat(wu1)]
        (hm1, gate1, up1, act1), (wd1,) = mlp_up(h1, at1, wo1, wg1, wu1, send=[Gather(wd, 1)], ident=4, marks=(2, 4, 6))
        wd1 = flat(wd1)

        def spread(grads):
            return [Spread(sums, a) for g in grads for (sums, _), (a, _, _) in zip(g, AXES)]

        def with_own(grads, sent):
            return [x for g, n in zip(grads, range(len(grads))) for r in range(3) for x in (g[r][1], sent[3 * n + r])]

        def backward(d, ident, final, h, a, q, k, v, at, lse, hm, gate, up, act, w_qkv, wo, wg, wu, wd, before=()):
            (down, down_own), _ = down_grad(act, d, ident=ident)
            (dgu, b, dhm, dat, delta), (down_in, *sent_before) = mlp_back(d, hm, at, gate, up, wo, wg, wu, wd, send=[Scatter(down), *spread(before)],
                                                                         ident=ident + 1)
            grads = mlp_grads(b, dgu, at, dhm, ident=ident + 2)
            (dq, dkv), sent = attend_back(q, k, v, dat, lse, delta, cs, send=spread(grads), ident=ident + 3)
            dh, dw = qkv_back(h, a, dq, dkv, dhm, w_qkv, ident=ident + 4, final=final)
            return dh, dw, with_own(grads, sent) + [down_own, down_in], sent_before

        d0, dw1, done1, _ = backward(dy[0], 8, False, h1, a1, q1, k1, v1, at1, lse1, hm1, gate1, up1, act1, w_qkv1, wo1, wg1, wu1, wd1)
        dx, dw0, done0, dw1_in = backward(d0, 14, True, h0, a0, q0, k0, v0, at0, lse0, hm0, gate0, up0, act0, w_qkv0, wo0, wg0, wu0, wd0, dw1)
        return (dx[None], *finish([dw0 + done0, with_own(dw1, dw1_in) + done1]))

    states, cut = P(("rep", "dp"), None, None), P(None, "dp", None)
    return jax.shard_map(
        both,
        mesh=mesh,
        in_specs=(states, states) + (cut,) * 7,
        out_specs=(states,) + (P("rep", "dp", None),) * 7,
        check_vma=False,
    )
```

```python
import functools
import itertools

import jax
import jax.numpy as jnp
import numpy as np
from jax import lax
from jax.experimental import pallas as pl
from jax.experimental.pallas import tpu as pltpu
from jax.sharding import PartitionSpec as P

T, D, HEADS, KV, HEAD, FF, THETA = 2048, 1024, 8, 2, 128, 3200, 10000
G = HEADS // KV
QKV = D + 2 * KV * HEAD
THIRD = QKV // 3
BF, F32 = jnp.bfloat16, jnp.float32
LOG2E = 1.4426950408889634
SCALE = HEAD**-0.5
NEG, HIDDEN = -1e30, -2e30
ANY = pl.BlockSpec(memory_space=pl.ANY)


def step():
    return pl.program_id(0)


def steps():
    return pl.num_programs(0)


def params(**kw):
    return pltpu.CompilerParams(vmem_limit_bytes=62 * 2**20, **kw)


def sds(shape, dtype=BF):
    return jax.ShapeDtypeStruct(shape, dtype)


def rows(bm, n):
    return pl.BlockSpec((bm, n), lambda i: (i, 0))


def held(shape):
    return pl.BlockSpec(shape, lambda i: (0,) * len(shape), pipeline_mode=pl.Buffered(1))


def dot(a, b, ca=1, cb=0):
    return lax.dot_general(a, b, (((ca,), (cb,)), ((), ())), preferred_element_type=F32)


def dot_nt(a, b):
    return dot(a, b, 1, 1)


def dot_tn(a, b):
    return dot(a, b, 0, 0)


def low(x):
    return x.astype(BF)


def wide(x):
    return x.astype(F32)


def norm_scale(w):
    return lax.rsqrt(jnp.mean(w * w, -1, keepdims=True) + 1e-6)


def normed(h):
    w = wide(h)
    return low(w * norm_scale(w))


def norm_back(h, c):
    w = wide(h)
    s = norm_scale(w)
    return s * (c - w * (s * s) * jnp.mean(c * w, -1, keepdims=True))


def tables():
    half = HEAD // 2
    angle = np.arange(T, dtype=np.float32)[:, None] * (np.float32(THETA) ** (-np.arange(half, dtype=np.float32) / np.float32(half)))
    cos, sin = np.cos(angle).astype(np.float32), np.sin(angle).astype(np.float32)
    return np.concatenate([cos, cos], 1), np.concatenate([-sin, sin], 1)


def flat(w):
    return w.reshape(-1, w.shape[-1])


def head(n):
    return slice(HEAD * n, HEAD * (n + 1))


def heads_of(x):
    return [x[:, head(n)] for n in range(x.shape[1] // HEAD)]


def turned(x, c, s):
    return [low(t * c + pltpu.roll(t, HEAD // 2, 1) * s) for t in heads_of(x)]


X, Y, Z = 4, 2, 1
NEAR = {1, 2 * X, 2 * Y, 2 * Z}
FAR = {2 * n for n in range(1, 8)}


def place():
    me = lax.axis_index("dp")
    return me, lax.div(me, 2), me % 2


def flipped(number, bits):
    for bit in sorted(NEAR):
        if bits & bit:
            number = number + bit - 2 * bit * (lax.div(number, bit) % 2)
    return number


AXES = ((X, Y, Z), (Y, Z, X), (Z, X, Y))
OTHERS = ((0, 1), (1, 1), (1, 0))


def thirds(n):
    units = n // 128
    sizes = [128 * (units // 3 + (r < units % 3)) for r in range(3)]
    return [(sum(sizes[:r]), sizes[r], axes) for r, axes in enumerate(AXES)]


class Gather:
    copies = 24
    partners = NEAR

    def __init__(self, src, layer, part=None):
        self.src, self.layer, self.part = src, layer, part
        rows, n = src.shape[1:]
        self.shape = (8, 2, rows, n if part is None else part[1])

    def bind(self, src, dst, send, recv):
        me, chip, core = place()
        own = src.at[self.layer] if self.part is None else src.at[self.layer, :, pl.ds(*self.part)]
        block = lambda bits: dst.at[flipped(chip, bits), core]
        count = iter(range(self.copies))

        def to(bits, where, first=0, n=None):
            k = next(count)
            cut = lambda ref: ref if n is None else ref.at[:, pl.ds(first, n)]
            return pltpu.make_async_remote_copy(cut(block(where)) if where else own, cut(block(where)), send.at[k], recv.at[k],
                                                device_id={"dp": flipped(me, bits)})

        split = thirds(dst.shape[3])
        self.links = [
            [to(2 * m, 0) for m in (X, Y, Z)],
            [to(2 * axes[to_], axes[from_], at, n) for from_, to_ in itertools.combinations(range(3), 2) for at, n, axes in split],
            [to(2 * c, a | b, at, n) for at, n, (a, b, c) in split],
        ]
        self.pairs = [[to(1, 0)], [to(1, m) for m in (X, Y, Z)], [to(1, m) for m in (X | Y, Y | Z, Z | X)], [to(1, X | Y | Z)]]
        self.local = pltpu.make_async_copy(own, block(0), send.at[self.copies - 1])
        self.ended = False

    def stage(self, n):
        for c in self.links[n - 1] if n else ():
            c.wait_recv()
        for c in (self.links[n] if n < 3 else []) + self.pairs[n]:
            c.start()
        if n == 0:
            self.local.start()

    def end(self):
        if not self.ended:
            self.ended = True
            for c in sum(self.pairs, []):
                c.wait_recv()
            for c in sum(self.links + self.pairs, []):
                c.wait_send()
            self.local.wait()


class Once:
    def stage(self, n):
        if n == 0:
            for c in self.all:
                c.start()

    def end(self):
        for c in self.all:
            c.wait()


class Scatter(Once):
    copies = 7
    partners = FAR

    def __init__(self, src):
        self.src = src
        self.shape = (7, *src.shape[1:])

    def bind(self, src, dst, send, recv):
        me, chip, _ = place()
        self.all = [
            pltpu.make_async_remote_copy(src.at[flipped(chip, m)], dst.at[m - 1], send.at[m - 1], recv.at[m - 1], device_id={"dp": flipped(me, 2 * m)})
            for m in (Z, Y | Z, Y, X | Y, X, X | Z, X | Y | Z)
        ]


def side(axis, index):
    return {X: (index,), Y: (slice(None), index), Z: (slice(None), slice(None), index)}[axis]


CUBE = (2, 2, 2)


def bit(chip, axis):
    return lax.div(chip, axis) % 2


def spreads(src, dst, axis, send, recv):
    me, chip, _ = place()
    out = []
    for k, far in enumerate(OTHERS):
        bits = [b for b in AXES[0] if b != axis]
        i, j = (1 - bit(chip, b) if f else bit(chip, b) for b, f in zip(bits, far))
        where = 2 * sum(b * f for b, f in zip(bits, far))
        out.append(pltpu.make_async_remote_copy(src.at[i, j], dst.at[k], send.at[k], recv.at[k], device_id={"dp": flipped(me, where)}))
    return out


class Spread(Once):
    copies = 3

    def __init__(self, src, axis):
        self.src, self.axis = src, axis
        self.planes = tuple(b for b in AXES[0] if b != axis)
        p, q = self.planes
        self.partners = {2 * p, 2 * q, 2 * (p + q)}
        self.shape = (3, *src.shape[2:])

    def bind(self, src, dst, send, recv):
        self.all = spreads(src, dst, self.axis, send, recv)


def meet(partners):
    me = lax.axis_index("dp")
    barrier = pltpu.get_barrier_semaphore()
    for bits in sorted(partners):
        pl.semaphore_signal(barrier, inc=1, device_id={"dp": flipped(me, bits)})
    pl.semaphore_wait(barrier, len(partners))


def staged(send, marks, count):
    marks = (0, *marks) if any(isinstance(t, Gather) for t in send) else (0,)

    def stage(n):
        for t in send:
            t.stage(n)

    def end():
        for n, mark in enumerate(marks):
            if mark == count:
                stage(n)
        for t in send:
            t.end()

    return {mark: functools.partial(stage, n) for n, mark in enumerate(marks) if mark != count}, end


def run(body, name, count, ins, in_specs, outs, out_specs, scratch=(), send=(), ident=None, marks=(), partners=(), plan=staged, shown=0, early=False):
    n_in, n_out, n_send, n_scratch = len(ins), len(outs), len(send), len(scratch)
    partners = set(partners).union(*(t.partners for t in send))

    def kernel(*refs):
        def take(n):
            nonlocal refs
            got, refs = refs[:n], refs[n:]
            return got

        a, c_src, o, c_dst = take(n_in), take(n_send), take(n_out), take(n_send)
        s, sems = take(n_scratch), refs
        i = step()
        for n, t in enumerate(send):
            t.bind(c_src[n], c_dst[n], sems[2 * n], sems[2 * n + 1])
        starts, end = plan(send, marks, count)
        inner = {mark: act for mark, act in starts.items() if isinstance(mark, tuple)}
        seen = (*a, *c_dst[:shown], *o, *s)

        @pl.when(i == 0)
        def _():
            if early:
                body(*seen, early=True)
            if partners:
                meet(partners)
                starts[0]()

        for mark, act in starts.items():
            if mark and mark not in inner:
                pl.when(i == mark)(act)

        def tick(j):
            for (first, then), act in inner.items():
                pl.when((i == first) & (j == then))(act)

        body(*seen, **({"tick": tick} if inner else {}))
        if send:
            pl.when(i == count - 1)(end)

    got = list(pl.pallas_call(
        kernel, grid=(count,), in_specs=[*in_specs, *[ANY] * n_send], out_specs=[*out_specs, *[ANY] * n_send],
        out_shape=[*outs, *(sds(t.shape) for t in send)],
        scratch_shapes=[*scratch, *(pltpu.SemaphoreType.DMA((t.copies,)) for t in send for _ in range(2))],
        compiler_params=params(**(dict(collective_id=ident, has_side_effects=True) if partners else {})), name=name,
    )(*ins, *(t.src for t in send)))
    return got[:n_out], got[n_out:]


def steps_of(t, first, after):
    return pl.when((t >= first) & (t < after))


def start(copies):
    for c in copies:
        c.start()


def wait(copies):
    for c in copies:
        c.wait()


def fetched(pairs, sem):
    return [pltpu.make_async_copy(a, b, sem.at[n]) for n, (a, b) in enumerate(pairs)]


def _qkv(h, c, s, w0, w1, w2, q, k, v, a_out):
    a = normed(h[:])
    a_out[:] = a
    cc, ss = c[:], s[:]
    for part, w in enumerate((w0, w1)):
        for n, t in enumerate(turned(wide(low(dot(a, flat(w[:])))), cc, ss)):
            at = HEAD * (n + part * G)
            q[:, at : at + HEAD] = t
    kv = low(dot(a, flat(w2[:])))
    for n, t in enumerate(turned(wide(kv[:, : KV * HEAD]), cc, ss)):
        k[:, head(n)] = t
    v[:] = kv[:, KV * HEAD :]


def later(bk, bq):
    place_of = functools.partial(lax.broadcasted_iota, jnp.int32, (bk, bq))
    return place_of(1) >= place_of(0)


def diagonal(part, at, size):
    half = size // 2
    part(at, half, 0, size, half)
    part(at + half, half, half, half, size)


def _attend(q, k, v, o, lse, top_s, mix_s, *, bq, iq=None, tick=lambda j: None):
    iq = step() if iq is None else iq
    e = SCALE * LOG2E
    top_s[:] = jnp.full(top_s.shape, NEG, F32)
    mix_s[:] = jnp.zeros(mix_s.shape, F32)

    def part(at, bk, first, nq, done=0):
        here, cols = pl.ds(pl.multiple_of(at, bk), bk), pl.ds(first, nq)
        scores = [dot_nt(k[here, head(n // G)], q[cols, head(n)]) for n in range(HEADS)]
        ok = later(bk, nq)
        ones = jnp.ones((8, bk), BF)
        weights, keeps = [], []
        for n, x in enumerate(scores):
            if done:
                x = jnp.where(ok, x, HIDDEN)
            old = top_s[n : n + 1, cols]
            top = jnp.maximum(old, x.max(axis=0, keepdims=True))
            top_s[n : n + 1, cols] = top
            weights.append(low(jnp.exp2((x - top) * e)))
            keeps.append(jnp.exp2((old - top) * e))
        for n in range(HEADS):
            i = n // G
            values = jnp.concatenate([v[here, head(i)].T, ones], axis=0)
            mix = mix_s[n, :, cols] * keeps[n] + dot(values, weights[n])
            mix_s[n, :, cols] = mix
            if done:
                w = done - first
                total = mix[HEAD : HEAD + 1, :w]
                o[first:done, head(n)] = low((mix[:HEAD, :w] * (1 / total)).T)
                lse[n : n + 1, first:done] = top_s[n : n + 1, first:done] * SCALE + jnp.log(total)

    def whole(j, _):
        tick(j)
        part(j * bq, bq, 0, bq)

    lax.fori_loop(0, iq, whole, None)
    tick(iq)
    diagonal(part, iq * bq, bq)


def attend(q, k, v, bq=512, **kw):
    return run(functools.partial(_attend, bq=bq), "attend", T // bq, [q, k, v],
               [rows(bq, D), held((T, KV * HEAD)), held((T, KV * HEAD))],
               [sds((T, D)), sds((HEADS, T), F32)], [rows(bq, D), pl.BlockSpec((HEADS, bq), lambda i: (0, i))],
               [pltpu.VMEM((HEADS, bq), F32), pltpu.VMEM((HEADS, HEAD + 8, bq), F32)], **kw)


TILES = 4


def _first(x, c, s, h0, h1, h2, q_out, k_out, v_out, a_out, o, lse, q, k, v, w0, w1, w2, sem, top_s, mix_s, *, bm, tick):
    i = step()

    @pl.when(i == 0)
    def _():
        cp = fetched(list(zip((h0, h1, h2), (w0, w1, w2))), sem)
        for d in cp:
            d.start()
        for d in cp:
            d.wait()

    @steps_of(i, 1, TILES + 1)
    def _():
        _qkv(x, c, s, w0, w1, w2, q_out, k_out, v_out, a_out)
        here = pl.ds(pl.multiple_of((i - 1) * bm, bm), bm)
        q[here, :] = q_out[:]
        k[here, :] = k_out[:]
        v[here, :] = v_out[:]

    @pl.when(i > TILES)
    def _():
        iq = i - TILES - 1
        _attend(q.at[pl.ds(pl.multiple_of(iq * bm, bm), bm)], k, v, o, lse, top_s, mix_s, bq=bm, iq=iq, tick=tick)


def first(x, cs, own, rest):
    bm, kv = T // TILES, KV * HEAD
    early = lambda i: (jnp.clip(i - 1, 0, TILES - 1), 0)
    late = lambda i: jnp.maximum(i - TILES - 1, 0)

    def plan(send, marks, count):
        def start():
            for stage in range(4):
                for t in own:
                    t.stage(stage)
                for t in {1: rest[:1], 2: rest[1:]}.get(stage, ()):
                    t.stage(0)
            for t in own:
                t.end()

        starts, end = staged(rest, marks, count)
        return {**starts, 0: start}, end

    return run(functools.partial(_first, bm=bm), "first", 2 * TILES + 1, [x, *cs], [pl.BlockSpec((bm, D), early)] + [pl.BlockSpec((bm, HEAD), early)] * 2,
               [sds((T, D)), sds((T, kv)), sds((T, kv)), sds((T, D)), sds((T, D)), sds((HEADS, T), F32)],
               [pl.BlockSpec((bm, w), early) for w in (D, kv, kv, D)] + [pl.BlockSpec((bm, D), lambda i: (late(i), 0)), pl.BlockSpec((HEADS, bm), lambda i: (0, late(i)))],
               [pltpu.VMEM((T, D), BF), pltpu.VMEM((T, kv), BF), pltpu.VMEM((T, kv), BF)] + [pltpu.VMEM((8, 2, D // 16, THIRD), BF)] * 3
               + [pltpu.SemaphoreType.DMA((3,)), pltpu.VMEM((HEADS, bm), F32), pltpu.VMEM((HEADS, HEAD + 8, bm), F32)],
               send=[*own, *rest], ident=0, marks=(TILES + 2, (2 * TILES, 2), 2 * TILES + 1), plan=plan, shown=len(own))


CHUNK = 768
CHUNKS = [(a, CHUNK if a + 2 * CHUNK <= FF else FF - a) for a in range(0, FF - CHUNK, CHUNK)]


def into(w, pieces):
    at, out = 0, []
    for p in pieces:
        out.append((p, w.at[:, pl.ds(at, p.shape[1])]))
        at += p.shape[1]
    return out


def lagged(bm, n):
    return pl.BlockSpec((bm, n), lambda i: (jnp.maximum(i - 1, 0), 0))


def ahead(bm, n):
    return pl.BlockSpec((bm, n), lambda i: (jnp.minimum(i, T // bm - 1), 0))


def _mlp_up(h, at, wo_h, *rest, n_gate, n_up, early=False):
    wg_h, wu_h, (hm, gate, up, act, wo, wg, wu, sem) = rest[:n_gate], rest[n_gate : n_gate + n_up], rest[n_gate + n_up :]
    first = step() == 0
    cp = fetched([(wo_h, wo), *into(wg, wg_h), *into(wu, wu_h)], sem)

    if early:
        return start(cp)

    @pl.when(first)
    def _():
        cp[0].wait()

    m = low(wide(h[:]) + wide(low(dot(at[:], wo[:]))))
    hm[:] = m
    b = normed(m)

    @pl.when(first)
    def _():
        for c in cp[1:]:
            c.wait()

    for a, n in CHUNKS:
        g, u = dot(b, wg[:, a : a + n]), dot(b, wu[:, a : a + n])
        gate[:, a : a + n] = g
        up[:, a : a + n] = u
        act[:, a : a + n] = low(jax.nn.silu(g) * u)


def mlp_up(h, at, wo, wg, wu, bm=256, **kw):
    return run(functools.partial(_mlp_up, n_gate=len(wg), n_up=len(wu)), "mlp_up", T // bm, [h, at, wo, *wg, *wu],
               [rows(bm, D), rows(bm, D)] + [ANY] * (1 + len(wg) + len(wu)),
               [sds((T, D)), sds((T, FF), F32), sds((T, FF), F32), sds((T, FF))], [rows(bm, D), rows(bm, FF), rows(bm, FF), rows(bm, FF)],
               [pltpu.VMEM((D, D), BF), pltpu.VMEM((D, FF), BF), pltpu.VMEM((D, FF), BF), pltpu.SemaphoreType.DMA((1 + len(wg) + len(wu),))], early=True, **kw)


def _down_qkv(m, act, wd, c, s, w0, w1, w2, y, q, k, v, a):
    y[:] = low(wide(m[:]) + wide(low(dot(act[:], wd[:]))))
    _qkv(y, c, s, w0, w1, w2, q, k, v, a)


def down_qkv(m, act, wd, cs, w, bm=256, **kw):
    kv = KV * HEAD
    return run(_down_qkv, "down_qkv", T // bm, [m, act, wd, *cs, *w],
               [rows(bm, D), rows(bm, FF), held((FF, D)), rows(bm, HEAD), rows(bm, HEAD)] + [held((D, THIRD))] * 3,
               [sds((T, D)), sds((T, D)), sds((T, kv)), sds((T, kv)), sds((T, D))], [rows(bm, w) for w in (D, D, kv, kv, D)], **kw)


def _mlp_back(dy, hm, at, gate, up, wo_h, wd_h, *rest, n_gate, n_up, early=False):
    wg_h, wu_h, rest = rest[:n_gate], rest[n_gate : n_gate + n_up], rest[n_gate + n_up :]
    dgu, b_out, dhm, dat, delta, wo, wg, wu, wd, sem, d_s, db_s = rest
    t, count = step(), steps() - 1
    now, last = t % 2, (t + 1) % 2
    cp = fetched([(wd_h.at[pl.ds(a, n)], wd.at[pl.ds(a, n)]) for a, n in CHUNKS] + [*into(wg, wg_h), *into(wu, wu_h), (wo_h, wo)], sem)
    n_down = len(CHUNKS)
    if early:
        return start(cp)

    def grads(wait=lambda copies: None):
        d = dy[:]
        d_s[now] = d
        for (a, n), c in zip(CHUNKS, cp):
            wait([c])
            da = wide(low(dot_nt(d, wd[a : a + n, :])))
            g, u = gate[:, a : a + n], up[:, a : a + n]
            s = jax.nn.sigmoid(g)
            gs = g * s
            dgu[:, a : a + n] = low(da * u * (s + gs * (1 - s)))
            dgu[:, FF + a : FF + a + n] = low(da * gs)
        wait(cp[n_down:])
        db_s[now] = low(wide(low(dot_nt(dgu[:, :FF], wg[:]))) + wide(low(dot_nt(dgu[:, FF:], wu[:]))))

    def leave():
        db, w = wide(db_s[last]), wide(hm[:])
        s = norm_scale(w)
        b_out[:] = low(w * s)
        m = low(wide(d_s[last]) + wide(low(s * (db - w * (s * s) * jnp.mean(db * w, -1, keepdims=True)))))
        dhm[:] = m
        x = low(dot_nt(m, wo[:]))
        dat[:] = x
        lane = lax.broadcasted_iota(jnp.int32, (m.shape[0], HEAD), 1)
        sums = jnp.zeros((m.shape[0], HEAD), F32)
        for n, r in enumerate(heads_of(wide(x) * wide(at[:]))):
            sums = jnp.where(lane == n, r.sum(-1, keepdims=True), sums)
        delta[:] = sums.T[:HEADS, :]

    @pl.when(t == 0)
    def _():
        grads(lambda copies: [c.wait() for c in copies])

    @steps_of(t, 1, count)
    def _():
        leave()
        grads()

    pl.when(t == count)(leave)


def mlp_back(dy, hm, at, gate, up, wo, wg, wu, wd, bm=256, **kw):
    n = len(wg) + len(wu) + len(CHUNKS) + 1
    return run(functools.partial(_mlp_back, n_gate=len(wg), n_up=len(wu)), "mlp_back", T // bm + 1, [dy, hm, at, gate, up, wo, wd, *wg, *wu],
               [ahead(bm, D), lagged(bm, D), lagged(bm, D), ahead(bm, FF), ahead(bm, FF)] + [ANY] * (2 + len(wg) + len(wu)),
               [sds((T, 2 * FF)), sds((T, D)), sds((T, D)), sds((T, D)), sds((HEADS, T), F32)],
               [ahead(bm, 2 * FF), lagged(bm, D), lagged(bm, D), lagged(bm, D), pl.BlockSpec((HEADS, bm), lambda i: (0, jnp.maximum(i - 1, 0)))],
               [pltpu.VMEM((D, D), BF), pltpu.VMEM((D, FF), BF), pltpu.VMEM((D, FF), BF), pltpu.VMEM((FF, D), BF), pltpu.SemaphoreType.DMA((n,)),
                pltpu.VMEM((2, bm, D), BF), pltpu.VMEM((2, bm, D), BF)], early=True, **kw)


def passed(out, back, send, recv, slot, bits):
    return pltpu.make_async_remote_copy(out.at[slot], back.at[slot], send.at[slot], recv.at[slot], device_id={"dp": flipped(lax.axis_index("dp"), bits)})


def keep(x, tile, out, slot, core):
    w = x.shape[1]
    tile[slot, :, :, :, :, :, :w] = x.reshape(*tile.shape[1:6], w)
    out[slot, :, :, :, :, :w] = low(tile[slot, :, :, :, 1 - core, :, :w])


PARTS = 4


def parts_of(h, v):
    return [(h.at[pl.ds(n * T // PARTS, T // PARTS)], v.at[pl.ds(n * T // PARTS, T // PARTS)]) for n in range(PARTS)]


def by_parts(a, b, wait):
    total = 0
    for n in range(PARTS):
        wait(n)
        rows = slice(n * T // PARTS, (n + 1) * T // PARTS)
        total += dot_tn(a[rows], b[rows])
    return total


def _pair(act, dy, sums, own, tile, out, back, send, recv):
    t = step()
    me, chip, core = place()
    now, last = t % 2, (t + 1) % 2
    count = steps() - 1

    @pl.when(t > 0)
    def _():
        passed(out, back, send, recv, last, 1).start()

    @pl.when(t < count)
    def _():
        keep(dot_tn(act[:], dy[:]), tile, out, now, core)

    @pl.when(t > 0)
    def _():
        passed(out, back, send, recv, last, 1).wait()
        sums[:] = low(tile[last, :, :, :, core] + wide(back[last])).reshape(sums.shape)
        here = (last, *(bit(chip, b) for b in AXES[0]))
        own[:] = tile[(*here, core)] + wide(back[here])


def pair_scratch(r, w):
    return [pltpu.VMEM((2, *CUBE, 2, r, w), F32), pltpu.VMEM((2, *CUBE, r, w), BF), pltpu.VMEM((2, *CUBE, r, w), BF),
            pltpu.SemaphoreType.DMA((2,)), pltpu.SemaphoreType.DMA((2,))]


def down_grad(act, dy, w=256, **kw):
    r, n = FF // 16, D // w
    done = lambda i: jnp.maximum(i - 1, 0)
    return run(_pair, "down_grad", n + 1, [act, dy], [held((T, FF)), pl.BlockSpec((T, w), lambda i: (0, jnp.minimum(i, n - 1)))],
               [sds((8, r, D)), sds((r, D), F32)], [pl.BlockSpec((8, r, w), lambda i: (0, 0, done(i))), pl.BlockSpec((r, w), lambda i: (0, done(i)))],
               pair_scratch(r, w), partners={1}, **kw)


ROWS = D // 16


def _quad(tiles, outs, tile, out, back, send, recv, half, *rest):
    half_out, half_back, half_send, half_recv = (rest[n : n + 3] for n in range(0, 12, 3))
    t = step()
    me, chip, core = place()
    now, last = t % 2, (t + 1) % 2
    count = tiles[-1][1]

    def turn(r, n):
        return pltpu.make_async_remote_copy(half_out[r].at[n % 2], half_back[r].at[n % 4], half_send[r].at[n % 2], half_recv[r].at[n % 4],
                                            device_id={"dp": flipped(me, 2 * AXES[r][0])})

    @pl.when((t > 0) & (t <= count))
    def _():
        passed(out, back, send, recv, last, 1).start()

    @pl.when((t > 1) & (t <= count + 1))
    def _():
        for r in range(3):
            turn(r, t - 2).start()

    for first, after, make in tiles:
        @steps_of(t, first, after)
        def _():
            keep(make(), tile, out, now, core)

    for (first, after, _), thirds_out in zip(tiles, outs):
        w = sum(o.shape[1] for _, o in thirds_out)

        @steps_of(t, first + 3, after + 3)
        def _():
            for r, ((at, n, (a, _, _)), (sums, own)) in enumerate(zip(thirds(w), thirds_out)):
                turn(r, t - 3).wait()
                here = pl.ds(at, n)
                came = half_back[r].at[(t - 3) % 4]
                sums[:] = low(half[last, :, :, :, here] + wide(came[:, :, :, :n]))
                i, j = (bit(chip, x) for x in AXES[0] if x != a)
                own[:] = half[last, i, j, :, here] + wide(came[i, j, :, :n])

        @steps_of(t, first + 1, after + 1)
        def _():
            passed(out, back, send, recv, last, 1).wait()
            for r, (at, n, (a, _, _)) in enumerate(thirds(w)):
                here = pl.ds(at, n)

                def pair(index):
                    index = side(a, index)
                    index = (last, *index, *[slice(None)] * (3 - len(index)))
                    return tile[(*index, core, slice(None), here)] + wide(back[(*index, slice(None), here)])

                half[last, :, :, :, here] = pair(bit(chip, a))
                half_out[r][last, :, :, :, :n] = low(pair(1 - bit(chip, a)))


def quad_scratch(widths):
    parts = [max(thirds(w)[r][1] for w in widths) for r in range(3)]
    sems = lambda n: [pltpu.SemaphoreType.DMA((n,))] * 3
    return [*pair_scratch(ROWS, max(widths)), pltpu.VMEM((*CUBE, ROWS, max(widths)), F32), *(pltpu.VMEM((*CUBE, ROWS, n), BF) for n in parts),
            *(pltpu.VMEM((4, 2, 2, ROWS, n), BF) for n in parts), *sems(2), *sems(4)]


def quad_outs(sizes):
    outs, specs = [], []
    for count, w, first in sizes:
        at = lambda i, first=first, count=count: jnp.clip(i - first - 3, 0, count - 1)
        for _, n, _ in thirds(w):
            outs += [sds((2, 2, ROWS, count * n)), sds((ROWS, count * n), F32)]
            specs += [pl.BlockSpec((2, 2, ROWS, n), lambda i, at=at: (0, 0, 0, at(i))), pl.BlockSpec((ROWS, n), lambda i, at=at: (0, at(i)))]
    return outs, specs


def grouped(refs):
    pairs = list(zip(refs[::2], refs[1::2]))
    return [pairs[n : n + 3] for n in range(0, len(pairs), 3)]


N_GU = 5
GU = 2 * FF // N_GU


def _mlp_grads(b, dgu, at_h, dhm_h, *rest):
    rest, (at, dhm, sem) = rest[:-3], rest[-3:]
    t = step()
    cp = fetched([(at_h, at), (dhm_h, dhm)], sem)

    @pl.when(t == 1)
    def _():
        for c in cp:
            c.start()

    @pl.when(t == N_GU)
    def _():
        for c in cp:
            c.wait()

    _quad([(0, N_GU, lambda: dot_tn(b[:], dgu[:])), (N_GU, N_GU + 1, lambda: dot_tn(at[:], dhm[:]))], grouped(rest[:12]), *rest[12:])


def mlp_grads(b, dgu, at, dhm, **kw):
    tile = lambda i: jnp.minimum(i, N_GU - 1)
    outs, specs = quad_outs([(N_GU, GU, 0), (1, D, N_GU)])
    got, _ = run(_mlp_grads, "mlp_grads", N_GU + 4, [b, dgu, at, dhm], [held((T, D)), pl.BlockSpec((T, GU), lambda i: (0, tile(i))), ANY, ANY],
                 outs, specs, [*quad_scratch((GU, D)), pltpu.VMEM((T, D), BF), pltpu.VMEM((T, D), BF), pltpu.SemaphoreType.DMA((2,))],
                 partners=NEAR, **kw)
    return grouped(got)


def _attend_back(q, k, v, do, lse, delta, c, s, c_all, s_all, dq, dkv, dq_s, dk_s, dv_s, *, bq):
    iq = step()
    e = SCALE * LOG2E

    @pl.when(iq == 0)
    def _():
        dk_s[:] = jnp.zeros_like(dk_s)
        dv_s[:] = jnp.zeros_like(dv_s)

    dq_s[:] = jnp.zeros_like(dq_s)
    lses = [lse[n : n + 1, :] * LOG2E for n in range(HEADS)]
    deltas = [delta[n : n + 1, :] for n in range(HEADS)]

    def part(at, bk, first, nq, done=0):
        here, cols = pl.ds(pl.multiple_of(at, bk), bk), slice(first, first + nq)
        qs, dos = ([x[cols, head(n)] for n in range(HEADS)] for x in (q, do))
        ks, vs = ([x[here, head(i)] for i in range(KV)] for x in (k, v))
        scores = [dot_nt(ks[n // G], qs[n]) for n in range(HEADS)]
        dps = [dot_nt(vs[n // G], dos[n]) for n in range(HEADS)]
        ok = later(bk, nq)
        for n in range(HEADS):
            i = n // G
            p = jnp.exp2(scores[n] * e - lses[n][:, cols])
            if done:
                p = jnp.where(ok, p, 0.0)
            ds = low(p * (dps[n] - deltas[n][:, cols]))
            dv_s[i, here, :] += dot(low(p), dos[n])
            dk_s[i, here, :] += dot(ds, qs[n])
            x = dq_s[n, :, cols] + dot(ks[i].T, ds)
            dq_s[n, :, cols] = x
            if done:
                rows = slice(first, done)
                dq[rows, head(n)] = turned(wide(low((x[:, : done - first] * SCALE).T)), c[rows], -s[rows])[0]

    lax.fori_loop(0, iq, lambda j, _: part(j * bq, bq, 0, bq), None)
    diagonal(part, iq * bq, bq)

    @pl.when(iq == steps() - 1)
    def _():
        for i in range(KV):
            dkv[:, head(i)] = turned(wide(low(dk_s[i] * SCALE)), c_all[:], -s_all[:])[0]
            dkv[:, head(KV + i)] = low(dv_s[i])


def attend_back(q, k, v, do, lse, delta, cs, bq=512, **kw):
    stats = pl.BlockSpec((HEADS, bq), lambda i: (0, i))
    keys = held((T, KV * HEAD))
    return run(functools.partial(_attend_back, bq=bq), "attend_back", T // bq, [q, k, v, do, lse, delta, *cs, *cs],
               [rows(bq, D), keys, keys, rows(bq, D), stats, stats, rows(bq, HEAD), rows(bq, HEAD), held((T, HEAD)), held((T, HEAD))],
               [sds((T, D)), sds((T, THIRD))], [rows(bq, D), held((T, THIRD))],
               [pltpu.VMEM((HEADS, HEAD, bq), F32), pltpu.VMEM((KV, T, HEAD), F32), pltpu.VMEM((KV, T, HEAD), F32)], **kw)


N_QKV = 3


def _qkv_back(h, a_h, dq_h, dkv_h, dhm, w0_h, w1_h, w2_h, dh, *rest, bm, final, early=False):
    t = step()
    rest, (a, dq, dkv, w0, w1, w2, sem) = rest[:-7], rest[-7:]
    cp = fetched([x for both in zip(parts_of(a_h, a), parts_of(dq_h, dq)) for x in both] + [(dkv_h, dkv), (w0_h, w0), (w1_h, w1), (w2_h, w2)], sem)
    if early:
        return start(cp)
    n_parts = 2 * PARTS
    moves = []

    for n, copies in ((2, cp[n_parts : n_parts + 1]), (N_QKV, cp[n_parts + 1 :])):
        @pl.when(t == n)
        def _():
            for c in copies:
                c.wait()

    def wait(n):
        for c in cp[2 * n : 2 * n + 2]:
            c.wait()

    if final:
        owns, came, rest, (*sums, send, recv) = rest[:6], rest[6:12], rest[12:-5], rest[-5:]
        outs = [[(sums[r].at[t - 3], owns[g + r]) for r in range(3)] for g in (0, 3)]
        for n in range(N_QKV):
            g, at = (0, n) if n < 2 else (3, 0)
            moves.append([c for r, (_, w, axes) in enumerate(thirds(THIRD))
                          for c in spreads(sums[r].at[n], came[g + r].at[:, :, pl.ds(at * w, w)], axes[0], send.at[n, r], recv.at[n, r])])
    else:
        outs, rest = grouped(rest[:12]), rest[12:]
    tiles = [(0, 1, lambda: by_parts(a, dq.at[:, pl.ds(0, THIRD)], wait)), (1, 2, lambda: dot_tn(a[:], dq[:, THIRD:])), (2, N_QKV, lambda: dot_tn(a[:], dkv[:]))]
    _quad(tiles, outs[:1] + outs, *rest)
    for n, copies in enumerate(moves):
        @pl.when(t == n + 4)
        def _():
            for c in copies:
                c.start()

    @pl.when(t >= N_QKV)
    def _():
        half = bm // 2
        for n in range(2):
            here = pl.ds(pl.multiple_of((t - N_QKV) * bm + n * half, half), half)
            there = slice(n * half, (n + 1) * half)
            da = dot_nt(dq[here, :THIRD], w0[:]) + dot_nt(dq[here, THIRD:], w1[:]) + dot_nt(dkv[here], w2[:])
            dh[there] = low(wide(dhm[there]) + wide(low(norm_back(h[there], wide(low(da))))))

    if final:
        @pl.when(t == steps() - 1)
        def _():
            for c in sum(moves, []):
                c.wait()


def qkv_back(h, a, dq, dkv, dhm, w, bm=512, final=False, **kw):
    at = lambda i: (jnp.maximum(i - N_QKV, 0), 0)
    outs, specs = quad_outs([(2, THIRD, 0), (1, THIRD, 2)])
    scratch, partners = quad_scratch((THIRD,)), NEAR
    mine = [pltpu.VMEM((T, D), BF)] * 2 + [pltpu.VMEM((T, THIRD), BF)] + [pltpu.VMEM((D, THIRD), BF)] * 3 + [pltpu.SemaphoreType.DMA((2 * PARTS + 4,))]
    if final:
        partners = NEAR | FAR
        scratch += [pltpu.VMEM((N_QKV, *CUBE[1:], ROWS, n), BF) for _, n, _ in thirds(THIRD)] + [pltpu.SemaphoreType.DMA((N_QKV, 3, 3))] * 2
        outs, specs = outs[1::2] + [sds((3, *o.shape[2:])) for o in outs[::2]], specs[1::2] + [ANY] * 6
    (dh, *got), _ = run(functools.partial(_qkv_back, bm=bm, final=final), "qkv_back", N_QKV + T // bm, [h, a, dq, dkv, dhm, *w],
                        [pl.BlockSpec((bm, D), at), ANY, ANY, ANY, pl.BlockSpec((bm, D), at)] + [ANY] * 3,
                        [sds((T, D)), *outs], [pl.BlockSpec((bm, D), at), *specs], scratch + mine, partners=partners, early=True, **kw)
    return dh, ([x for pair in zip(got[:6], got[6:]) for x in pair] if final else grouped(got))


def _finish(*refs, layers):
    outs = refs[len(refs) - 7 :]
    refs = list(refs[: len(refs) - 7])
    take = lambda: low(refs.pop(0)[:] + wide(refs.pop(0)[:]).sum(0))
    q, k, v, o, gate, up, down = outs
    for layer in range(layers):
        for parts, count, w in (((q,), 2, THIRD), ((k, v), 1, THIRD), ((gate, up), N_GU, GU), ((o,), 1, D)):
            ends = [sum(p.shape[2] for p in parts[:n]) for n in range(len(parts) + 1)]
            for first, n, _ in thirds(w):
                got = take()
                for t in range(count):
                    at = t * w + first
                    for p, begin, end in zip(parts, ends, ends[1:]):
                        a, b = max(at, begin), min(at + n, end)
                        if a < b:
                            p[layer, :, a - begin : b - begin] = got[:, t * n + a - at : t * n + b - at]
        down[layer] = take()


def finish(per_layer):
    ins = [a for arrays in per_layer for a in arrays]
    kv, layers = KV * HEAD, len(per_layer)
    shapes = [(layers, ROWS, n) for n in (D, kv, kv, D, FF, FF)] + [(layers, FF // 16, D)]
    whole = [pl.BlockSpec(memory_space=pltpu.VMEM)] * len(ins)
    return pl.pallas_call(functools.partial(_finish, layers=layers), in_specs=whole, out_specs=[pl.BlockSpec(memory_space=pltpu.VMEM)] * 7,
                          out_shape=[sds(s) for s in shapes], compiler_params=params(), name="finish")(*ins)


def solution(mesh):
    def both(x, dy, wq, wk, wv, wo, wg, wu, wd):
        cs = tuple(jnp.asarray(t) for t in tables())
        wkv = jnp.concatenate([wk, wv], axis=2)

        def projections(n):
            return [Gather(wq, n, (0, THIRD)), Gather(wq, n, (THIRD, THIRD)), Gather(wkv, n)]

        h0 = x[0]
        (q0, k0, v0, a0, at0, lse0), (*w_qkv0, wo0, wg0, wu0) = first(h0, cs, projections(0), [Gather(wo, 0), Gather(wg, 0), Gather(wu, 0)])
        w_qkv0, wo0, wg0, wu0 = [flat(w) for w in w_qkv0], flat(wo0), [flat(wg0)], [flat(wu0)]
        (hm0, gate0, up0, act0), (wd0, *w_qkv1) = mlp_up(h0, at0, wo0, wg0, wu0, send=[Gather(wd, 0), *projections(1)], ident=1, marks=(2, 5, 7))
        wd0, w_qkv1 = flat(wd0), [flat(w) for w in w_qkv1]
        (h1, q1, k1, v1, a1), (wg1,) = down_qkv(hm0, act0, wd0, cs, w_qkv1, send=[Gather(wg, 1)], ident=2, marks=(4, 7, 8))
        (at1, lse1), (wo1, wu1) = attend(q1, k1, v1, send=[Gather(wo, 1), Gather(wu, 1)], ident=3, marks=((2, 2), (3, 3), 4))
        wo1, wg1, wu1 = flat(wo1), [flat(wg1)], [flat(wu1)]
        (hm1, gate1, up1, act1), (wd1,) = mlp_up(h1, at1, wo1, wg1, wu1, send=[Gather(wd, 1)], ident=4, marks=(2, 4, 6))
        wd1 = flat(wd1)

        def spread(grads):
            return [Spread(sums, a) for g in grads for (sums, _), (a, _, _) in zip(g, AXES)]

        def with_own(grads, sent):
            return [x for g, n in zip(grads, range(len(grads))) for r in range(3) for x in (g[r][1], sent[3 * n + r])]

        def backward(d, ident, final, h, a, q, k, v, at, lse, hm, gate, up, act, w_qkv, wo, wg, wu, wd, before=()):
            (down, down_own), _ = down_grad(act, d, ident=ident)
            (dgu, b, dhm, dat, delta), (down_in, *sent_before) = mlp_back(d, hm, at, gate, up, wo, wg, wu, wd, send=[Scatter(down), *spread(before)],
                                                                         ident=ident + 1)
            grads = mlp_grads(b, dgu, at, dhm, ident=ident + 2)
            (dq, dkv), sent = attend_back(q, k, v, dat, lse, delta, cs, send=spread(grads), ident=ident + 3)
            dh, dw = qkv_back(h, a, dq, dkv, dhm, w_qkv, ident=ident + 4, final=final)
            return dh, dw, with_own(grads, sent) + [down_own, down_in], sent_before

        d0, dw1, done1, _ = backward(dy[0], 8, False, h1, a1, q1, k1, v1, at1, lse1, hm1, gate1, up1, act1, w_qkv1, wo1, wg1, wu1, wd1)
        dx, dw0, done0, dw1_in = backward(d0, 14, True, h0, a0, q0, k0, v0, at0, lse0, hm0, gate0, up0, act0, w_qkv0, wo0, wg0, wu0, wd0, dw1)
        return (dx[None], *finish([dw0 + done0, with_own(dw1, dw1_in) + done1]))

    states, cut = P(("rep", "dp"), None, None), P(None, "dp", None)
    return jax.shard_map(
        both,
        mesh=mesh,
        in_specs=(states, states) + (cut,) * 7,
        out_specs=(states,) + (P("rep", "dp", None),) * 7,
        check_vma=False,
    )
```

```python
import functools
import itertools

import jax
import jax.numpy as jnp
import numpy as np
from jax import lax
from jax.experimental import pallas as pl
from jax.experimental.pallas import tpu as pltpu
from jax.sharding import PartitionSpec as P

T, D, HEADS, KV, HEAD, FF, THETA = 2048, 1024, 8, 2, 128, 3200, 10000
G = HEADS // KV
VMEM = 62 * 2**20
MOST = 67043328
QKV = D + 2 * KV * HEAD
THIRD = QKV // 3
BF, F32 = jnp.bfloat16, jnp.float32
LOG2E = 1.4426950408889634
SCALE = HEAD**-0.5
NEG, HIDDEN = -1e30, -2e30
ANY = pl.BlockSpec(memory_space=pl.ANY)


def step():
    return pl.program_id(0)


def steps():
    return pl.num_programs(0)


def params(**kw):
    return pltpu.CompilerParams(**{"vmem_limit_bytes": VMEM, **kw})


def sds(shape, dtype=BF):
    return jax.ShapeDtypeStruct(shape, dtype)


def by_rows(bm, n, at):
    return pl.BlockSpec((bm, n), lambda i: (at(i), 0))


def by_cols(n, bm, at):
    return pl.BlockSpec((n, bm), lambda i: (0, at(i)))


def rows(bm, n):
    return by_rows(bm, n, lambda i: i)


def held(shape):
    return pl.BlockSpec(shape, lambda i: (0,) * len(shape), pipeline_mode=pl.Buffered(1))


def dot(a, b, ca=1, cb=0):
    return lax.dot_general(a, b, (((ca,), (cb,)), ((), ())), preferred_element_type=F32)


def dot_nt(a, b):
    return dot(a, b, 1, 1)


def dot_tn(a, b):
    return dot(a, b, 0, 0)


def low(x):
    return x.astype(BF)


def wide(x):
    return x.astype(F32)


def row_mean(x):
    return jnp.mean(x, -1, keepdims=True)


def norm_scale(w):
    return lax.rsqrt(row_mean(w * w) + 1e-6)


def normed(h):
    w = wide(h)
    return low(w * norm_scale(w))


def norm_back(h, c):
    w = wide(h)
    s = norm_scale(w)
    return s * (c - w * (s * s) * row_mean(c * w))


def enter_back(da, h, dhm):
    return low(wide(dhm) + wide(low(norm_back(h, wide(da)))))


def tables():
    half = HEAD // 2
    angle = np.arange(T, dtype=np.float32)[:, None] * (np.float32(THETA) ** (-np.arange(half, dtype=np.float32) / np.float32(half)))
    cos, sin = np.cos(angle).astype(np.float32), np.sin(angle).astype(np.float32)
    return np.concatenate([cos, cos], 1), np.concatenate([-sin, sin], 1)


def flat(w):
    return w.reshape(-1, w.shape[-1])


def head(n):
    return slice(HEAD * n, HEAD * (n + 1))


def heads_of(x):
    return [x[:, head(n)] for n in range(x.shape[1] // HEAD)]


def turned(x, c, s):
    return [low(t * c + pltpu.roll(t, HEAD // 2, 1) * s) for t in heads_of(x)]


X, Y, Z = 4, 2, 1
NEAR = {1, 2 * X, 2 * Y, 2 * Z}
FAR = {2 * n for n in range(1, 8)}


def place():
    me = lax.axis_index("dp")
    return me, lax.div(me, 2), me % 2


def flipped(number, bits):
    for bit in sorted(NEAR):
        if bits & bit:
            number = number + bit - 2 * bit * (lax.div(number, bit) % 2)
    return number


AXES = ((X, Y, Z), (Y, Z, X), (Z, X, Y))
OTHERS = ((0, 1), (1, 1), (1, 0))


def thirds(n):
    units = n // 128
    sizes = [128 * (units // 3 + (r < units % 3)) for r in range(3)]
    return [(sum(sizes[:r]), sizes[r], axes) for r, axes in enumerate(AXES)]


class Gather:
    copies = 24
    partners = NEAR

    def __init__(self, src, layer):
        self.src, self.layer = src, layer
        self.shape = (8, 2, *src.shape[1:])

    def bind(self, src, dst, send, recv):
        me, chip, core = place()
        own = src.at[self.layer]
        block = lambda bits: dst.at[flipped(chip, bits), core]
        count = iter(range(self.copies))

        def to(bits, where, first=0, n=None):
            k = next(count)
            cut = lambda ref: ref if n is None else ref.at[:, pl.ds(first, n)]
            return pltpu.make_async_remote_copy(cut(block(where)) if where else own, cut(block(where)), send.at[k], recv.at[k],
                                                device_id={"dp": flipped(me, bits)})

        split = thirds(dst.shape[3])
        self.links = [
            [to(2 * m, 0) for m in (X, Y, Z)],
            [to(2 * axes[to_], axes[from_], at, n) for from_, to_ in itertools.combinations(range(3), 2) for at, n, axes in split],
            [to(2 * c, a | b, at, n) for at, n, (a, b, c) in split],
        ]
        self.pairs = [[to(1, 0)], [to(1, m) for m in (X, Y, Z)], [to(1, m) for m in (X | Y, Y | Z, Z | X)], [to(1, X | Y | Z)]]
        self.local = pltpu.make_async_copy(own, block(0), send.at[self.copies - 1])
        self.ended = False

    def stage(self, n):
        for c in self.links[n - 1] if n else ():
            c.wait_recv()
        for c in (self.links[n] if n < 3 else []) + self.pairs[n]:
            c.start()
        if n == 0:
            self.local.start()

    def end(self):
        if not self.ended:
            self.ended = True
            for c in sum(self.pairs, []):
                c.wait_recv()
            for c in sum(self.links + self.pairs, []):
                c.wait_send()
            self.local.wait()


class Once:
    def stage(self, n):
        if n == 0:
            for c in self.all:
                c.start()

    def end(self):
        for c in self.all:
            c.wait()


class Scatter(Once):
    copies = 7
    partners = FAR

    def __init__(self, src):
        self.src = src
        self.shape = (7, *src.shape[1:])

    def bind(self, src, dst, send, recv):
        me, chip, _ = place()
        self.all = [
            pltpu.make_async_remote_copy(src.at[flipped(chip, m)], dst.at[m - 1], send.at[m - 1], recv.at[m - 1], device_id={"dp": flipped(me, 2 * m)})
            for m in (Z, Y | Z, Y, X | Y, X, X | Z, X | Y | Z)
        ]


def side(axis, index):
    return {X: (index,), Y: (slice(None), index), Z: (slice(None), slice(None), index)}[axis]


CUBE = (2, 2, 2)


def bit(chip, axis):
    return chip // axis % 2 if isinstance(chip, int) else lax.div(chip, axis) % 2


def spreads(src, dst, axis, send, recv):
    me, chip, _ = place()
    out = []
    for k, far in enumerate(OTHERS):
        bits = [b for b in AXES[0] if b != axis]
        i, j = (1 - bit(chip, b) if f else bit(chip, b) for b, f in zip(bits, far))
        where = 2 * sum(b * f for b, f in zip(bits, far))
        out.append(pltpu.make_async_remote_copy(src.at[i, j], dst.at[k], send.at[k], recv.at[k], device_id={"dp": flipped(me, where)}))
    return out


class Spread(Once):
    copies = 3

    def __init__(self, src, axis):
        self.src, self.axis = src, axis
        self.planes = tuple(b for b in AXES[0] if b != axis)
        p, q = self.planes
        self.partners = {2 * p, 2 * q, 2 * (p + q)}
        self.shape = (3, *src.shape[2:])

    def bind(self, src, dst, send, recv):
        self.all = spreads(src, dst, self.axis, send, recv)


def meet(partners):
    me = lax.axis_index("dp")
    barrier = pltpu.get_barrier_semaphore()
    for bits in sorted(partners):
        pl.semaphore_signal(barrier, inc=1, device_id={"dp": flipped(me, bits)})
    pl.semaphore_wait(barrier, len(partners))


def staged(send, marks, count):
    marks = (0, *marks) if any(isinstance(t, Gather) for t in send) else (0,)

    def stage(n):
        for t in send:
            t.stage(n)

    def end():
        for n, mark in enumerate(marks):
            if mark == count:
                stage(n)
        for t in send:
            t.end()

    return {mark: functools.partial(stage, n) for n, mark in enumerate(marks) if mark != count}, end


def run(body, name, count, ins, in_specs, outs, out_specs, scratch=(), send=(), ident=None, marks=(), partners=(), plan=staged, shown=0, early=False, **kw):
    n_in, n_out, n_send, n_scratch = len(ins), len(outs), len(send), len(scratch)
    partners = set(partners).union(*(t.partners for t in send))

    def kernel(*refs):
        def take(n):
            nonlocal refs
            got, refs = refs[:n], refs[n:]
            return got

        a, c_src, o, c_dst = take(n_in), take(n_send), take(n_out), take(n_send)
        s, sems = take(n_scratch), refs
        i = step()
        for n, t in enumerate(send):
            t.bind(c_src[n], c_dst[n], sems[2 * n], sems[2 * n + 1])
        starts, end = plan(send, marks, count)
        inner = {mark: act for mark, act in starts.items() if isinstance(mark, tuple)}
        seen = (*a, *c_dst[:shown], *o, *s)

        @pl.when(i == 0)
        def _():
            if early:
                body(*seen, early=True)
            if partners:
                meet(partners)
                starts[0]()

        for mark, act in starts.items():
            if mark and mark not in inner:
                pl.when(i == mark)(act)

        def tick(j):
            for (first, then), act in inner.items():
                pl.when((i == first) & (j == then))(act)

        body(*seen, **({"tick": tick} if inner else {}))
        if send:
            pl.when(i == count - 1)(end)

    got = list(pl.pallas_call(
        kernel, grid=(count,), in_specs=[*in_specs, *[ANY] * n_send], out_specs=[*out_specs, *[ANY] * n_send],
        out_shape=[*outs, *(sds(t.shape) for t in send)],
        scratch_shapes=[*scratch, *(pltpu.SemaphoreType.DMA((t.copies,)) for t in send for _ in range(2))],
        compiler_params=params(**(dict(collective_id=ident, has_side_effects=True) if partners else {}), **kw), name=name,
    )(*ins, *(t.src for t in send)))
    return got[:n_out], got[n_out:]


def steps_of(t, first, after):
    return pl.when((t >= first) & (t < after))


def start(copies):
    for c in copies:
        c.start()


def wait(copies):
    for c in copies:
        c.wait()


def fetched(pairs, sem):
    return [pltpu.make_async_copy(a, b, sem.at[n]) for n, (a, b) in enumerate(pairs)]


def _qkv(h, c, s, wq, wkv, q, k, v, a_out):
    a = normed(h[:])
    a_out[:] = a
    cc, ss = c[:], s[:]
    for n, t in enumerate(turned(wide(low(dot(a, flat(wq[:])))), cc, ss)):
        q[:, head(n)] = t
    kv = low(dot(a, flat(wkv[:])))
    for n, t in enumerate(turned(wide(kv[:, : KV * HEAD]), cc, ss)):
        k[:, head(n)] = t
    v[:] = kv[:, KV * HEAD :]


def later(bk, bq):
    place_of = functools.partial(lax.broadcasted_iota, jnp.int32, (bk, bq))
    return place_of(1) >= place_of(0)


def diagonal(part, at, size):
    half = size // 2
    part(at, half, 0, size, half)
    part(at + half, half, half, half, size)


def _attend(q, k, v, o, lse, top_s, mix_s, *, iq, tick):
    bq = TILE
    e = SCALE * LOG2E
    top_s[:] = jnp.full(top_s.shape, NEG, F32)
    mix_s[:] = jnp.zeros(mix_s.shape, F32)

    def part(at, bk, first, nq, done=0):
        here, cols = pl.ds(pl.multiple_of(at, bk), bk), pl.ds(first, nq)
        scores = [dot_nt(k[here, head(n // G)], q[cols, head(n)]) for n in range(HEADS)]
        ok = later(bk, nq)
        ones = jnp.ones((8, bk), BF)
        weights, keeps = [], []
        for n, x in enumerate(scores):
            if done:
                x = jnp.where(ok, x, HIDDEN)
            old = top_s[n : n + 1, cols]
            top = jnp.maximum(old, x.max(axis=0, keepdims=True))
            top_s[n : n + 1, cols] = top
            weights.append(low(jnp.exp2((x - top) * e)))
            keeps.append(jnp.exp2((old - top) * e))
        for n in range(HEADS):
            i = n // G
            values = jnp.concatenate([v[here, head(i)].T, ones], axis=0)
            mix = mix_s[n, :, cols] * keeps[n] + dot(values, weights[n])
            mix_s[n, :, cols] = mix
            if done:
                w = done - first
                total = mix[HEAD : HEAD + 1, :w]
                o[first:done, head(n)] = low((mix[:HEAD, :w] * (1 / total)).T)
                lse[n : n + 1, first:done] = top_s[n : n + 1, first:done] * SCALE + jnp.log(total)

    def whole(j, _):
        tick(j)
        part(j * bq, bq, 0, bq)

    lax.fori_loop(0, iq, whole, None)
    tick(iq)
    diagonal(part, iq * bq, bq)


TILE = 512


def project(x, c, s, wq, wkv, outs, kept, at):
    _qkv(x, c, s, wq, wkv, *outs)
    for ref, out in zip(kept, outs):
        ref[pl.ds(pl.multiple_of(at, out.shape[0]), out.shape[0]), :] = out[:]


def attend_to(iq, kept, o, lse, top_s, mix_s, tick):
    q, k, v = kept
    _attend(q.at[pl.ds(pl.multiple_of(iq * TILE, TILE), TILE)], k, v, o, lse, top_s, mix_s, iq=iq, tick=tick)


def joint(body, name, ins, in_specs, before, bm, outs, weights, **kw):
    kv, tiles = KV * HEAD, T // bm
    late = lambda i: jnp.maximum(i - before - tiles, 0)
    widths = [*outs, D, kv, kv, D]
    return run(functools.partial(body, bm=bm), name, before + tiles + T // TILE, ins, in_specs, [sds((T, w)) for w in widths] + [sds((T, D)), sds((HEADS, T), F32)],
               [early_rows(bm, w, before) for w in widths] + [by_rows(TILE, D, late), by_cols(HEADS, TILE, late)],
               [pltpu.VMEM((T, D), BF), pltpu.VMEM((T, kv), BF), pltpu.VMEM((T, kv), BF)] + [pltpu.VMEM(w, BF) for w in weights]
               + [pltpu.SemaphoreType.DMA((len(weights),)), pltpu.VMEM((HEADS, TILE), F32), pltpu.VMEM((HEADS, HEAD + 8, TILE), F32)], **kw)


def early_rows(bm, n, before):
    return by_rows(bm, n, lambda i: jnp.clip(i - before, 0, T // bm - 1))


def _first(x, c, s, wq_h, wkv_h, q_out, k_out, v_out, a_out, o, lse, q, k, v, wq, wkv, sem, top_s, mix_s, *, bm, tick):
    i = step()

    @pl.when(i == 0)
    def _():
        cp = fetched([(wq_h, wq), (wkv_h, wkv)], sem)
        start(cp)
        wait(cp)

    @steps_of(i, 1, T // bm + 1)
    def _():
        project(x, c, s, wq, wkv, (q_out, k_out, v_out, a_out), (q, k, v), (i - 1) * bm)

    @pl.when(i > T // bm)
    def _():
        attend_to(i - T // bm - 1, (q, k, v), o, lse, top_s, mix_s, tick)


def first(x, cs, own, rest, bm=512):
    def plan(send, marks, count):
        def begin():
            for stage in range(4):
                for t in own:
                    t.stage(stage)
                for t in {1: rest[:1], 2: rest[1:]}.get(stage, ()):
                    t.stage(0)
            for t in own:
                t.end()

        starts, end = staged(rest, marks, count)
        return {**starts, 0: begin}, end

    tiles = T // bm
    return joint(_first, "first", [x, *cs], [early_rows(bm, n, 1) for n in (D, HEAD, HEAD)], 1, bm, [], [own[0].shape, own[1].shape],
                 send=[*own, *rest], ident=0, marks=(tiles + 1, (2 * tiles, 1), (2 * tiles, 3)), plan=plan, shown=len(own))


def _second(m, act, c, s, wd_h, wq_h, wkv_h, y, q_out, k_out, v_out, a_out, o, lse, q, k, v, wd, wq, wkv, sem, top_s, mix_s, *, bm, tick=None, early=False):
    i = step()
    cp = fetched([(wd_h, wd), (wq_h, wq), (wkv_h, wkv)], sem)
    if early:
        return start(cp)

    @pl.when(i == 0)
    def _():
        wait(cp)

    @pl.when(i < T // bm)
    def _():
        y[:] = low(wide(m[:]) + wide(low(dot(act[:], wd[:]))))
        project(y, c, s, wq, wkv, (q_out, k_out, v_out, a_out), (q, k, v), i * bm)

    @pl.when(i >= T // bm)
    def _():
        attend_to(i - T // bm, (q, k, v), o, lse, top_s, mix_s, tick)


def second(m, act, wd, cs, w, bm=256, **kw):
    return joint(_second, "second", [m, act, *cs, wd, *w], [early_rows(bm, n, 0) for n in (D, FF, HEAD, HEAD)] + [ANY] * 3, 0, bm, [D],
                 [wd.shape, *(x.shape for x in w)], early=True, **kw)


CHUNK = 768
CHUNKS = [(a, CHUNK if a + 2 * CHUNK <= FF else FF - a) for a in range(0, FF - CHUNK, CHUNK)]


def into(w, pieces):
    at, out = 0, []
    for p in pieces:
        out.append((p, w.at[:, pl.ds(at, p.shape[1])]))
        at += p.shape[1]
    return out


def lagged(bm, n):
    return by_rows(bm, n, lambda i: jnp.maximum(i - 2, 0))


def ahead(bm, n):
    return early_rows(bm, n, 1)


def _mlp_up(h, at, wo_h, *rest, n_gate, n_up, early=False):
    wg_h, wu_h, (hm, gate, up, act, wo, wg, wu, sem) = rest[:n_gate], rest[n_gate : n_gate + n_up], rest[n_gate + n_up :]
    first = step() == 0
    cp = fetched([(wo_h, wo), *into(wg, wg_h), *into(wu, wu_h)], sem)

    if early:
        return start(cp)

    @pl.when(first)
    def _():
        cp[0].wait()

    m = low(wide(h[:]) + wide(low(dot(at[:], wo[:]))))
    hm[:] = m
    b = normed(m)

    @pl.when(first)
    def _():
        for c in cp[1:]:
            c.wait()

    for a, n in CHUNKS:
        g, u = dot(b, wg[:, a : a + n]), dot(b, wu[:, a : a + n])
        gate[:, a : a + n] = g
        up[:, a : a + n] = u
        act[:, a : a + n] = low(jax.nn.silu(g) * u)


def mlp_up(h, at, wo, wg, wu, bm=256, **kw):
    return run(functools.partial(_mlp_up, n_gate=len(wg), n_up=len(wu)), "mlp_up", T // bm, [h, at, wo, *wg, *wu],
               [rows(bm, D), rows(bm, D)] + [ANY] * (1 + len(wg) + len(wu)),
               [sds((T, D)), sds((T, FF), F32), sds((T, FF), F32), sds((T, FF))], [rows(bm, D), rows(bm, FF), rows(bm, FF), rows(bm, FF)],
               [pltpu.VMEM((D, D), BF), pltpu.VMEM((D, FF), BF), pltpu.VMEM((D, FF), BF), pltpu.SemaphoreType.DMA((1 + len(wg) + len(wu),))], early=True, **kw)


def _mlp_back(dy, hm, at, gate, up, wo_h, wd_h, *rest, n_gate, n_up, early=False):
    wg_h, wu_h, rest = rest[:n_gate], rest[n_gate : n_gate + n_up], rest[n_gate + n_up :]
    dgu, b_out, dhm, dat, delta, wo, wg, wu, wd, sem, d_s, db_s = rest
    t, count = step() - 1, steps() - 2
    now, last = (t + 2) % 2, (t + 1) % 2
    cp = fetched([(wd_h.at[pl.ds(a, n)], wd.at[pl.ds(a, n)]) for a, n in CHUNKS] + [*into(wg, wg_h), *into(wu, wu_h), (wo_h, wo)], sem)
    n_down = len(CHUNKS)
    if early:
        return start(cp)

    def grads(wait=lambda copies: None):
        d = dy[:]
        d_s[now] = d
        for (a, n), c in zip(CHUNKS, cp):
            wait([c])
            da = wide(low(dot_nt(d, wd[a : a + n, :])))
            g, u = gate[:, a : a + n], up[:, a : a + n]
            s = jax.nn.sigmoid(g)
            gs = g * s
            dgu[:, a : a + n] = low(da * u * (s + gs * (1 - s)))
            dgu[:, FF + a : FF + a + n] = low(da * gs)
        wait(cp[n_down:])
        db_s[now] = low(wide(low(dot_nt(dgu[:, :FF], wg[:]))) + wide(low(dot_nt(dgu[:, FF:], wu[:]))))

    def leave():
        h = hm[:]
        b_out[:] = normed(h)
        m = enter_back(db_s[last], h, d_s[last])
        dhm[:] = m
        x = low(dot_nt(m, wo[:]))
        dat[:] = x
        lane = lax.broadcasted_iota(jnp.int32, (m.shape[0], HEAD), 1)
        sums = jnp.zeros((m.shape[0], HEAD), F32)
        for n, r in enumerate(heads_of(wide(x) * wide(at[:]))):
            sums = jnp.where(lane == n, r.sum(-1, keepdims=True), sums)
        delta[:] = sums.T[:HEADS, :]

    @pl.when(t == 0)
    def _():
        grads(lambda copies: [c.wait() for c in copies])

    @steps_of(t, 1, count)
    def _():
        leave()
        grads()

    pl.when(t == count)(leave)


def mlp_back(dy, hm, at, gate, up, wo, wg, wu, wd, bm=256, **kw):
    n = len(wg) + len(wu) + len(CHUNKS) + 1
    return run(functools.partial(_mlp_back, n_gate=len(wg), n_up=len(wu)), "mlp_back", T // bm + 2, [dy, hm, at, gate, up, wo, wd, *wg, *wu],
               [ahead(bm, D), lagged(bm, D), lagged(bm, D), ahead(bm, FF), ahead(bm, FF)] + [ANY] * (2 + len(wg) + len(wu)),
               [sds((T, 2 * FF)), sds((T, D)), sds((T, D)), sds((T, D)), sds((HEADS, T), F32)],
               [ahead(bm, 2 * FF), lagged(bm, D), lagged(bm, D), lagged(bm, D), by_cols(HEADS, bm, lambda i: jnp.maximum(i - 2, 0))],
               [pltpu.VMEM((D, D), BF), pltpu.VMEM((D, FF), BF), pltpu.VMEM((D, FF), BF), pltpu.VMEM((FF, D), BF), pltpu.SemaphoreType.DMA((n,)),
                pltpu.VMEM((2, bm, D), BF), pltpu.VMEM((2, bm, D), BF)], early=True, **kw)


def passed(out, back, send, recv, slot):
    return pltpu.make_async_remote_copy(out.at[slot], back.at[slot], send.at[slot], recv.at[slot], device_id={"dp": flipped(lax.axis_index("dp"), 1)})


def keep(x, tile, out, slot, core):
    w = x.shape[1]
    tile[slot, :, :, :, :, :, :w] = x.reshape(*tile.shape[1:6], w)
    out[slot, :, :, :, :, :w] = low(tile[slot, :, :, :, 1 - core, :, :w])


def _pair(act, dy, sums, own, tile, out, back, send, recv):
    t = step()
    me, chip, core = place()
    now, last = t % 2, (t + 1) % 2
    count = steps() - 1

    @pl.when(t > 0)
    def _():
        passed(out, back, send, recv, last).start()

    @pl.when(t < count)
    def _():
        keep(dot_tn(act[:], dy[:]), tile, out, now, core)

    @pl.when(t > 0)
    def _():
        passed(out, back, send, recv, last).wait()
        settle(tile, back, last, sums, own)


def settle(tile, back, slot, sums, own):
    _, chip, core = place()
    w = own.shape[1]
    sums[:] = low(tile[slot, :, :, :, core, :, :w] + wide(back[slot, :, :, :, :, :w])).reshape(sums.shape)
    here = (slot, *(bit(chip, b) for b in AXES[0]))
    own[:] = tile[(*here, core)][:, :w] + wide(back[here][:, :w])


def pair_scratch(r, w):
    return [pltpu.VMEM((2, *CUBE, 2, r, w), F32), pltpu.VMEM((2, *CUBE, r, w), BF), pltpu.VMEM((2, *CUBE, r, w), BF),
            pltpu.SemaphoreType.DMA((2,)), pltpu.SemaphoreType.DMA((2,))]


def down_grad(act, dy, w=256, **kw):
    r, n = FF // 16, D // w
    done = lambda i: jnp.maximum(i - 1, 0)
    return run(_pair, "down_grad", n + 1, [act, dy], [held((T, FF)), by_cols(T, w, lambda i: jnp.minimum(i, n - 1))],
               [sds((8, r, D)), sds((r, D), F32)], [pl.BlockSpec((8, r, w), lambda i: (0, 0, done(i))), by_cols(r, w, done)],
               pair_scratch(r, w), partners={1}, **kw)


ROWS = D // 16


def _quad(t, tiles, outs, tile, out, back, send, recv, half, *rest):
    half_out, half_back, half_send, half_recv = (rest[n : n + 3] for n in range(0, 12, 3))
    me, chip, core = place()
    now, last = (t + 8) % 2, (t + 9) % 2
    count = tiles[-1][1]

    def turn(r, n):
        return pltpu.make_async_remote_copy(half_out[r].at[n % 2], half_back[r].at[n % 4], half_send[r].at[n % 2], half_recv[r].at[n % 4],
                                            device_id={"dp": flipped(me, 2 * AXES[r][0])})

    @pl.when((t > 0) & (t <= count))
    def _():
        passed(out, back, send, recv, last).start()

    @steps_of(t, 2, 2 + max(after for (_, after, _), o in zip(tiles, outs) if len(o) == 3))
    def _():
        for r in range(3):
            turn(r, t - 2).start()

    for first, after, make in tiles:
        @steps_of(t, first, after)
        def _():
            keep(make(), tile, out, now, core)

    for (first, after, _), thirds_out in zip(tiles, outs):
        if len(thirds_out) == 1:
            @steps_of(t, first + 1, after + 1)
            def _():
                passed(out, back, send, recv, last).wait()
                settle(tile, back, last, *thirds_out[0])

            continue
        w = sum(o.shape[1] for _, o in thirds_out)

        @steps_of(t, first + 3, after + 3)
        def _():
            for r, ((at, n, (a, _, _)), (sums, own)) in enumerate(zip(thirds(w), thirds_out)):
                turn(r, t - 3).wait()
                here = pl.ds(at, n)
                came = half_back[r].at[(t - 3) % 4]
                sums[:] = low(half[last, :, :, :, here] + wide(came[:, :, :, :n]))
                i, j = (bit(chip, x) for x in AXES[0] if x != a)
                own[:] = half[last, i, j, :, here] + wide(came[i, j, :, :n])

        @steps_of(t, first + 1, after + 1)
        def _():
            passed(out, back, send, recv, last).wait()
            for r, (at, n, (a, _, _)) in enumerate(thirds(w)):
                here = pl.ds(at, n)

                def pair(index):
                    index = side(a, index)
                    index = (last, *index, *[slice(None)] * (3 - len(index)))
                    return tile[(*index, core, slice(None), here)] + wide(back[(*index, slice(None), here)])

                half[last, :, :, :, here] = pair(bit(chip, a))
                half_out[r][last, :, :, :, :n] = low(pair(1 - bit(chip, a)))


def quad_scratch(widths):
    parts = [max(thirds(w)[r][1] for w in widths) for r in range(3)]
    sems = lambda n: [pltpu.SemaphoreType.DMA((n,))] * 3
    return [*pair_scratch(ROWS, max(widths)), pltpu.VMEM((*CUBE, ROWS, max(widths)), F32), *(pltpu.VMEM((*CUBE, ROWS, n), BF) for n in parts),
            *(pltpu.VMEM((4, 2, 2, ROWS, n), BF) for n in parts), *sems(2), *sems(4)]


def quad_outs(sizes):
    outs, specs = [], []
    for count, w, first in sizes:
        at = lambda i, first=first, count=count: jnp.clip(i - first - 3, 0, count - 1)
        for _, n, _ in thirds(w):
            outs += [sds((2, 2, ROWS, count * n)), sds((ROWS, count * n), F32)]
            specs += [pl.BlockSpec((2, 2, ROWS, n), lambda i, at=at: (0, 0, 0, at(i))), by_cols(ROWS, n, at)]
    return outs, specs


def grouped(refs):
    pairs = list(zip(refs[::2], refs[1::2]))
    return [pairs[n : n + 3] for n in range(0, len(pairs), 3)]


N_GU = 5
GU = 2 * FF // N_GU


def _mlp_grads(b, dgu, at_h, dhm_h, *rest):
    rest, (at, dhm, sem) = rest[:-3], rest[-3:]
    t = step()
    cp = fetched([(at_h, at), (dhm_h, dhm)], sem)

    @pl.when(t == 1)
    def _():
        for c in cp:
            c.start()

    @pl.when(t == N_GU)
    def _():
        for c in cp:
            c.wait()

    outs = grouped(rest[:6]) + [[rest[6:8]]]
    _quad(t, [(0, N_GU, lambda: dot_tn(b[:], dgu[:])), (N_GU, N_GU + 1, lambda: dot_tn(at[:], dhm[:]))], outs, *rest[8:])


def mlp_grads(b, dgu, at, dhm, **kw):
    tile = lambda i: jnp.minimum(i, N_GU - 1)
    outs, specs = quad_outs([(N_GU, GU, 0)])
    outs += [sds((8, ROWS, D)), sds((ROWS, D), F32)]
    specs += [held((8, ROWS, D)), held((ROWS, D))]
    got, _ = run(_mlp_grads, "mlp_grads", N_GU + 3, [b, dgu, at, dhm], [held((T, D)), by_cols(T, GU, tile), ANY, ANY],
                 outs, specs, [*quad_scratch((GU, D)), pltpu.VMEM((T, D), BF), pltpu.VMEM((T, D), BF), pltpu.SemaphoreType.DMA((2,))],
                 partners=NEAR, **kw)
    return grouped(got[:6]), got[6:]


def _attend_back(iq, q, k, v, do, lse, delta, c_all, s_all, dq_all, dkv, sums, dk_s, dv_s):
    bq = TILE
    e = SCALE * LOG2E
    mine = pl.ds(pl.multiple_of(iq * bq, bq), bq)
    c, s, dq = c_all.at[mine], s_all.at[mine], dq_all.at[mine]

    @pl.when(iq == 0)
    def _():
        dk_s[:] = jnp.zeros_like(dk_s)
        dv_s[:] = jnp.zeros_like(dv_s)

    sums[:] = jnp.zeros(sums.shape, F32)
    lses = [lse[n : n + 1, :] * LOG2E for n in range(HEADS)]
    deltas = [delta[n : n + 1, :] for n in range(HEADS)]

    def part(at, bk, first, nq, done=0):
        here, cols = pl.ds(pl.multiple_of(at, bk), bk), slice(first, first + nq)
        ok = later(bk, nq)
        for i in range(KV):
            heads = range(G * i, G * (i + 1))
            kk, vv = k[here, head(i)], v[here, head(i)]
            scores = [dot_nt(kk, q[cols, head(n)]) for n in heads]
            dps = [dot_nt(vv, do[cols, head(n)]) for n in heads]
            for n, score, dp in zip(heads, scores, dps):
                p = jnp.exp2(score * e - lses[n][:, cols])
                if done:
                    p = jnp.where(ok, p, 0.0)
                ds = low(p * (dp - deltas[n][:, cols]))
                dv_s[i, here, :] += dot(low(p), do[cols, head(n)])
                dk_s[i, here, :] += dot(ds, q[cols, head(n)])
                at = (*(bit(n, b) for b in AXES[0]), slice(None), slice(None), cols)
                x = sums[at].reshape(HEAD, nq) + dot(kk.T, ds)
                sums[at] = x.reshape(-1, ROWS, nq)
                if done:
                    rows = slice(first, done)
                    dq[rows, head(n)] = turned(wide(low((x[:, : done - first] * SCALE).T)), c[rows], -s[rows])[0]

    lax.fori_loop(0, iq, lambda j, _: part(j * bq, bq, 0, bq), None)
    diagonal(part, iq * bq, bq)

    @pl.when(iq == BLOCKS - 1)
    def _():
        for i in range(KV):
            dkv[:, head(i)] = turned(wide(low(dk_s[i] * SCALE)), c_all[:], -s_all[:])[0]
            dkv[:, head(KV + i)] = low(dv_s[i])


N_QKV = 3
BLOCKS = T // TILE


def _enter_back(q, k, v, do, lse, delta, c_all, s_all, a_h, wq_h, wkv_h, *rest, bm, final, early=False):
    given, (dh, *rest) = ((), rest) if final else (rest[:2], rest[2:])
    rest, (dk_s, dv_s, dq, dkv, a, wq, wkv, sem) = rest[:-8], rest[-8:]
    t = step() - BLOCKS
    cp = fetched([(a_h, a), (wq_h, wq), (wkv_h, wkv)], sem)
    if early:
        return start(cp)

    moves = []
    if final:
        owns, came, rest, (*sums, send, recv) = rest[:6], rest[6:12], rest[12:-5], rest[-5:]
        outs = [[(sums[r].at[jnp.clip(t - 3, 0, N_QKV - 1)], owns[g + r]) for r in range(3)] for g in (0, 3)]
        for n in range(N_QKV):
            g, at = (0, n) if n < 2 else (3, 0)
            moves.append([c for r, (_, w, axes) in enumerate(thirds(THIRD))
                          for c in spreads(sums[r].at[n], came[g + r].at[:, :, pl.ds(at * w, w)], axes[0], send.at[n, r], recv.at[n, r])])
    else:
        outs, rest = grouped(rest[:12]), rest[12:]

    @pl.when(t < 0)
    def _():
        _attend_back(step(), q, k, v, do, lse, delta, c_all, s_all, dq, dkv, rest[0].at[0], dk_s, dv_s)

    pl.when(t == 0)(lambda: wait(cp))
    tiles = [(0, 1, lambda: dot_tn(a[:], dq[:, :THIRD])), (1, 2, lambda: dot_tn(a[:], dq[:, THIRD:])), (2, N_QKV, lambda: dot_tn(a[:], dkv[:]))]
    _quad(t, tiles, outs[:1] + outs, *rest)
    for n, copies in enumerate(moves):
        pl.when(t == n + 4)(functools.partial(start, copies))

    @pl.when(t >= N_QKV)
    def _():
        half = bm // 2
        for n in range(2):
            here = pl.ds(pl.multiple_of((t - N_QKV) * bm + n * half, half), half)
            there = slice(n * half, (n + 1) * half)
            da = low(dot_nt(dq[here], wq[:]) + dot_nt(dkv[here], wkv[:]))
            dh[there] = da if final else enter_back(da, *(x[there] for x in given))

    if final:
        pl.when(step() == steps() - 1)(lambda: wait(sum(moves, [])))


def attend_enter_back(q, k, v, do, lse, delta, cs, a, w, given, bm=512, final=False, **kw):
    at = lambda i: jnp.maximum(i - BLOCKS - N_QKV, 0)
    block = lambda i: jnp.minimum(i, BLOCKS - 1)
    outs, specs = quad_outs([(2, THIRD, BLOCKS), (1, THIRD, BLOCKS + 2)])
    scratch, partners = quad_scratch((THIRD,)), NEAR
    if final:
        partners = NEAR | FAR
        scratch += [pltpu.VMEM((N_QKV, *CUBE[1:], ROWS, n), BF) for _, n, _ in thirds(THIRD)] + [pltpu.SemaphoreType.DMA((N_QKV, 3, 3))] * 2
        outs, specs = outs[1::2] + [sds((3, *o.shape[2:])) for o in outs[::2]], specs[1::2] + [ANY] * 6
    scratch += [pltpu.VMEM((KV, T, HEAD), F32)] * 2
    scratch += [pltpu.VMEM(x, BF) for x in ((T, D), (T, THIRD), (T, D), *(x.shape for x in w))] + [pltpu.SemaphoreType.DMA((3,))]
    tile, keys, stats = by_rows(bm, D, at), held((T, KV * HEAD)), by_cols(HEADS, TILE, block)
    queries = by_rows(TILE, D, block)
    (dh, *got), sent = run(functools.partial(_enter_back, bm=bm, final=final), "attend_enter_back", BLOCKS + N_QKV + T // bm,
                           [q, k, v, do, lse, delta, *cs, a, *w, *given],
                           [queries, keys, keys, queries, stats, stats, held((T, HEAD)), held((T, HEAD))] + [ANY] * 3 + [tile] * len(given),
                           [sds((T, D)), *outs], [tile, *specs], scratch, partners=partners, early=True, vmem_limit_bytes=MOST, **kw)
    return dh, ([x for pair in zip(got[:6], got[6:]) for x in pair] if final else grouped(got)), sent


def _finish(da, h, dhm, *refs, n):
    arrays, dx, outs, here, sem = refs[:n], refs[n], refs[n + 1 : n + 8], refs[n + 8 : -1], refs[-1]
    t, layers = step(), outs[0].shape[0]
    cp = fetched(list(zip(arrays, here)), sem)
    pl.when(t == 0)(lambda: start(cp))
    dx[:] = enter_back(da[:], h[:], dhm[:])
    each = n // layers
    q, k, v, o, gate, up, down = outs
    for layer in range(layers):
        left = list(here[layer * each : (layer + 1) * each])
        take = lambda: low(left.pop(0)[:] + wide(left.pop(0)[:]).sum(0))

        @pl.when(t == steps() - layers + layer)
        def _():
            wait(cp[layer * each : (layer + 1) * each])
            for parts, count, w in (((q,), 2, THIRD), ((k, v), 1, THIRD), ((gate, up), N_GU, GU)):
                ends = list(itertools.accumulate([p.shape[2] for p in parts], initial=0))
                for first, n, _ in thirds(w):
                    got = take()
                    for tile in range(count):
                        at = tile * w + first
                        for p, begin, end in zip(parts, ends, ends[1:]):
                            a, b = max(at, begin), min(at + n, end)
                            if a < b:
                                p[layer, :, a - begin : b - begin] = got[:, tile * n + a - at : tile * n + b - at]
            o[layer] = take()
            down[layer] = take()


def finish(da, h, dhm, per_layer, bm=512):
    ins = [a for arrays in per_layer for a in arrays]
    kv, layers = KV * HEAD, len(per_layer)
    shapes = [(layers, ROWS, n) for n in (D, kv, kv, D, FF, FF)] + [(layers, FF // 16, D)]
    return run(functools.partial(_finish, n=len(ins)), "finish", T // bm, [da, h, dhm, *ins], [rows(bm, D)] * 3 + [ANY] * len(ins),
               [sds((T, D)), *(sds(s) for s in shapes)], [rows(bm, D), *(held(s) for s in shapes)],
               [pltpu.VMEM(a.shape, a.dtype) for a in ins] + [pltpu.SemaphoreType.DMA((len(ins),))])[0]


def solution(mesh):
    def both(x, dy, wq, wk, wv, wo, wg, wu, wd):
        cs = tuple(jnp.asarray(t) for t in tables())
        wkv = jnp.concatenate([wk, wv], axis=2)

        def projections(n):
            return [Gather(wq, n), Gather(wkv, n)]

        h0 = x[0]
        (q0, k0, v0, a0, at0, lse0), (*w_qkv0, wo0, wg0, wu0) = first(h0, cs, projections(0), [Gather(wo, 0), Gather(wg, 0), Gather(wu, 0)])
        w_qkv0, wo0, wg0, wu0 = [flat(w) for w in w_qkv0], flat(wo0), [flat(wg0)], [flat(wu0)]
        (hm0, gate0, up0, act0), (wd0, *w_qkv1) = mlp_up(h0, at0, wo0, wg0, wu0, send=[Gather(wd, 0), *projections(1)], ident=1, marks=(2, 5, 7))
        wd0, w_qkv1 = flat(wd0), [flat(w) for w in w_qkv1]
        (h1, q1, k1, v1, a1, at1, lse1), (wg1, wo1, wu1) = second(hm0, act0, wd0, cs, w_qkv1, send=[Gather(wg, 1), Gather(wo, 1), Gather(wu, 1)],
                                                                  ident=2, marks=(6, (10, 2), (11, 2)))
        wo1, wg1, wu1 = flat(wo1), [flat(wg1)], [flat(wu1)]
        (hm1, gate1, up1, act1), (wd1,) = mlp_up(h1, at1, wo1, wg1, wu1, send=[Gather(wd, 1)], ident=4, marks=(2, 4, 6))
        wd1 = flat(wd1)

        def spread(grads):
            return [Spread(sums, a) for g in grads for (sums, _), (a, _, _) in zip(g, AXES)]

        def with_own(grads, sent):
            return [x for g, n in zip(grads, range(len(grads))) for r in range(3) for x in (g[r][1], sent[3 * n + r])]

        def backward(d, ident, final, h, a, q, k, v, at, lse, hm, gate, up, act, w_qkv, wo, wg, wu, wd, before=()):
            (down, down_own), _ = down_grad(act, d, ident=ident)
            (dgu, b, dhm, dat, delta), (down_in, *sent_before) = mlp_back(d, hm, at, gate, up, wo, wg, wu, wd, send=[Scatter(down), *spread(before)],
                                                                         ident=ident + 1)
            gu, (o, o_own) = mlp_grads(b, dgu, at, dhm, ident=ident + 2)
            dh, dw, (*sent, o_in) = attend_enter_back(q, k, v, dat, lse, delta, cs, a, w_qkv, () if final else (h, dhm), final=final,
                                                      send=[*spread(gu), Scatter(o)], ident=ident + 3)
            return dh, dhm, dw, with_own(gu, sent) + [o_own, o_in, down_own, down_in], sent_before

        d0, _, dw1, done1, _ = backward(dy[0], 8, False, h1, a1, q1, k1, v1, at1, lse1, hm1, gate1, up1, act1, w_qkv1, wo1, wg1, wu1, wd1)
        da0, dhm0, dw0, done0, dw1_in = backward(d0, 14, True, h0, a0, q0, k0, v0, at0, lse0, hm0, gate0, up0, act0, w_qkv0, wo0, wg0, wu0, wd0, dw1)
        dx, *dws = finish(da0, h0, dhm0, [dw0 + done0, with_own(dw1, dw1_in) + done1])
        return (dx[None], *dws)

    states, cut = P(("rep", "dp"), None, None), P(None, "dp", None)
    return jax.shard_map(
        both,
        mesh=mesh,
        in_specs=(states, states) + (cut,) * 7,
        out_specs=(states,) + (P("rep", "dp", None),) * 7,
        check_vma=False,
    )
```

```python
import functools
import itertools

import jax
import jax.numpy as jnp
import numpy as np
from jax import lax
from jax.experimental import pallas as pl
from jax.experimental.pallas import tpu as pltpu
from jax.sharding import PartitionSpec as P

T, D, HEADS, KV, HEAD, FF, THETA = 2048, 1024, 8, 2, 128, 3200, 10000
G = HEADS // KV
VMEM = 62 * 2**20
MOST = 67043328
QKV = D + 2 * KV * HEAD
THIRD = QKV // 3
BF, F32 = jnp.bfloat16, jnp.float32
LOG2E = 1.4426950408889634
SCALE = HEAD**-0.5
NEG, HIDDEN = -1e30, -2e30
ANY = pl.BlockSpec(memory_space=pl.ANY)


def step():
    return pl.program_id(0)


def steps():
    return pl.num_programs(0)


def params(**kw):
    return pltpu.CompilerParams(**{"vmem_limit_bytes": VMEM, **kw})


def sds(shape, dtype=BF):
    return jax.ShapeDtypeStruct(shape, dtype)


def by_rows(bm, n, at):
    return pl.BlockSpec((bm, n), lambda i: (at(i), 0))


def by_cols(n, bm, at):
    return pl.BlockSpec((n, bm), lambda i: (0, at(i)))


def rows(bm, n):
    return by_rows(bm, n, lambda i: i)


def held(shape):
    return pl.BlockSpec(shape, lambda i: (0,) * len(shape), pipeline_mode=pl.Buffered(1))


def dot(a, b, ca=1, cb=0):
    return lax.dot_general(a, b, (((ca,), (cb,)), ((), ())), preferred_element_type=F32)


def dot_nt(a, b):
    return dot(a, b, 1, 1)


def dot_tn(a, b):
    return dot(a, b, 0, 0)


def low(x):
    return x.astype(BF)


def wide(x):
    return x.astype(F32)


def row_mean(x):
    return jnp.mean(x, -1, keepdims=True)


def norm_scale(w):
    return lax.rsqrt(row_mean(w * w) + 1e-6)


def normed(h):
    w = wide(h)
    return low(w * norm_scale(w))


def norm_back(h, c):
    w = wide(h)
    s = norm_scale(w)
    return s * (c - w * (s * s) * row_mean(c * w))


def enter_back(da, h, dhm):
    return low(wide(dhm) + wide(low(norm_back(h, wide(da)))))


def tables():
    half = HEAD // 2
    angle = np.arange(T, dtype=np.float32)[:, None] * (np.float32(THETA) ** (-np.arange(half, dtype=np.float32) / np.float32(half)))
    cos, sin = np.cos(angle).astype(np.float32), np.sin(angle).astype(np.float32)
    return np.concatenate([cos, cos], 1), np.concatenate([-sin, sin], 1)


def flat(w):
    return w.reshape(-1, w.shape[-1])


def head(n):
    return slice(HEAD * n, HEAD * (n + 1))


def heads_of(x):
    return [x[:, head(n)] for n in range(x.shape[1] // HEAD)]


def turned(x, c, s):
    return [low(t * c + pltpu.roll(t, HEAD // 2, 1) * s) for t in heads_of(x)]


X, Y, Z = 4, 2, 1
NEAR = {1, 2 * X, 2 * Y, 2 * Z}
FAR = {2 * n for n in range(1, 8)}


def place():
    me = lax.axis_index("dp")
    return me, lax.div(me, 2), me % 2


def flipped(number, bits):
    for bit in sorted(NEAR):
        if bits & bit:
            number = number + bit - 2 * bit * (lax.div(number, bit) % 2)
    return number


AXES = ((X, Y, Z), (Y, Z, X), (Z, X, Y))
OTHERS = ((0, 1), (1, 1), (1, 0))


def thirds(n):
    units = n // 128
    sizes = [128 * (units // 3 + (r < units % 3)) for r in range(3)]
    return [(sum(sizes[:r]), sizes[r], axes) for r, axes in enumerate(AXES)]


class Gather:
    copies = 24
    partners = NEAR

    def __init__(self, src, layer):
        self.src, self.layer = src, layer
        self.shape = (8, 2, *src.shape[1:])

    def bind(self, src, dst, send, recv):
        me, chip, core = place()
        own = src.at[self.layer]
        block = lambda bits: dst.at[flipped(chip, bits), core]
        count = iter(range(self.copies))

        def to(bits, where, first=0, n=None):
            k = next(count)
            cut = lambda ref: ref if n is None else ref.at[:, pl.ds(first, n)]
            return pltpu.make_async_remote_copy(cut(block(where)) if where else own, cut(block(where)), send.at[k], recv.at[k],
                                                device_id={"dp": flipped(me, bits)})

        split = thirds(dst.shape[3])
        self.links = [
            [to(2 * m, 0) for m in (X, Y, Z)],
            [to(2 * axes[to_], axes[from_], at, n) for from_, to_ in itertools.combinations(range(3), 2) for at, n, axes in split],
            [to(2 * c, a | b, at, n) for at, n, (a, b, c) in split],
        ]
        self.pairs = [[to(1, 0)], [to(1, m) for m in (X, Y, Z)], [to(1, m) for m in (X | Y, Y | Z, Z | X)], [to(1, X | Y | Z)]]
        self.local = pltpu.make_async_copy(own, block(0), send.at[self.copies - 1])
        self.ended = False

    def stage(self, n):
        for c in self.links[n - 1] if n else ():
            c.wait_recv()
        for c in (self.links[n] if n < 3 else []) + self.pairs[n]:
            c.start()
        if n == 0:
            self.local.start()

    def end(self):
        if not self.ended:
            self.ended = True
            for c in sum(self.pairs, []):
                c.wait_recv()
            for c in sum(self.links + self.pairs, []):
                c.wait_send()
            self.local.wait()


class Once:
    def stage(self, n):
        if n == 0:
            for c in self.all:
                c.start()

    def end(self):
        for c in self.all:
            c.wait()


class Scatter(Once):
    copies = 7
    partners = FAR

    def __init__(self, src):
        self.src = src
        self.shape = (7, *src.shape[1:])

    def bind(self, src, dst, send, recv):
        me, chip, _ = place()
        self.all = [
            pltpu.make_async_remote_copy(src.at[flipped(chip, m)], dst.at[m - 1], send.at[m - 1], recv.at[m - 1], device_id={"dp": flipped(me, 2 * m)})
            for m in (Z, Y | Z, Y, X | Y, X, X | Z, X | Y | Z)
        ]


def side(axis, index):
    return {X: (index,), Y: (slice(None), index), Z: (slice(None), slice(None), index)}[axis]


CUBE = (2, 2, 2)


def bit(chip, axis):
    return chip // axis % 2 if isinstance(chip, int) else lax.div(chip, axis) % 2


def spreads(src, dst, axis, send, recv):
    me, chip, _ = place()
    out = []
    for k, far in enumerate(OTHERS):
        bits = [b for b in AXES[0] if b != axis]
        i, j = (1 - bit(chip, b) if f else bit(chip, b) for b, f in zip(bits, far))
        where = 2 * sum(b * f for b, f in zip(bits, far))
        out.append(pltpu.make_async_remote_copy(src.at[i, j], dst.at[k], send.at[k], recv.at[k], device_id={"dp": flipped(me, where)}))
    return out


class Spread(Once):
    copies = 3

    def __init__(self, src, axis):
        self.src, self.axis = src, axis
        self.planes = tuple(b for b in AXES[0] if b != axis)
        p, q = self.planes
        self.partners = {2 * p, 2 * q, 2 * (p + q)}
        self.shape = (3, *src.shape[2:])

    def bind(self, src, dst, send, recv):
        self.all = spreads(src, dst, self.axis, send, recv)


def meet(partners):
    me = lax.axis_index("dp")
    barrier = pltpu.get_barrier_semaphore()
    for bits in sorted(partners):
        pl.semaphore_signal(barrier, inc=1, device_id={"dp": flipped(me, bits)})
    pl.semaphore_wait(barrier, len(partners))


def staged(send, marks, count):
    marks = (0, *marks) if any(isinstance(t, Gather) for t in send) else (0,)

    def stage(n):
        for t in send:
            t.stage(n)

    def end():
        for n, mark in enumerate(marks):
            if mark == count:
                stage(n)
        for t in send:
            t.end()

    return {mark: functools.partial(stage, n) for n, mark in enumerate(marks) if mark != count}, end


def run(body, name, count, ins, in_specs, outs, out_specs, scratch=(), send=(), ident=None, marks=(), partners=(), plan=staged, shown=0, early=False, **kw):
    n_in, n_out, n_send, n_scratch = len(ins), len(outs), len(send), len(scratch)
    partners = set(partners).union(*(t.partners for t in send))

    def kernel(*refs):
        def take(n):
            nonlocal refs
            got, refs = refs[:n], refs[n:]
            return got

        a, c_src, o, c_dst = take(n_in), take(n_send), take(n_out), take(n_send)
        s, sems = take(n_scratch), refs
        i = step()
        for n, t in enumerate(send):
            t.bind(c_src[n], c_dst[n], sems[2 * n], sems[2 * n + 1])
        starts, end = plan(send, marks, count)
        inner = {mark: act for mark, act in starts.items() if isinstance(mark, tuple)}
        seen = (*a, *c_dst[:shown], *o, *s)

        @pl.when(i == 0)
        def _():
            if early:
                body(*seen, early=True)
            if partners:
                meet(partners)
                starts[0]()

        for mark, act in starts.items():
            if mark and mark not in inner:
                pl.when(i == mark)(act)

        def tick(j):
            for (first, then), act in inner.items():
                pl.when((i == first) & (j == then))(act)

        body(*seen, **({"tick": tick} if inner else {}))
        if send:
            pl.when(i == count - 1)(end)

    got = list(pl.pallas_call(
        kernel, grid=(count,), in_specs=[*in_specs, *[ANY] * n_send], out_specs=[*out_specs, *[ANY] * n_send],
        out_shape=[*outs, *(sds(t.shape) for t in send)],
        scratch_shapes=[*scratch, *(pltpu.SemaphoreType.DMA((t.copies,)) for t in send for _ in range(2))],
        compiler_params=params(**(dict(collective_id=ident, has_side_effects=True) if partners else {}), **kw), name=name,
    )(*ins, *(t.src for t in send)))
    return got[:n_out], got[n_out:]


def steps_of(t, first, after):
    return pl.when((t >= first) & (t < after))


def start(copies):
    for c in copies:
        c.start()


def wait(copies):
    for c in copies:
        c.wait()


def fetched(pairs, sem):
    return [pltpu.make_async_copy(a, b, sem.at[n]) for n, (a, b) in enumerate(pairs)]


def _qkv(h, c, s, wq, wkv, q, k, v, a_out):
    a = normed(h[:])
    a_out[:] = a
    cc, ss = c[:], s[:]
    for n, t in enumerate(turned(wide(low(dot(a, flat(wq[:])))), cc, ss)):
        q[:, head(n)] = t
    kv = low(dot(a, flat(wkv[:])))
    for n, t in enumerate(turned(wide(kv[:, : KV * HEAD]), cc, ss)):
        k[:, head(n)] = t
    v[:] = kv[:, KV * HEAD :]


def later(bk, bq):
    place_of = functools.partial(lax.broadcasted_iota, jnp.int32, (bk, bq))
    return place_of(1) >= place_of(0)


def diagonal(part, at, size):
    half = size // 2
    part(at, half, 0, size, half)
    part(at + half, half, half, half, size)


def _attend(q, k, v, o, lse, top_s, mix_s, *, iq, tick):
    bq = TILE
    e = SCALE * LOG2E
    top_s[:] = jnp.full(top_s.shape, NEG, F32)
    mix_s[:] = jnp.zeros(mix_s.shape, F32)

    def part(at, bk, first, nq, done=0):
        here, cols = pl.ds(pl.multiple_of(at, bk), bk), pl.ds(first, nq)
        scores = [dot_nt(k[here, head(n // G)], q[cols, head(n)]) for n in range(HEADS)]
        ok = later(bk, nq)
        ones = jnp.ones((8, bk), BF)
        weights, keeps = [], []
        for n, x in enumerate(scores):
            if done:
                x = jnp.where(ok, x, HIDDEN)
            old = top_s[n : n + 1, cols]
            top = jnp.maximum(old, x.max(axis=0, keepdims=True))
            top_s[n : n + 1, cols] = top
            weights.append(low(jnp.exp2((x - top) * e)))
            keeps.append(jnp.exp2((old - top) * e))
        for n in range(HEADS):
            i = n // G
            values = jnp.concatenate([v[here, head(i)].T, ones], axis=0)
            mix = mix_s[n, :, cols] * keeps[n] + dot(values, weights[n])
            mix_s[n, :, cols] = mix
            if done:
                w = done - first
                total = mix[HEAD : HEAD + 1, :w]
                o[first:done, head(n)] = low((mix[:HEAD, :w] * (1 / total)).T)
                lse[n : n + 1, first:done] = top_s[n : n + 1, first:done] * SCALE + jnp.log(total)

    def whole(j, _):
        tick(j)
        part(j * bq, bq, 0, bq)

    lax.fori_loop(0, iq, whole, None)
    tick(iq)
    diagonal(part, iq * bq, bq)


TILE = 512


def project(x, c, s, wq, wkv, outs, kept, at):
    _qkv(x, c, s, wq, wkv, *outs)
    for ref, out in zip(kept, outs):
        ref[pl.ds(pl.multiple_of(at, out.shape[0]), out.shape[0]), :] = out[:]


def attend_to(iq, kept, o, lse, top_s, mix_s, tick):
    q, k, v = kept
    _attend(q.at[pl.ds(pl.multiple_of(iq * TILE, TILE), TILE)], k, v, o, lse, top_s, mix_s, iq=iq, tick=tick)


def joint(body, name, ins, in_specs, before, bm, outs, weights, **kw):
    kv, tiles = KV * HEAD, T // bm
    late = lambda i: jnp.maximum(i - before - tiles, 0)
    widths = [*outs, D, kv, kv, D]
    return run(functools.partial(body, bm=bm), name, before + tiles + T // TILE, ins, in_specs, [sds((T, w)) for w in widths] + [sds((T, D)), sds((HEADS, T), F32)],
               [early_rows(bm, w, before) for w in widths] + [by_rows(TILE, D, late), by_cols(HEADS, TILE, late)],
               [pltpu.VMEM((T, D), BF), pltpu.VMEM((T, kv), BF), pltpu.VMEM((T, kv), BF)] + [pltpu.VMEM(w, BF) for w in weights]
               + [pltpu.SemaphoreType.DMA((len(weights),)), pltpu.VMEM((HEADS, TILE), F32), pltpu.VMEM((HEADS, HEAD + 8, TILE), F32)], **kw)


def early_rows(bm, n, before):
    return by_rows(bm, n, lambda i: jnp.clip(i - before, 0, T // bm - 1))


def _first(x, c, s, wq_h, wkv_h, q_out, k_out, v_out, a_out, o, lse, q, k, v, wq, wkv, sem, top_s, mix_s, *, bm, tick):
    i = step()

    @pl.when(i == 0)
    def _():
        cp = fetched([(wq_h, wq), (wkv_h, wkv)], sem)
        start(cp)
        wait(cp)

    @steps_of(i, 1, T // bm + 1)
    def _():
        project(x, c, s, wq, wkv, (q_out, k_out, v_out, a_out), (q, k, v), (i - 1) * bm)

    @pl.when(i > T // bm)
    def _():
        attend_to(i - T // bm - 1, (q, k, v), o, lse, top_s, mix_s, tick)


def first(x, cs, own, rest, bm=512):
    def plan(send, marks, count):
        def begin():
            for stage in range(4):
                for t in own:
                    t.stage(stage)
                for t in {1: rest[:1], 2: rest[1:]}.get(stage, ()):
                    t.stage(0)
            for t in own:
                t.end()

        starts, end = staged(rest, marks, count)
        return {**starts, 0: begin}, end

    tiles = T // bm
    return joint(_first, "first", [x, *cs], [early_rows(bm, n, 1) for n in (D, HEAD, HEAD)], 1, bm, [], [own[0].shape, own[1].shape],
                 send=[*own, *rest], ident=0, marks=(tiles + 1, (2 * tiles, 2), 2 * tiles + 1), plan=plan, shown=len(own))


def _second(m, act, c, s, wd_h, wq_h, wkv_h, y, q_out, k_out, v_out, a_out, o, lse, q, k, v, wd, wq, wkv, sem, top_s, mix_s, *, bm, tick=None, early=False):
    i = step()
    cp = fetched([(wd_h, wd), (wq_h, wq), (wkv_h, wkv)], sem)
    if early:
        return start(cp)

    @pl.when(i == 0)
    def _():
        wait(cp)

    @pl.when(i < T // bm)
    def _():
        y[:] = low(wide(m[:]) + wide(low(dot(act[:], wd[:]))))
        project(y, c, s, wq, wkv, (q_out, k_out, v_out, a_out), (q, k, v), i * bm)

    @pl.when(i >= T // bm)
    def _():
        attend_to(i - T // bm, (q, k, v), o, lse, top_s, mix_s, tick)


def second(m, act, wd, cs, w, bm=256, **kw):
    return joint(_second, "second", [m, act, *cs, wd, *w], [early_rows(bm, n, 0) for n in (D, FF, HEAD, HEAD)] + [ANY] * 3, 0, bm, [D],
                 [wd.shape, *(x.shape for x in w)], early=True, **kw)


CHUNK = 768
CHUNKS = [(a, CHUNK if a + 2 * CHUNK <= FF else FF - a) for a in range(0, FF - CHUNK, CHUNK)]


def into(w, pieces):
    at, out = 0, []
    for p in pieces:
        out.append((p, w.at[:, pl.ds(at, p.shape[1])]))
        at += p.shape[1]
    return out


def lagged(bm, n):
    return by_rows(bm, n, lambda i: jnp.maximum(i - 2, 0))


def ahead(bm, n):
    return early_rows(bm, n, 1)


def _mlp_up(h, at, wo_h, *rest, n_gate, n_up, early=False):
    wg_h, wu_h, (hm, gate, up, act, wo, wg, wu, sem) = rest[:n_gate], rest[n_gate : n_gate + n_up], rest[n_gate + n_up :]
    first = step() == 0
    cp = fetched([(wo_h, wo), *into(wg, wg_h), *into(wu, wu_h)], sem)

    if early:
        return start(cp)

    @pl.when(first)
    def _():
        cp[0].wait()

    m = low(wide(h[:]) + wide(low(dot(at[:], wo[:]))))
    hm[:] = m
    b = normed(m)

    @pl.when(first)
    def _():
        for c in cp[1:]:
            c.wait()

    for a, n in CHUNKS:
        g, u = dot(b, wg[:, a : a + n]), dot(b, wu[:, a : a + n])
        gate[:, a : a + n] = g
        up[:, a : a + n] = u
        act[:, a : a + n] = low(jax.nn.silu(g) * u)


def mlp_up(h, at, wo, wg, wu, bm=256, **kw):
    return run(functools.partial(_mlp_up, n_gate=len(wg), n_up=len(wu)), "mlp_up", T // bm, [h, at, wo, *wg, *wu],
               [rows(bm, D), rows(bm, D)] + [ANY] * (1 + len(wg) + len(wu)),
               [sds((T, D)), sds((T, FF), F32), sds((T, FF), F32), sds((T, FF))], [rows(bm, D), rows(bm, FF), rows(bm, FF), rows(bm, FF)],
               [pltpu.VMEM((D, D), BF), pltpu.VMEM((D, FF), BF), pltpu.VMEM((D, FF), BF), pltpu.SemaphoreType.DMA((1 + len(wg) + len(wu),))], early=True, **kw)


def _mlp_back(dy, hm, at, gate, up, wo_h, wd_h, *rest, n_gate, n_up, early=False):
    wg_h, wu_h, rest = rest[:n_gate], rest[n_gate : n_gate + n_up], rest[n_gate + n_up :]
    dgu, b_out, dhm, dat, delta, wo, wg, wu, wd, sem, d_s, db_s = rest
    t, count = step() - 1, steps() - 2
    now, last = (t + 2) % 2, (t + 1) % 2
    cp = fetched([(wd_h.at[pl.ds(a, n)], wd.at[pl.ds(a, n)]) for a, n in CHUNKS] + [*into(wg, wg_h), *into(wu, wu_h), (wo_h, wo)], sem)
    n_down = len(CHUNKS)
    if early:
        return start(cp)

    def grads(wait=lambda copies: None):
        d = dy[:]
        d_s[now] = d
        for (a, n), c in zip(CHUNKS, cp):
            wait([c])
            da = wide(low(dot_nt(d, wd[a : a + n, :])))
            g, u = gate[:, a : a + n], up[:, a : a + n]
            s = jax.nn.sigmoid(g)
            gs = g * s
            dgu[:, a : a + n] = low(da * u * (s + gs * (1 - s)))
            dgu[:, FF + a : FF + a + n] = low(da * gs)
        wait(cp[n_down:])
        db_s[now] = low(wide(low(dot_nt(dgu[:, :FF], wg[:]))) + wide(low(dot_nt(dgu[:, FF:], wu[:]))))

    def leave():
        h = hm[:]
        b_out[:] = normed(h)
        m = enter_back(db_s[last], h, d_s[last])
        dhm[:] = m
        x = low(dot_nt(m, wo[:]))
        dat[:] = x
        lane = lax.broadcasted_iota(jnp.int32, (m.shape[0], HEAD), 1)
        sums = jnp.zeros((m.shape[0], HEAD), F32)
        for n, r in enumerate(heads_of(wide(x) * wide(at[:]))):
            sums = jnp.where(lane == n, r.sum(-1, keepdims=True), sums)
        delta[:] = sums.T[:HEADS, :]

    @pl.when(t == 0)
    def _():
        grads(lambda copies: [c.wait() for c in copies])

    @steps_of(t, 1, count)
    def _():
        leave()
        grads()

    pl.when(t == count)(leave)


def mlp_back(dy, hm, at, gate, up, wo, wg, wu, wd, bm=256, **kw):
    n = len(wg) + len(wu) + len(CHUNKS) + 1
    return run(functools.partial(_mlp_back, n_gate=len(wg), n_up=len(wu)), "mlp_back", T // bm + 2, [dy, hm, at, gate, up, wo, wd, *wg, *wu],
               [ahead(bm, D), lagged(bm, D), lagged(bm, D), ahead(bm, FF), ahead(bm, FF)] + [ANY] * (2 + len(wg) + len(wu)),
               [sds((T, 2 * FF)), sds((T, D)), sds((T, D)), sds((T, D)), sds((HEADS, T), F32)],
               [ahead(bm, 2 * FF), lagged(bm, D), lagged(bm, D), lagged(bm, D), by_cols(HEADS, bm, lambda i: jnp.maximum(i - 2, 0))],
               [pltpu.VMEM((D, D), BF), pltpu.VMEM((D, FF), BF), pltpu.VMEM((D, FF), BF), pltpu.VMEM((FF, D), BF), pltpu.SemaphoreType.DMA((n,)),
                pltpu.VMEM((2, bm, D), BF), pltpu.VMEM((2, bm, D), BF)], early=True, **kw)


def passed(out, back, send, recv, slot):
    return pltpu.make_async_remote_copy(out.at[slot], back.at[slot], send.at[slot], recv.at[slot], device_id={"dp": flipped(lax.axis_index("dp"), 1)})


def keep(x, tile, out, slot, core):
    w = x.shape[1]
    tile[slot, :, :, :, :, :, :w] = x.reshape(*tile.shape[1:6], w)
    out[slot, :, :, :, :, :w] = low(tile[slot, :, :, :, 1 - core, :, :w])


def _pair(act, dy, sums, own, tile, out, back, send, recv):
    t = step()
    me, chip, core = place()
    now, last = t % 2, (t + 1) % 2
    count = steps() - 1

    @pl.when(t > 0)
    def _():
        passed(out, back, send, recv, last).start()

    @pl.when(t < count)
    def _():
        keep(dot_tn(act[:], dy[:]), tile, out, now, core)

    @pl.when(t > 0)
    def _():
        passed(out, back, send, recv, last).wait()
        settle(tile, back, last, sums, own)


def settle(tile, back, slot, sums, own):
    _, chip, core = place()
    w = own.shape[1]
    sums[:] = low(tile[slot, :, :, :, core, :, :w] + wide(back[slot, :, :, :, :, :w])).reshape(sums.shape)
    here = (slot, *(bit(chip, b) for b in AXES[0]))
    own[:] = tile[(*here, core)][:, :w] + wide(back[here][:, :w])


def pair_scratch(r, w):
    return [pltpu.VMEM((2, *CUBE, 2, r, w), F32), pltpu.VMEM((2, *CUBE, r, w), BF), pltpu.VMEM((2, *CUBE, r, w), BF),
            pltpu.SemaphoreType.DMA((2,)), pltpu.SemaphoreType.DMA((2,))]


def down_grad(act, dy, w=256, **kw):
    r, n = FF // 16, D // w
    done = lambda i: jnp.maximum(i - 1, 0)
    return run(_pair, "down_grad", n + 1, [act, dy], [held((T, FF)), by_cols(T, w, lambda i: jnp.minimum(i, n - 1))],
               [sds((8, r, D)), sds((r, D), F32)], [pl.BlockSpec((8, r, w), lambda i: (0, 0, done(i))), by_cols(r, w, done)],
               pair_scratch(r, w), partners={1}, **kw)


ROWS = D // 16


def _quad(t, tiles, outs, tile, out, back, send, recv, half, *rest):
    half_out, half_back, half_send, half_recv = (rest[n : n + 3] for n in range(0, 12, 3))
    me, chip, core = place()
    now, last = (t + 8) % 2, (t + 9) % 2
    count = tiles[-1][1]

    def turn(r, n):
        return pltpu.make_async_remote_copy(half_out[r].at[n % 2], half_back[r].at[n % 4], half_send[r].at[n % 2], half_recv[r].at[n % 4],
                                            device_id={"dp": flipped(me, 2 * AXES[r][0])})

    @pl.when((t > 0) & (t <= count))
    def _():
        passed(out, back, send, recv, last).start()

    @steps_of(t, 2, 2 + max(after for (_, after, _), o in zip(tiles, outs) if len(o) == 3))
    def _():
        for r in range(3):
            turn(r, t - 2).start()

    for first, after, make in tiles:
        @steps_of(t, first, after)
        def _():
            keep(make(), tile, out, now, core)

    for (first, after, _), thirds_out in zip(tiles, outs):
        if len(thirds_out) == 1:
            @steps_of(t, first + 1, after + 1)
            def _():
                passed(out, back, send, recv, last).wait()
                settle(tile, back, last, *thirds_out[0])

            continue
        w = sum(o.shape[1] for _, o in thirds_out)

        @steps_of(t, first + 3, after + 3)
        def _():
            for r, ((at, n, (a, _, _)), (sums, own)) in enumerate(zip(thirds(w), thirds_out)):
                turn(r, t - 3).wait()
                here = pl.ds(at, n)
                came = half_back[r].at[(t - 3) % 4]
                sums[:] = low(half[last, :, :, :, here] + wide(came[:, :, :, :n]))
                i, j = (bit(chip, x) for x in AXES[0] if x != a)
                own[:] = half[last, i, j, :, here] + wide(came[i, j, :, :n])

        @steps_of(t, first + 1, after + 1)
        def _():
            passed(out, back, send, recv, last).wait()
            for r, (at, n, (a, _, _)) in enumerate(thirds(w)):
                here = pl.ds(at, n)

                def pair(index):
                    index = side(a, index)
                    index = (last, *index, *[slice(None)] * (3 - len(index)))
                    return tile[(*index, core, slice(None), here)] + wide(back[(*index, slice(None), here)])

                half[last, :, :, :, here] = pair(bit(chip, a))
                half_out[r][last, :, :, :, :n] = low(pair(1 - bit(chip, a)))


def quad_scratch(widths):
    parts = [max(thirds(w)[r][1] for w in widths) for r in range(3)]
    sems = lambda n: [pltpu.SemaphoreType.DMA((n,))] * 3
    return [*pair_scratch(ROWS, max(widths)), pltpu.VMEM((*CUBE, ROWS, max(widths)), F32), *(pltpu.VMEM((*CUBE, ROWS, n), BF) for n in parts),
            *(pltpu.VMEM((4, 2, 2, ROWS, n), BF) for n in parts), *sems(2), *sems(4)]


def quad_outs(sizes):
    outs, specs = [], []
    for count, w, first in sizes:
        at = lambda i, first=first, count=count: jnp.clip(i - first - 3, 0, count - 1)
        for _, n, _ in thirds(w):
            outs += [sds((2, 2, ROWS, count * n)), sds((ROWS, count * n), F32)]
            specs += [pl.BlockSpec((2, 2, ROWS, n), lambda i, at=at: (0, 0, 0, at(i))), by_cols(ROWS, n, at)]
    return outs, specs


def grouped(refs):
    pairs = list(zip(refs[::2], refs[1::2]))
    return [pairs[n : n + 3] for n in range(0, len(pairs), 3)]


N_GU = 5
GU = 2 * FF // N_GU


def _mlp_grads(b, dgu, at_h, dhm_h, *rest):
    rest, (at, dhm, sem) = rest[:-3], rest[-3:]
    t = step()
    cp = fetched([(at_h, at), (dhm_h, dhm)], sem)

    @pl.when(t == 1)
    def _():
        for c in cp:
            c.start()

    @pl.when(t == N_GU)
    def _():
        for c in cp:
            c.wait()

    outs = grouped(rest[:6]) + [[rest[6:8]]]
    _quad(t, [(0, N_GU, lambda: dot_tn(b[:], dgu[:])), (N_GU, N_GU + 1, lambda: dot_tn(at[:], dhm[:]))], outs, *rest[8:])


def mlp_grads(b, dgu, at, dhm, **kw):
    tile = lambda i: jnp.minimum(i, N_GU - 1)
    outs, specs = quad_outs([(N_GU, GU, 0)])
    outs += [sds((8, ROWS, D)), sds((ROWS, D), F32)]
    specs += [held((8, ROWS, D)), held((ROWS, D))]
    got, _ = run(_mlp_grads, "mlp_grads", N_GU + 3, [b, dgu, at, dhm], [held((T, D)), by_cols(T, GU, tile), ANY, ANY],
                 outs, specs, [*quad_scratch((GU, D)), pltpu.VMEM((T, D), BF), pltpu.VMEM((T, D), BF), pltpu.SemaphoreType.DMA((2,))],
                 partners=NEAR, **kw)
    return grouped(got[:6]), got[6:]


def _attend_back(iq, q, k, v, do, lse, delta, c_all, s_all, dq_all, dkv, sums, dk_s, dv_s):
    bq = TILE
    e = SCALE * LOG2E
    mine = pl.ds(pl.multiple_of(iq * bq, bq), bq)
    c, s, dq = c_all.at[mine], s_all.at[mine], dq_all.at[mine]

    @pl.when(iq == 0)
    def _():
        dk_s[:] = jnp.zeros_like(dk_s)
        dv_s[:] = jnp.zeros_like(dv_s)

    sums[:] = jnp.zeros(sums.shape, F32)
    lses = [lse[n : n + 1, :] * LOG2E for n in range(HEADS)]
    deltas = [delta[n : n + 1, :] for n in range(HEADS)]

    def part(at, bk, first, nq, done=0):
        here, cols = pl.ds(pl.multiple_of(at, bk), bk), slice(first, first + nq)
        ok = later(bk, nq)
        for i in range(KV):
            heads = range(G * i, G * (i + 1))
            kk, vv = k[here, head(i)], v[here, head(i)]
            scores = [dot_nt(kk, q[cols, head(n)]) for n in heads]
            dps = [dot_nt(vv, do[cols, head(n)]) for n in heads]
            for n, score, dp in zip(heads, scores, dps):
                p = jnp.exp2(score * e - lses[n][:, cols])
                if done:
                    p = jnp.where(ok, p, 0.0)
                ds = low(p * (dp - deltas[n][:, cols]))
                dv_s[i, here, :] += dot(low(p), do[cols, head(n)])
                dk_s[i, here, :] += dot(ds, q[cols, head(n)])
                at = (*(bit(n, b) for b in AXES[0]), slice(None), slice(None), cols)
                x = sums[at].reshape(HEAD, nq) + dot(kk.T, ds)
                sums[at] = x.reshape(-1, ROWS, nq)
                if done:
                    rows = slice(first, done)
                    dq[rows, head(n)] = turned(wide(low((x[:, : done - first] * SCALE).T)), c[rows], -s[rows])[0]

    lax.fori_loop(0, iq, lambda j, _: part(j * bq, bq, 0, bq), None)
    diagonal(part, iq * bq, bq)

    @pl.when(iq == BLOCKS - 1)
    def _():
        for i in range(KV):
            dkv[:, head(i)] = turned(wide(low(dk_s[i] * SCALE)), c_all[:], -s_all[:])[0]
            dkv[:, head(KV + i)] = low(dv_s[i])


N_QKV = 3
BLOCKS = T // TILE


def _enter_back(q, k, v, do, lse, delta, c_all, s_all, a_h, wq_h, wkv_h, *rest, bm, final, early=False):
    given, (dh, *rest) = ((), rest) if final else (rest[:2], rest[2:])
    rest, (dk_s, dv_s, dq, dkv, a, wq, wkv, sem) = rest[:-8], rest[-8:]
    t = step() - BLOCKS
    cp = fetched([(a_h, a), (wq_h, wq), (wkv_h, wkv)], sem)
    if early:
        return start(cp)

    moves = []
    if final:
        owns, came, rest, (*sums, send, recv) = rest[:6], rest[6:12], rest[12:-5], rest[-5:]
        outs = [[(sums[r].at[jnp.clip(t - 3, 0, N_QKV - 1)], owns[g + r]) for r in range(3)] for g in (0, 3)]
        for n in range(N_QKV):
            g, at = (0, n) if n < 2 else (3, 0)
            moves.append([c for r, (_, w, axes) in enumerate(thirds(THIRD))
                          for c in spreads(sums[r].at[n], came[g + r].at[:, :, pl.ds(at * w, w)], axes[0], send.at[n, r], recv.at[n, r])])
    else:
        outs, rest = grouped(rest[:12]), rest[12:]

    @pl.when(t < 0)
    def _():
        _attend_back(step(), q, k, v, do, lse, delta, c_all, s_all, dq, dkv, rest[0].at[0], dk_s, dv_s)

    pl.when(t == 0)(lambda: wait(cp))
    tiles = [(0, 1, lambda: dot_tn(a[:], dq[:, :THIRD])), (1, 2, lambda: dot_tn(a[:], dq[:, THIRD:])), (2, N_QKV, lambda: dot_tn(a[:], dkv[:]))]
    _quad(t, tiles, outs[:1] + outs, *rest)
    for n, copies in enumerate(moves):
        pl.when(t == n + 4)(functools.partial(start, copies))

    @pl.when(t >= N_QKV)
    def _():
        half = bm // 2
        for n in range(2):
            here = pl.ds(pl.multiple_of((t - N_QKV) * bm + n * half, half), half)
            there = slice(n * half, (n + 1) * half)
            da = low(dot_nt(dq[here], wq[:]) + dot_nt(dkv[here], wkv[:]))
            dh[there] = da if final else enter_back(da, *(x[there] for x in given))

    if final:
        pl.when(step() == steps() - 1)(lambda: wait(sum(moves, [])))


def attend_enter_back(q, k, v, do, lse, delta, cs, a, w, given, bm=512, final=False, **kw):
    at = lambda i: jnp.maximum(i - BLOCKS - N_QKV, 0)
    block = lambda i: jnp.minimum(i, BLOCKS - 1)
    outs, specs = quad_outs([(2, THIRD, BLOCKS), (1, THIRD, BLOCKS + 2)])
    scratch, partners = quad_scratch((THIRD,)), NEAR
    if final:
        partners = NEAR | FAR
        scratch += [pltpu.VMEM((N_QKV, *CUBE[1:], ROWS, n), BF) for _, n, _ in thirds(THIRD)] + [pltpu.SemaphoreType.DMA((N_QKV, 3, 3))] * 2
        outs, specs = outs[1::2] + [sds((3, *o.shape[2:])) for o in outs[::2]], specs[1::2] + [ANY] * 6
    scratch += [pltpu.VMEM((KV, T, HEAD), F32)] * 2
    scratch += [pltpu.VMEM(x, BF) for x in ((T, D), (T, THIRD), (T, D), *(x.shape for x in w))] + [pltpu.SemaphoreType.DMA((3,))]
    tile, keys, stats = by_rows(bm, D, at), held((T, KV * HEAD)), by_cols(HEADS, TILE, block)
    queries = by_rows(TILE, D, block)
    (dh, *got), sent = run(functools.partial(_enter_back, bm=bm, final=final), "attend_enter_back", BLOCKS + N_QKV + T // bm,
                           [q, k, v, do, lse, delta, *cs, a, *w, *given],
                           [queries, keys, keys, queries, stats, stats, held((T, HEAD)), held((T, HEAD))] + [ANY] * 3 + [tile] * len(given),
                           [sds((T, D)), *outs], [tile, *specs], scratch, partners=partners, early=True, vmem_limit_bytes=MOST, **kw)
    return dh, ([x for pair in zip(got[:6], got[6:]) for x in pair] if final else grouped(got)), sent


def _finish(da, h, dhm, *refs, n):
    arrays, dx, outs, here, sem = refs[:n], refs[n], refs[n + 1 : n + 8], refs[n + 8 : -1], refs[-1]
    t, layers = step(), outs[0].shape[0]
    cp = fetched(list(zip(arrays, here)), sem)
    pl.when(t == 0)(lambda: start(cp))
    dx[:] = enter_back(da[:], h[:], dhm[:])
    each = n // layers
    q, k, v, o, gate, up, down = outs
    for layer in range(layers):
        left = list(here[layer * each : (layer + 1) * each])
        take = lambda: low(left.pop(0)[:] + wide(left.pop(0)[:]).sum(0))

        @pl.when(t == steps() - layers + layer)
        def _():
            wait(cp[layer * each : (layer + 1) * each])
            for parts, count, w in (((q,), 2, THIRD), ((k, v), 1, THIRD), ((gate, up), N_GU, GU)):
                ends = list(itertools.accumulate([p.shape[2] for p in parts], initial=0))
                for first, n, _ in thirds(w):
                    got = take()
                    for tile in range(count):
                        at = tile * w + first
                        for p, begin, end in zip(parts, ends, ends[1:]):
                            a, b = max(at, begin), min(at + n, end)
                            if a < b:
                                p[layer, :, a - begin : b - begin] = got[:, tile * n + a - at : tile * n + b - at]
            o[layer] = take()
            down[layer] = take()


def finish(da, h, dhm, per_layer, bm=512):
    ins = [a for arrays in per_layer for a in arrays]
    kv, layers = KV * HEAD, len(per_layer)
    shapes = [(layers, ROWS, n) for n in (D, kv, kv, D, FF, FF)] + [(layers, FF // 16, D)]
    return run(functools.partial(_finish, n=len(ins)), "finish", T // bm, [da, h, dhm, *ins], [rows(bm, D)] * 3 + [ANY] * len(ins),
               [sds((T, D)), *(sds(s) for s in shapes)], [rows(bm, D), *(held(s) for s in shapes)],
               [pltpu.VMEM(a.shape, a.dtype) for a in ins] + [pltpu.SemaphoreType.DMA((len(ins),))])[0]


def solution(mesh):
    def both(x, dy, wq, wk, wv, wo, wg, wu, wd):
        cs = tuple(jnp.asarray(t) for t in tables())
        wkv = jnp.concatenate([wk, wv], axis=2)

        def projections(n):
            return [Gather(wq, n), Gather(wkv, n)]

        h0 = x[0]
        (q0, k0, v0, a0, at0, lse0), (*w_qkv0, wo0, wg0, wu0) = first(h0, cs, projections(0), [Gather(wo, 0), Gather(wg, 0), Gather(wu, 0)])
        w_qkv0, wo0, wg0, wu0 = [flat(w) for w in w_qkv0], flat(wo0), [flat(wg0)], [flat(wu0)]
        (hm0, gate0, up0, act0), (wd0, *w_qkv1) = mlp_up(h0, at0, wo0, wg0, wu0, send=[Gather(wd, 0), *projections(1)], ident=1, marks=(2, 5, 7))
        wd0, w_qkv1 = flat(wd0), [flat(w) for w in w_qkv1]
        (h1, q1, k1, v1, a1, at1, lse1), (wg1, wo1, wu1) = second(hm0, act0, wd0, cs, w_qkv1, send=[Gather(wg, 1), Gather(wo, 1), Gather(wu, 1)],
                                                                  ident=2, marks=(6, (10, 2), (11, 2)))
        wo1, wg1, wu1 = flat(wo1), [flat(wg1)], [flat(wu1)]
        (hm1, gate1, up1, act1), (wd1,) = mlp_up(h1, at1, wo1, wg1, wu1, send=[Gather(wd, 1)], ident=4, marks=(2, 4, 6))
        wd1 = flat(wd1)

        def spread(grads):
            return [Spread(sums, a) for g in grads for (sums, _), (a, _, _) in zip(g, AXES)]

        def with_own(grads, sent):
            return [x for g, n in zip(grads, range(len(grads))) for r in range(3) for x in (g[r][1], sent[3 * n + r])]

        def backward(d, ident, final, h, a, q, k, v, at, lse, hm, gate, up, act, w_qkv, wo, wg, wu, wd, before=()):
            (down, down_own), _ = down_grad(act, d, ident=ident)
            (dgu, b, dhm, dat, delta), (down_in, *sent_before) = mlp_back(d, hm, at, gate, up, wo, wg, wu, wd, send=[Scatter(down), *spread(before)],
                                                                         ident=ident + 1)
            gu, (o, o_own) = mlp_grads(b, dgu, at, dhm, ident=ident + 2)
            dh, dw, (*sent, o_in) = attend_enter_back(q, k, v, dat, lse, delta, cs, a, w_qkv, () if final else (h, dhm), final=final,
                                                      send=[*spread(gu), Scatter(o)], ident=ident + 3)
            return dh, dhm, dw, with_own(gu, sent) + [o_own, o_in, down_own, down_in], sent_before

        d0, _, dw1, done1, _ = backward(dy[0], 8, False, h1, a1, q1, k1, v1, at1, lse1, hm1, gate1, up1, act1, w_qkv1, wo1, wg1, wu1, wd1)
        da0, dhm0, dw0, done0, dw1_in = backward(d0, 14, True, h0, a0, q0, k0, v0, at0, lse0, hm0, gate0, up0, act0, w_qkv0, wo0, wg0, wu0, wd0, dw1)
        dx, *dws = finish(da0, h0, dhm0, [dw0 + done0, with_own(dw1, dw1_in) + done1])
        return (dx[None], *dws)

    states, cut = P(("rep", "dp"), None, None), P(None, "dp", None)
    return jax.shard_map(
        both,
        mesh=mesh,
        in_specs=(states, states) + (cut,) * 7,
        out_specs=(states,) + (P("rep", "dp", None),) * 7,
        check_vma=False,
    )
```
